16 devices in a mesh: stage: 2 (over z), data: 8 (over y, x, core).
Axes of the slice: x: 2, y: 2, z: 2, core: 2. Of those that a mesh axis runs over, the one named last changes fastest.
Arguments:
- inputs: bfloat16 [32, 256, 2560], P('data')
- targets: bfloat16 [32, 256, 2560], P('data')
- w_up: bfloat16 [2, 2560, 10240], P('stage')
- w_down: bfloat16 [2, 10240, 2560], P('stage')
Outputs:
- output 1: float32 [], replicated
- output 2: float32 [2, 2560, 10240], P('stage', 'data')
- output 3: float32 [2, 10240, 2560], P('stage', None, 'data')
All inputs are finite; a program needn't handle non-finite values.
Results may differ from the reference program's by a relative error of at most 0.0029477.
Values are sent between devices in bfloat16 or wider.
A program may use at most 1 GiB of HBM per device.

```python
import jax
import jax.numpy as jnp
from jax import lax

DATA_REPLICAS = 8
MICRO = 4
TOKENS = 256
D_MODEL = 2560
FFN = 10240
LAYERS = 2


def setup_inputs(seed: int = 0) -> dict:
    root_key = jax.random.key(seed)
    key_inputs, key_targets, key_up, key_down = jax.random.split(root_key, 4)
    n_rows = DATA_REPLICAS * MICRO
    inputs = jax.random.normal(key_inputs, (n_rows, TOKENS, D_MODEL), jnp.float32)
    targets = jax.random.normal(key_targets, (n_rows, TOKENS, D_MODEL), jnp.float32)
    w_up = jax.random.normal(key_up, (LAYERS, D_MODEL, FFN), jnp.float32) * D_MODEL ** -0.5
    w_down = jax.random.normal(key_down, (LAYERS, FFN, D_MODEL), jnp.float32) * 1.5 * (FFN * LAYERS) ** -0.5
    return {'inputs': inputs.astype(jnp.bfloat16), 'targets': targets.astype(jnp.bfloat16), 'w_up': w_up.astype(jnp.bfloat16), 'w_down': w_down.astype(jnp.bfloat16)}


def layer_forward(h_in, w_up, w_down):
    pre_act = jnp.dot(h_in, w_up, preferred_element_type=jnp.float32)
    gelu_out = jax.nn.gelu(pre_act).astype(jnp.bfloat16)
    branch = jnp.dot(gelu_out, w_down, preferred_element_type=jnp.float32)
    return (h_in.astype(jnp.float32) + branch).astype(jnp.bfloat16)


def layer_backward(h_in, grad_out, w_up, w_down):
    pre_act = jnp.dot(h_in, w_up, preferred_element_type=jnp.float32)
    gelu_full, gelu_vjp = jax.vjp(jax.nn.gelu, pre_act)
    gelu_out = gelu_full.astype(jnp.bfloat16)
    g_down = jnp.dot(gelu_out.T, grad_out, preferred_element_type=jnp.float32)
    grad_act = jnp.dot(grad_out, w_down.T, preferred_element_type=jnp.float32).astype(jnp.bfloat16)
    grad_pre = gelu_vjp(grad_act.astype(jnp.float32))[0].astype(jnp.bfloat16)
    g_up = jnp.dot(h_in.T, grad_pre, preferred_element_type=jnp.float32)
    back_prod = jnp.dot(grad_pre, w_up.T, preferred_element_type=jnp.float32)
    grad_in = (grad_out.astype(jnp.float32) + back_prod).astype(jnp.bfloat16)
    return grad_in, g_up, g_down


def reference(inputs, targets, w_up, w_down):
    inv_total = 1.0 / (inputs.shape[0] * inputs.shape[1])

    def fwd_step(h_cur, weights):
        return layer_forward(h_cur, weights[0], weights[1]), h_cur

    def bwd_step(grad_cur, packed):
        grad_in, g_up, g_down = layer_backward(packed[0], grad_cur, packed[1], packed[2])
        return grad_in, (g_up, g_down)

    def one_micro(loop_state, mb_pair):
        acc_up, acc_down, loss_sum = loop_state
        h_last, layer_ins = lax.scan(fwd_step, mb_pair[0], (w_up, w_down))
        resid_diff = h_last.astype(jnp.float32) - mb_pair[1].astype(jnp.float32)
        top_grad = (resid_diff * inv_total).astype(jnp.bfloat16)
        scan_out = lax.scan(bwd_step, top_grad, (layer_ins, w_up, w_down), reverse=True)
        grads_up, grads_down = scan_out[1]
        new_state = (acc_up + grads_up, acc_down + grads_down, loss_sum + jnp.sum(resid_diff * resid_diff))
        return new_state, None

    init_state = (jnp.zeros(w_up.shape, jnp.float32), jnp.zeros(w_down.shape, jnp.float32), jnp.zeros((), jnp.float32))
    final_state = lax.scan(one_micro, init_state, (inputs, targets))[0]
    return final_state[2] * (0.5 * inv_total), final_state[0], final_state[1]
```

```python
import functools
import math

import jax
import jax.numpy as jnp
from jax import lax
from jax.experimental import pallas as pl
from jax.experimental.pallas import tpu as pltpu
from jax.sharding import PartitionSpec as P

F32 = jnp.float32
BF16 = jnp.bfloat16
MESH = pl.DeviceIdType.MESH
COLS = (((1,), (1,)), ((), ()))
GC = math.sqrt(2.0 / math.pi)


def dot(a, b):
    return jnp.dot(a, b, preferred_element_type=F32)


def dot_cols(a, b):
    return lax.dot_general(a, b, COLS, preferred_element_type=F32)


def gelu(u):
    return u * (0.5 * (1.0 + jnp.tanh(GC * (u + 0.044715 * (u * u * u)))))


def gelu_grad(u):
    u2 = u * u
    t = jnp.tanh(GC * (u + 0.044715 * (u2 * u)))
    return 0.5 * (1.0 + t) + (0.5 * u) * (1.0 - t * t) * (GC + (3.0 * 0.044715 * GC) * u2)


def loop(n, body):
    lax.fori_loop(0, n, lambda i, c: (body(i), c)[1], 0)


def kernel(dims, x, y, w1, w2, m1, r1, m2, r2, lb, hc, ec, hn, en, ub, gb, qb, vx, pb,
           wb1, wb2, lacc, wsem, z_s, z_r, d_s, d_r, v_s, v_r, n_s, n_r, ms_s, ms_r, pe_s, pe_r, ls_s, ls_r):
    nm, T, D, Fk, fs, inv = dims
    nj = Fk // fs
    nt = 2 * nm
    dq, dr = D // 4, D // 8
    s = lax.axis_index('stage')
    r = lax.axis_index('data')
    k = r % 2
    pr = r + 1 - 2 * k
    fx = r + 2 - 4 * ((r // 2) % 2)
    fy = r + 4 - 8 * (r // 4)
    nb = fy * (1 - k) + fx * k
    pe = fx * (1 - k) + fy * k
    fb = k * Fk
    own = pl.ds(pl.multiple_of(k * T, T), T)
    oth = pl.ds(pl.multiple_of((1 - k) * T, T), T)
    is0, is1 = s == 0, s == 1

    def fcols(j):
        return pl.ds(pl.multiple_of(j * fs, fs), fs)

    def remote(src, dst, ss, rs, dev):
        return pltpu.make_async_remote_copy(src_ref=src, dst_ref=dst, send_sem=ss, recv_sem=rs, device_id=dev, device_id_type=MESH)

    def sched(t):
        kind0, i0 = t // nm, t % nm
        mid = (t > 0) & (t < nt - 1)
        kind1 = jnp.where(mid, (t + 1) % 2, jnp.where(t == 0, 0, 1))
        i1 = jnp.where(mid, jnp.where(t % 2 == 1, (t + 1) // 2, (t - 2) // 2), jnp.where(t == 0, 0, nm - 1))
        return jnp.where(is1, kind1, kind0), jnp.where(is1, i1, i0)

    def weights(g):
        j, sl = g % nj, g % 2
        cols = pl.ds(pl.multiple_of(fb + j * fs, fs), fs)
        return (pltpu.make_async_copy(w1.at[:, cols], wb1.at[sl], wsem.at[0, sl]),
                pltpu.make_async_copy(w2.at[cols, :], wb2.at[sl], wsem.at[1, sl]))

    for c in weights(0):
        c.start()

    @pl.when(is0)
    def _():
        for i in range(nm):
            remote(x.at[i], hc.at[i, own], d_s.at[i], d_r.at[i], (s, pr)).start()

    def phase1(ab, acc, uo, ui, go, tmp, yb, ob, alsem, usem, isem, gsem, psem, lsem, hsem):
        lacc[...] = jnp.zeros_like(lacc)

        def prep_a(t):
            kind, i = sched(t)

            @pl.when(is1 & (kind == 0))
            def _():
                c = remote(hc.at[i, own], hc.at[i, own], z_s.at[i], z_r.at[i], (s, r))
                c.wait_recv()
                remote(hc.at[i, own], hc.at[i, own], d_s.at[i], d_r.at[i], (s, pr)).start()

            @pl.when(is0 & (kind == 1))
            def _():
                c = remote(ec.at[i, own], ec.at[i, own], z_s.at[nm + i], z_r.at[nm + i], (s, r))
                c.wait_recv()
                remote(ec.at[i, own], ec.at[i, own], d_s.at[nm + i], d_r.at[nm + i], (s, pr)).start()

        def prep_b(t):
            kind, i = sched(t)
            ap = t % 2
            for kk, X, XN in ((0, hc, hn), (1, ec, en)):
                @pl.when(kind == kk)
                def _():
                    n = kk * nm + i
                    remote(X.at[i, own], X.at[i, oth], d_s.at[n], d_r.at[n], (s, pr)).wait_recv()
                    if kk == 1:
                        @pl.when(is1)
                        def _():
                            pltpu.make_async_copy(ob.at[0], ec.at[i, own], lsem.at[i]).wait()
                    if kk == 0:
                        @pl.when(is0)
                        def _():
                            remote(x.at[i], XN.at[i, own], n_s.at[n, 0], n_r.at[n, 0], (s, nb)).start()
                            pltpu.make_async_copy(x.at[i], ab.at[ap, own], alsem.at[ap, 0]).start()

                    @pl.when(is1 if kk == 0 else (s >= 0))
                    def _():
                        remote(X.at[i, own], XN.at[i, own], n_s.at[n, 0], n_r.at[n, 0], (s, nb)).start()
                        pltpu.make_async_copy(X.at[i, own], ab.at[ap, own], alsem.at[ap, 0]).start()
                    remote(X.at[i, oth], XN.at[i, oth], n_s.at[n, 1], n_r.at[n, 1], (s, nb)).start()
                    pltpu.make_async_copy(X.at[i, oth], ab.at[ap, oth], alsem.at[ap, 1]).start()

        def exchange(t):
            kind, i = sched(t)
            n = kind * nm + i
            return remote(acc.at[t % 2, oth], vx.at[n], v_s.at[n], v_r.at[n], (s, pr))

        def wait_out(t):
            kind, i = sched(t)

            @pl.when(is0 | (kind == 1))
            def _():
                n = kind * nm + i
                remote(ob.at[0], ec.at[i, own], z_s.at[n], z_r.at[n], (1 - s, r)).wait_send()

            @pl.when(is1 & (kind == 0))
            def _():
                remote(ob.at[0], ec.at[i, own], d_s.at[nm + i], d_r.at[nm + i], (s, pr)).wait_send()

        def post(t):
            kind, i = sched(t)
            n = kind * nm + i
            ap = t % 2
            exchange(t).wait()
            ld = pltpu.make_async_copy(vx.at[n], tmp, psem.at[0])
            ld.start()
            ly = pltpu.make_async_copy(y.at[i], yb, psem.at[1])
            ly.start()

            @pl.when(t >= 2)
            def _():
                wait_out(t - 2)
            ld.wait()
            ly.wait()
            last = is1 & (kind == 0)
            rb = min(64, T)

            def rows(b):
                lo = pl.ds(pl.multiple_of(b * rb, rb), rb)
                mine = pl.ds(pl.multiple_of(k * T + b * rb, rb), rb)
                h = (ab[ap, mine, :].astype(F32) + (acc[ap, mine, :] + tmp[lo, :])).astype(BF16)

                @pl.when(last)
                def _():
                    d = h.astype(F32) - yb[lo, :].astype(F32)
                    ob[ap, lo, :] = (d * inv).astype(BF16)
                    sq = jnp.sum((d * d).reshape(rb // 8, 8, D), axis=0)
                    part = lacc[...]
                    for c in range(D // 128):
                        part = part + sq[:, c * 128:(c + 1) * 128]
                    lacc[...] = part

                @pl.when(jnp.logical_not(last))
                def _():
                    ob[ap, lo, :] = h
            loop(T // rb, rows)

            @pl.when(is0)
            def _():
                remote(ob.at[ap], hc.at[i, own], z_s.at[n], z_r.at[n], (1 - s, r)).start()

            @pl.when(is1 & (kind == 1))
            def _():
                remote(ob.at[ap], ec.at[i, own], z_s.at[n], z_r.at[n], (1 - s, r)).start()

            @pl.when(last)
            def _():
                remote(ob.at[ap], ec.at[i, own], d_s.at[nm + i], d_r.at[nm + i], (s, pr)).start()
                pltpu.make_async_copy(ob.at[ap], ec.at[i, own], lsem.at[i]).start()

        def slot(t):
            kind, i = sched(t)
            ap = t % 2
            fwd, bwd = kind == 0, kind == 1

            def u_in(j):
                sl = (t * nj + j) % 2
                return pltpu.make_async_copy(ub.at[i, :, fcols(j)], ui.at[sl], isem.at[sl])

            def u_out(j):
                sl = (t * nj + j) % 2
                return pltpu.make_async_copy(uo.at[sl], ub.at[i, :, fcols(j)], usem.at[sl])

            def g_out(j, dst):
                sl = (t * nj + j) % 2
                return pltpu.make_async_copy(go.at[sl], dst.at[i, :, fcols(j)], gsem.at[sl])

            @pl.when(is0 | (t == 0))
            def _():
                prep_a(t)
                prep_b(t)

            @pl.when(bwd)
            def _():
                u_in(0).start()
            acc[ap] = jnp.zeros((2 * T, D), F32)
            pltpu.make_async_copy(hc.at[i, own], ab.at[ap, own], alsem.at[ap, 0]).wait()
            pltpu.make_async_copy(hc.at[i, oth], ab.at[ap, oth], alsem.at[ap, 1]).wait()

            @pl.when(is0 & fwd)
            def _():
                pltpu.make_async_copy(ab.at[ap, own], hc.at[i, own], hsem).start()

            def step(j):
                g = t * nj + j
                sl = g % 2
                for c in weights(g):
                    c.wait()
                for c in weights(g + 1):
                    c.start()

                @pl.when(is1 & (t > 0) & (j == nj // 2))
                def _():
                    post(t - 1)

                @pl.when(is1 & (t < nt - 1) & (j == nj // 2 + 1))
                def _():
                    prep_a(t + 1)

                @pl.when(is1 & (t < nt - 1) & (j == nj - 1))
                def _():
                    prep_b(t + 1)

                @pl.when(j >= 2)
                def _():
                    g_out(j - 2, gb).wait()

                @pl.when(fwd)
                def _():
                    @pl.when(j >= 2)
                    def _():
                        u_out(j - 2).wait()
                    uo[sl] = dot(ab[ap], wb1[sl])
                    go[sl] = gelu(uo[sl]).astype(BF16)
                    u_out(j).start()
                    g_out(j, gb).start()
                    acc[ap] += dot(go[sl], wb2[sl])

                @pl.when(bwd)
                def _():
                    u_in(j).wait()

                    @pl.when(j + 1 < nj)
                    def _():
                        u_in(j + 1).start()
                    p = dot_cols(ab[ap], wb2[sl]).astype(BF16)
                    go[sl] = (p.astype(F32) * gelu_grad(ui[sl])).astype(BF16)
                    g_out(j, qb).start()

                    @pl.when(is1)
                    def _():
                        acc[ap] += dot_cols(go[sl], wb1[sl])
            loop(nj, step)

            for j in (nj - 2, nj - 1):
                g_out(j, gb).wait()

                @pl.when(fwd)
                def _():
                    u_out(j).wait()

            @pl.when(is0 & fwd)
            def _():
                pltpu.make_async_copy(ab.at[ap, own], hc.at[i, own], hsem).wait()

            @pl.when(is1 | fwd)
            def _():
                exchange(t).start()

            @pl.when((is0 & fwd) | (is1 & (t == nt - 1)))
            def _():
                post(t)
        loop(nt, slot)

        for t in (2, 1):
            @pl.when(is0)
            def _():
                wait_out(nm - t)

            @pl.when(is1)
            def _():
                wait_out(nt - t)

    pl.run_scoped(
        phase1,
        pltpu.VMEM((2, 2 * T, D), BF16), pltpu.VMEM((2, 2 * T, D), F32),
        pltpu.VMEM((2, 2 * T, fs), F32), pltpu.VMEM((2, 2 * T, fs), F32), pltpu.VMEM((2, 2 * T, fs), BF16),
        pltpu.VMEM((T, D), F32), pltpu.VMEM((T, D), BF16), pltpu.VMEM((2, T, D), BF16),
        pltpu.SemaphoreType.DMA((2, 2)), pltpu.SemaphoreType.DMA((2,)), pltpu.SemaphoreType.DMA((2,)),
        pltpu.SemaphoreType.DMA((2,)), pltpu.SemaphoreType.DMA((2,)), pltpu.SemaphoreType.DMA((nm,)),
        pltpu.SemaphoreType.DMA,
    )

    def loss_copy(d):
        return remote(lacc, lb.at[r], ls_s.at[d], ls_r.at[r], (d // 8, d % 8))

    def loss_self():
        return pltpu.make_async_copy(lacc, lb.at[r], ls_s.at[8 + r])

    @pl.when(is1)
    def _():
        def send(d):
            @pl.when(d != 8 + r)
            def _():
                loss_copy(d).start()
        loop(16, send)
        loss_self().start()

    def phase2(ht, et, gv, qv, a, b, o, tb, tsem, asem, gqsem, osem):
        own_cols = pl.ds(pl.multiple_of((r // 2) * dq, 128), dq)
        peer_cols = pl.ds(pl.multiple_of((pe // 2) * dq, 128), dq)

        for q, X, dst in ((0, hc, ht), (0, hn, ht), (1, ec, et), (1, en, et)):
            near = X is hc or X is ec

            def build(i):
                if not near:
                    for h, rows in ((0, own), (1, oth)):
                        n = q * nm + i
                        remote(X.at[i, rows], X.at[i, rows], n_s.at[n, h], n_r.at[n, h], (s, nb)).wait_recv()
                cs = [pltpu.make_async_copy(X.at[i, :, cols], tb.at[c], tsem.at[c]) for c, cols in enumerate((own_cols, peer_cols))]
                for c in cs:
                    c.start()
                at = pl.multiple_of((i if near else nm + i) * 2 * T, 2 * T)
                for c in range(2):
                    cs[c].wait()
                    dst[c * dq:(c + 1) * dq, pl.ds(at, 2 * T)] = tb[c].T
            loop(nm, build)

        def stream(v):
            i, sl = v % nm, v % 2
            return (pltpu.make_async_copy(hn.at[i], a.at[sl], asem.at[0, sl]),
                    pltpu.make_async_copy(en.at[i], b.at[sl], asem.at[1, sl]))

        def saved(j, i):
            rows = pl.ds(pl.multiple_of(i * 2 * T, 2 * T), 2 * T)
            return (pltpu.make_async_copy(gb.at[i, :, fcols(j)], gv.at[rows], gqsem.at[0, i]),
                    pltpu.make_async_copy(qb.at[i, :, fcols(j)], qv.at[rows], gqsem.at[1, i]))

        def kept(q, j, m):
            cols = pl.ds(pl.multiple_of(fb + j * fs, fs), fs)
            mine = pltpu.make_async_copy(o.at[q, m], (m1, m2)[q].at[:, cols], osem.at[q, m])
            rest = pltpu.make_async_copy(o.at[q, m], pb.at[q, j, m], osem.at[q, m])
            return mine, rest

        def sends(j):
            cols = pl.ds(pl.multiple_of(fb + j * fs, fs), fs)
            out = []
            for q in range(2):
                out.append(remote(pb.at[q, j, 1 - k], (m1, m2)[q].at[:, cols], ms_s.at[q, j], ms_r.at[q, j], (s, pr)))
                for c in range(2):
                    out.append(remote(pb.at[q, j, 2 + c], (r1, r2)[q].at[:, cols], pe_s.at[q, c, j], pe_r.at[q, k, j], (s, pe - k + c)))
            return out

        def ship(j):
            for q in range(2):
                loop(4, lambda m: kept(q, j, m)[1].wait())
            for c in sends(j):
                c.start()

        for c in stream(0):
            c.start()

        def part(j):
            g = nt * nj + j
            ws = g % 2
            loop(nm, lambda i: [c.start() for c in saved(j, i)])
            for c in weights(g):
                c.wait()

            @pl.when(j + 1 < nj)
            def _():
                for c in weights(g + 1):
                    c.start()

            @pl.when(j >= 1)
            def _():
                ship(j - 1)

            def again(i):
                v = j * nm + i
                sl = v % 2
                for c in stream(v):
                    c.wait()

                @pl.when(v + 1 < nj * nm)
                def _():
                    for c in stream(v + 1):
                        c.start()
                rows = pl.ds(pl.multiple_of((nm + i) * 2 * T, 2 * T), 2 * T)
                u = dot(a[sl], wb1[ws])
                gv[rows, :] = gelu(u).astype(BF16)
                p = dot_cols(b[sl], wb2[ws]).astype(BF16)
                qv[rows, :] = (p.astype(F32) * gelu_grad(u)).astype(BF16)
            loop(nm, again)
            loop(nm, lambda i: [c.wait() for c in saved(j, i)])

            def grads(m):
                rows = pl.ds(pl.multiple_of(m * dr, dr), dr)
                o[0, m] = dot(ht[rows, :], qv[...])
                o[1, m] = dot(et[rows, :], gv[...])
                for q in range(2):
                    mine, rest = kept(q, j, m)

                    @pl.when(m == k)
                    def _():
                        mine.start()

                    @pl.when(m != k)
                    def _():
                        rest.start()
            loop(4, grads)
        loop(nj, part)
        ship(nj - 1)

        def finish(j):
            for c in sends(j):
                c.wait_send()
            cols = pl.ds(pl.multiple_of(fb + j * fs, fs), fs)
            for q in range(2):
                remote(pb.at[q, j, 0], (m1, m2)[q].at[:, cols], ms_s.at[q, j], ms_r.at[q, j], (s, pr)).wait_recv()
                for c in range(2):
                    remote(pb.at[q, j, 0], (r1, r2)[q].at[:, cols], pe_s.at[q, c, j], pe_r.at[q, c, j], (s, pr)).wait_recv()
        loop(nj, finish)

    nr = 2 * nm * 2 * T
    pl.run_scoped(
        phase2,
        pltpu.VMEM((2 * dq, nr), BF16), pltpu.VMEM((2 * dq, nr), BF16),
        pltpu.VMEM((nr, fs), BF16), pltpu.VMEM((nr, fs), BF16),
        pltpu.VMEM((2, 2 * T, D), BF16), pltpu.VMEM((2, 2 * T, D), BF16),
        pltpu.VMEM((2, 4, dr, fs), F32), pltpu.VMEM((2, 2 * T, dq), BF16),
        pltpu.SemaphoreType.DMA((2,)), pltpu.SemaphoreType.DMA((2, 2)), pltpu.SemaphoreType.DMA((2, nm)), pltpu.SemaphoreType.DMA((2, 4)),
    )

    def settle(n):
        @pl.when(is0 | (n < nm))
        def _():
            remote(hc.at[0, own], hc.at[0, own], d_s.at[n], d_r.at[n], (s, pr)).wait_send()
        for h in range(2):
            remote(hc.at[0, own], hn.at[0, own], n_s.at[n, h], n_r.at[n, h], (s, nb)).wait_send()
    loop(nt, settle)

    @pl.when(is1)
    def _():
        def sent(d):
            @pl.when(d != 8 + r)
            def _():
                loss_copy(d).wait_send()
        loop(16, sent)
        loss_self().wait()

    def got(n):
        @pl.when(is0 | (n != r))
        def _():
            remote(lacc, lb.at[n], ls_s.at[n], ls_r.at[n], (s, r)).wait_recv()
    loop(8, got)


def solution(mesh):
    n_data = mesh.shape['data']

    def per_device(inputs, targets, w_up, w_down):
        nm, T, D = inputs.shape
        F = w_up.shape[2]
        Fk = F // 2
        fs = min(512, Fk // 2)
        nj = Fk // fs
        dr = D // 8
        inv = 1.0 / (n_data * nm * T)
        dims = (nm, T, D, Fk, fs, inv)
        sd = jax.ShapeDtypeStruct
        out_shape = [
            sd((dr, F), F32), sd((dr, F), F32), sd((dr, F), F32), sd((dr, F), F32), sd((8, 8, 128), F32),
            sd((nm, 2 * T, D), BF16), sd((nm, 2 * T, D), BF16), sd((nm, 2 * T, D), BF16), sd((nm, 2 * T, D), BF16),
            sd((nm, 2 * T, Fk), F32), sd((nm, 2 * T, Fk), BF16), sd((nm, 2 * T, Fk), BF16),
            sd((2 * nm, T, D), F32), sd((2, nj, 4, dr, fs), F32),
        ]
        any_spec = pl.BlockSpec(memory_space=pl.ANY)
        sem = pltpu.SemaphoreType.DMA
        units = 8 * 2 * nm * T * D * F
        outs = pl.pallas_call(
            functools.partial(kernel, dims),
            out_shape=out_shape,
            in_specs=[any_spec] * 4,
            out_specs=[any_spec] * len(out_shape),
            scratch_shapes=[
                pltpu.VMEM((2, D, fs), BF16), pltpu.VMEM((2, fs, D), BF16), pltpu.VMEM((8, 128), F32),
                sem((2, 2)), sem((2 * nm,)), sem((2 * nm,)), sem((2 * nm,)), sem((2 * nm,)), sem((2 * nm,)), sem((2 * nm,)),
                sem((2 * nm, 2)), sem((2 * nm, 2)), sem((2, nj)), sem((2, nj)), sem((2, 2, nj)), sem((2, 2, nj)), sem((16,)), sem((8,)),
            ],
            compiler_params=pltpu.CompilerParams(has_side_effects=True, vmem_limit_bytes=67_000_000),
            cost_estimate=pl.CostEstimate(flops=units, bytes_accessed=10**9, transcendentals=0),
            name='train_step',
        )(inputs, targets, w_up.reshape(D, F), w_down.reshape(F, D))
        m1, r1, m2, r2, lb = outs[:5]
        loss = jnp.sum(lb) * (0.5 * inv)
        return loss, (m1 + r1)[None], (m2 + r2).T[None]

    return jax.shard_map(per_device, mesh=mesh, in_specs=(P('data', None, None), P('data', None, None), P('stage', None, None), P('stage', None, None)), out_specs=(P(), P('stage', 'data', None), P('stage', None, 'data')), check_vma=False)
```

```python
import functools
import math

import jax
import jax.numpy as jnp
from jax import lax
from jax.experimental import pallas as pl
from jax.experimental.pallas import tpu as pltpu
from jax.sharding import PartitionSpec as P

F32 = jnp.float32
BF16 = jnp.bfloat16
MESH = pl.DeviceIdType.MESH
COLS = (((1,), (1,)), ((), ()))
GC = math.sqrt(2.0 / math.pi)
DMA = pltpu.SemaphoreType.DMA
VMEM = pltpu.VMEM


def dot(a, b):
    return jnp.dot(a, b, preferred_element_type=F32)


def dot_cols(a, b):
    return lax.dot_general(a, b, COLS, preferred_element_type=F32)


def gelu_both(u):
    u2 = u * u
    t = jnp.tanh(GC * (u + 0.044715 * (u2 * u)))
    half = 0.5 * (1.0 + t)
    return u * half, half + (0.5 * u) * (1.0 - t * t) * (GC + (3.0 * 0.044715 * GC) * u2)


def loop(n, body):
    lax.fori_loop(0, n, lambda i, c: (body(i), c)[1], 0)


def local(src, dst, sem):
    return pltpu.make_async_copy(src, dst, sem)


def remote(src, dst, ss, rs, dev):
    return pltpu.make_async_remote_copy(src_ref=src, dst_ref=dst, send_sem=ss, recv_sem=rs, device_id=dev, device_id_type=MESH)


def kernel(dims, x, y, w1, w2, m1, r1, m2, r2, lb, ha, ea, ub, gb, qb, ua, ga, qa, vx, pb,
           lacc, z_s, z_r, d_s, d_r, v_s, v_r, n_s, n_r, x_s, x_r, f_s, f_r, h_s, h_r, ms_s, ms_r, pe_s, pe_r, ls_s, ls_r):
    nm, T, D, Fk, fs, inv = dims
    nj = Fk // fs
    nq = nj // 2
    nt = 2 * nm
    T2 = 2 * T
    dq, dr = D // 4, D // 8
    s = lax.axis_index('stage')
    r = lax.axis_index('data')
    k = r % 2
    xb = (r // 2) % 2
    yb_ = r // 4
    pr = r + 1 - 2 * k
    fx = r + 2 - 4 * xb
    fy = r + 4 - 8 * yb_
    dg = fy + 2 - 4 * xb
    ry, rx = fy - k, fx - k + 1
    nb = fy * (1 - k) + fx * k
    pe = fx * (1 - k) + fy * k
    fb = k * Fk
    fq = fb + (yb_ * (1 - k) + xb * k) * (Fk // 2)
    own = pl.ds(pl.multiple_of(k * T, T), T)
    oth = pl.ds(pl.multiple_of((1 - k) * T, T), T)
    is0, is1 = s == 0, s == 1

    def fcols(j):
        return pl.ds(pl.multiple_of(j * fs, fs), fs)

    def wcols(j, base):
        return pl.ds(pl.multiple_of(base + j * fs, fs), fs)

    def chip_cols(dev):
        return pl.ds(pl.multiple_of((dev // 2) * dq, 128), dq)

    def give(src, A, n, i, far):
        out = [
            remote(src, A.at[0, i, own], d_s.at[n], d_r.at[n], (s, pr)),
            remote(src, A.at[1, i, own], n_s.at[n, 0], n_r.at[n, k], (s, ry)),
            remote(src, A.at[1, i, own], n_s.at[n, 1], n_r.at[n, k], (s, rx)),
        ]
        if far:
            out.append(remote(src, A.at[3, i, own], x_s.at[n], x_r.at[n], (s, dg)))
        return out

    def got_half(sem):
        return remote(ha.at[0, 0, own], ha.at[0, 0, oth], x_s.at[0], sem, (s, pr))

    @pl.when(is0)
    def _():
        for i in range(nm):
            for c in give(x.at[i], ha, i, i, True):
                c.start()

    def phase1(wb1, wb2, ab, acc, uo, ui, go, tmp, yb, ob, wsem, alsem, usem, isem, gsem, psem, lsem, hsem):
        lacc[...] = jnp.zeros_like(lacc)

        def sched(t):
            mid = (t > 0) & (t < nt - 1)
            kind1 = jnp.where(mid, (t + 1) % 2, jnp.where(t == 0, 0, 1))
            i1 = jnp.where(mid, jnp.where(t % 2 == 1, (t + 1) // 2, (t - 2) // 2), jnp.where(t == 0, 0, nm - 1))
            return jnp.where(is1, kind1, 0), jnp.where(is1, i1, t)

        def c_w1(j):
            return local(w1.at[:, wcols(j, fb)], wb1.at[j % 2], wsem.at[0, j % 2])

        def c_w2(j):
            return local(w2.at[wcols(j, fb), :], wb2.at[j % 2], wsem.at[1, j % 2])

        def prep_a(t):
            kind, i = sched(t)

            @pl.when(is1 & (kind == 0))
            def _():
                got_half(z_r.at[i]).wait_recv()
                for c in give(ha.at[0, i, own], ha, i, i, False):
                    c.start()

        def u_in(i, j):
            return local(ub.at[i, :, fcols(j)], ui.at[j % 2], isem.at[j % 2])

        def prep_b(t):
            kind, i = sched(t)
            ap = t % 2
            for kk, A in ((0, ha), (1, ea)):
                @pl.when(kind == kk)
                def _():
                    got_half(d_r.at[kk * nm + i]).wait_recv()
                    if kk == 1:
                        local(ob.at[0], ea.at[0, i, own], lsem.at[i]).wait()
                        u_in(i, 0).start()
                    if kk == 0:
                        @pl.when(is0)
                        def _():
                            local(x.at[i], ab.at[ap, own], alsem.at[ap, 0]).start()

                    @pl.when(is1)
                    def _():
                        local(A.at[0, i, own], ab.at[ap, own], alsem.at[ap, 0]).start()
                    local(A.at[0, i, oth], ab.at[ap, oth], alsem.at[ap, 1]).start()

        def exchange(t):
            kind, i = sched(t)
            n = kind * nm + i
            return remote(acc.at[t % 2, oth], vx.at[n], v_s.at[n], v_r.at[n], (s, pr))

        def wait_out(t):
            kind, i = sched(t)

            @pl.when(is0 | (kind == 1))
            def _():
                n = kind * nm + i
                remote(ob.at[0], ea.at[0, i, own], z_s.at[n], z_r.at[n], (1 - s, r)).wait_send()

            @pl.when(is1 & (kind == 0))
            def _():
                for c in give(ob.at[0], ea, nm + i, i, False):
                    c.wait_send()

        def post_a(t):
            kind, i = sched(t)
            exchange(t).wait()
            local(vx.at[kind * nm + i], tmp, psem.at[0]).start()
            local(y.at[i], yb, psem.at[1]).start()

        def post_b(t):
            kind, i = sched(t)
            n = kind * nm + i
            ap = t % 2

            @pl.when(t >= 2)
            def _():
                wait_out(t - 2)
            local(vx.at[n], tmp, psem.at[0]).wait()
            local(y.at[i], yb, psem.at[1]).wait()
            last = is1 & (kind == 0)
            rb = min(64, T)

            def rows(b):
                lo = pl.ds(pl.multiple_of(b * rb, rb), rb)
                mine = pl.ds(pl.multiple_of(k * T + b * rb, rb), rb)
                h = (ab[ap, mine, :].astype(F32) + (acc[ap, mine, :] + tmp[lo, :])).astype(BF16)

                @pl.when(last)
                def _():
                    d = h.astype(F32) - yb[lo, :].astype(F32)
                    ob[ap, lo, :] = (d * inv).astype(BF16)
                    sq = jnp.sum((d * d).reshape(rb // 8, 8, D), axis=0)
                    part = lacc[...]
                    for c in range(D // 128):
                        part = part + sq[:, c * 128:(c + 1) * 128]
                    lacc[...] = part

                @pl.when(jnp.logical_not(last))
                def _():
                    ob[ap, lo, :] = h
            loop(T // rb, rows)

            @pl.when(is0)
            def _():
                remote(ob.at[ap], ha.at[0, i, own], z_s.at[n], z_r.at[n], (1 - s, r)).start()

            @pl.when(is1 & (kind == 1))
            def _():
                remote(ob.at[ap], ea.at[0, i, own], z_s.at[n], z_r.at[n], (1 - s, r)).start()

            @pl.when(last)
            def _():
                for c in give(ob.at[ap], ea, nm + i, i, False):
                    c.start()
                local(ob.at[ap], ea.at[0, i, own], lsem.at[i]).start()

        j_a = max(0, nj // 2 - 2)
        j_b = j_a + 1
        j_c = min(j_b + 1, nj - 2)
        j_d = nj - 2

        def slot(t):
            kind, i = sched(t)
            ap = t % 2
            more = t + 1 < nm + nm * s

            @pl.when(is0 | (t == 0))
            def _():
                prep_a(t)
                prep_b(t)

            local(ha.at[0, i, own], ab.at[ap, own], alsem.at[ap, 0]).wait()
            local(ha.at[0, i, oth], ab.at[ap, oth], alsem.at[ap, 1]).wait()

            @pl.when(is0)
            def _():
                local(ab.at[ap, own], ha.at[0, i, own], hsem).start()

            def hooks(j):
                late = is1 & (t > 0)

                @pl.when(late & (j == j_a))
                def _():
                    post_a(t - 1)

                @pl.when(late & (j == j_b))
                def _():
                    post_b(t - 1)

                @pl.when(is1 & more & (j == jnp.where(t == 0, j_d, j_c)))
                def _():
                    prep_a(t + 1)

                @pl.when(is1 & more & (j == j_d))
                def _():
                    prep_b(t + 1)

            def run(c1, c2, before, first, second, after):
                c1(0).wait()
                c1(1).start()
                before(0)
                acc[ap] = jnp.zeros((T2, D), F32)
                first(0)
                after(0)

                def step(j):
                    c1(j + 1).wait()
                    c2(j).wait()

                    @pl.when(j + 2 < nj)
                    def _():
                        c1(j + 2).start()
                    c2(j + 1).start()
                    hooks(j)
                    before(j + 1)
                    first(j + 1)
                    acc[ap] += second(j)
                    after(j + 1)
                loop(nj - 1, step)
                c2(nj - 1).wait()

                @pl.when(more)
                def _():
                    c_w1(0).start()
                    c_w2(0).start()
                acc[ap] += second(nj - 1)

            def g_out(j, dst):
                return local(go.at[j % 2], dst.at[i, :, fcols(j)], gsem.at[j % 2])

            def u_out(j):
                return local(uo.at[j % 2], ub.at[i, :, fcols(j)], usem.at[j % 2])

            @pl.when(kind == 0)
            def _():
                def before(j):
                    @pl.when(j >= 2)
                    def _():
                        u_out(j - 2).wait()
                        g_out(j - 2, gb).wait()

                def first(j):
                    for h in (slice(0, T), slice(T, T2)):
                        g, uo[j % 2, h] = gelu_both(dot(ab[ap, h], wb1[j % 2]))
                        go[j % 2, h] = g.astype(BF16)

                def after(j):
                    u_out(j).start()
                    g_out(j, gb).start()
                run(c_w1, c_w2, before, first, lambda j: dot(go[j % 2], wb2[j % 2]), after)
                for j in (nj - 2, nj - 1):
                    u_out(j).wait()
                    g_out(j, gb).wait()

            @pl.when(kind == 1)
            def _():
                def before(j):
                    @pl.when(j >= 2)
                    def _():
                        g_out(j - 2, qb).wait()
                    u_in(i, j).wait()

                    @pl.when(j + 1 < nj)
                    def _():
                        u_in(i, j + 1).start()

                def first(j):
                    p = dot_cols(ab[ap], wb2[j % 2]).astype(BF16)
                    go[j % 2] = (p.astype(F32) * ui[j % 2]).astype(BF16)
                run(c_w2, c_w1, before, first, lambda j: dot_cols(go[j % 2], wb1[j % 2]), lambda j: g_out(j, qb).start())
                for j in (nj - 2, nj - 1):
                    g_out(j, qb).wait()

            @pl.when(is0)
            def _():
                local(ab.at[ap, own], ha.at[0, i, own], hsem).wait()
            exchange(t).start()

            @pl.when(is0 | (t == nt - 1))
            def _():
                post_a(t)
                post_b(t)

        c_w1(0).start()
        c_w2(0).start()
        n_slots = nm + nm * s
        lax.fori_loop(0, n_slots, lambda t, c: (slot(t), c)[1], 0)
        wait_out(n_slots - 2)
        wait_out(n_slots - 1)

    pl.run_scoped(
        phase1,
        VMEM((2, D, fs), BF16), VMEM((2, fs, D), BF16), VMEM((2, T2, D), BF16), VMEM((2, T2, D), F32),
        VMEM((2, T2, fs), F32), VMEM((2, T2, fs), F32), VMEM((2, T2, fs), BF16),
        VMEM((T, D), F32), VMEM((T, D), BF16), VMEM((2, T, D), BF16),
        DMA((2, 2)), DMA((2, 2)), DMA((2,)), DMA((2,)), DMA((2,)), DMA((2,)), DMA((nm,)), DMA,
    )

    def loss_copy(d):
        return remote(lacc, lb.at[r], ls_s.at[d], ls_r.at[r], (d // 8, d % 8))

    def loss_self():
        return local(lacc, lb.at[r], ls_s.at[8 + r])

    @pl.when(is1)
    def _():
        def send(d):
            @pl.when(d != 8 + r)
            def _():
                loss_copy(d).start()
        loop(16, send)
        loss_self().start()

    nc = 4 * nm

    def all_tokens(wq1, wq2, ab, uo, ui, go, qsem, alsem, usem, isem, gsem):
        def c_q1(j):
            return local(w1.at[:, wcols(j, fq)], wq1.at[j], qsem.at[0, j])

        def c_q2(j):
            return local(w2.at[wcols(j, fq), :], wq2.at[j], qsem.at[1, j])
        for j in range(nq):
            c_q1(j).start()

        def arrive(A, n, c, i):
            @pl.when(c == 1)
            def _():
                for h in range(2):
                    got_half(n_r.at[n, h]).wait_recv()
                remote(A.at[1, i], A.at[2, i], f_s.at[n], f_r.at[n], (s, pr)).start()

            @pl.when(c == 2)
            def _():
                remote(A.at[1, i], A.at[2, i], f_s.at[n], f_r.at[n], (s, pr)).wait_recv()

            @pl.when(c == 3)
            def _():
                got_half(x_r.at[n]).wait_recv()
                remote(A.at[3, i, own], A.at[3, i, own], h_s.at[n], h_r.at[n], (s, pr)).start()
                got_half(h_r.at[n]).wait_recv()

        def c_ab(A, c, i, v):
            return local(A.at[c, i], ab.at[v % 2], alsem.at[v % 2])

        def block(c, i):
            return pl.ds(pl.multiple_of((c * nm + i) * T2, T2), T2)

        def run(A, at, ready, before, first, outs):
            def load(v):
                c, i = at(v)
                ready(c, i)
                c_ab(A, c, i, v).start()
            load(0)

            def chunk(v):
                c, i = at(v)
                c_ab(A, c, i, v).wait()

                def step(j):
                    g = v * nq + j

                    @pl.when((j == nq - 1) & (v + 1 < nc))
                    def _():
                        load(v + 1)

                    @pl.when(g >= 2)
                    def _():
                        for o in outs(g - 2):
                            o.wait()
                    before(g)
                    first(v, j, g % 2)
                    for o in outs(g):
                        o.start()
                loop(nq, step)
            loop(nc, chunk)
            for g in (nc * nq - 2, nc * nq - 1):
                for o in outs(g):
                    o.wait()

        def at_h(v):
            return v // nm, v % nm

        def outs_h(g):
            c, i = at_h(g // nq)
            return [local(uo.at[g % 2], ua.at[block(c, i), fcols(g % nq)], usem.at[g % 2]),
                    local(go.at[g % 2], ga.at[block(c, i), fcols(g % nq)], gsem.at[g % 2])]

        def before_h(g):
            @pl.when(g < nq)
            def _():
                c_q1(g).wait()
                c_q2(g).start()

        def first_h(v, j, sl):
            for h in (slice(0, T), slice(T, T2)):
                g, uo[sl, h] = gelu_both(dot(ab[v % 2, h], wq1[j]))
                go[sl, h] = g.astype(BF16)
        run(ha, at_h, lambda c, i: arrive(ha, i, c, i), before_h, first_h, outs_h)

        def at_e(v):
            return v % 4, v // 4

        def outs_e(g):
            c, i = at_e(g // nq)
            return [local(go.at[g % 2], qa.at[block(c, i), fcols(g % nq)], gsem.at[g % 2])]

        def u_in(g):
            c, i = at_e(g // nq)
            return local(ua.at[block(c, i), fcols(g % nq)], ui.at[g % 2], isem.at[g % 2])

        def before_e(g):
            @pl.when(g < nq)
            def _():
                c_q2(g).wait()
            u_in(g).wait()

            @pl.when(g + 1 < nc * nq)
            def _():
                u_in(g + 1).start()

        def ready_e(c, i):
            n = nm + i

            @pl.when(c == 0)
            def _():
                got_half(z_r.at[n]).wait_recv()
                for cp in give(ea.at[0, i, own], ea, n, i, True):
                    cp.start()
                got_half(d_r.at[n]).wait_recv()
            arrive(ea, n, c, i)

        def first_e(v, j, sl):
            p = dot_cols(ab[v % 2], wq2[j]).astype(BF16)
            go[sl] = (p.astype(F32) * ui[sl]).astype(BF16)
        u_in(0).start()
        run(ea, at_e, ready_e, before_e, first_e, outs_e)

    def sums0(hv, bv, o, tb, tsem, bsem, osem):
        nw = 4 * nq

        def at(w):
            return w // (2 * nq), (w // 2) % nq, w % 2

        def load(w):
            _, j, q = at(w)
            for qq, A in ((0, qa), (1, ga)):
                @pl.when(q == qq)
                def _():
                    local(A.at[:, fcols(j)], bv.at[w % 2], bsem.at[w % 2]).start()

        def far(w, q, m):
            j = at(w)[1]
            return remote(pb.at[q, j, 2 + m], (m1, m2)[q].at[:, wcols(j, fq)], pe_s.at[q, m, j], pe_r.at[q, k, j], (s, nb - k + m))

        def near(w, q):
            j = at(w)[1]
            return remote(pb.at[q, j, 1 - k], (m1, m2)[q].at[:, wcols(j, fq)], ms_s.at[q, j], ms_r.at[q, j], (s, pr))

        def ship(w):
            ps, j, q = at(w)
            for qq in range(2):
                @pl.when(q == qq)
                def _():
                    for m in range(2):
                        local(o.at[qq, m], pb.at[qq, j, m], osem.at[qq, m]).wait()

                    @pl.when(ps == 0)
                    def _():
                        for m in range(2):
                            far(w, qq, m).start()

                    @pl.when(ps == 1)
                    def _():
                        near(w, qq).start()

        def one(ps):
            cols = pl.ds(pl.multiple_of((nb // 2) * dq * (1 - ps) + (r // 2) * dq * ps, 128), dq)
            for qq, A in ((0, ha), (1, ea)):
                def c_t(v):
                    return local(A.at[v // nm, v % nm, :, cols], tb.at[v % 2], tsem.at[v % 2])
                c_t(0).start()

                def build(v):
                    c_t(v).wait()

                    @pl.when(v + 1 < nc)
                    def _():
                        c_t(v + 1).start()
                    hv[qq, :, pl.ds(pl.multiple_of(v * T2, T2), T2)] = tb[v % 2].T
                loop(nc, build)

            def unit(ww):
                w = ps * 2 * nq + ww
                _, j, q = at(w)
                local(qa.at[:, fcols(j)], bv.at[w % 2], bsem.at[w % 2]).wait()

                @pl.when(w + 1 < nw)
                def _():
                    load(w + 1)

                @pl.when(w >= 1)
                def _():
                    ship(w - 1)

                def grads(m):
                    rows = pl.ds(pl.multiple_of(m * dr, dr), dr)
                    o[q, m] = dot(hv[q, rows, :], bv[w % 2])
                    for qq, M in ((0, m1), (1, m2)):
                        here = (ps == 1) & (m == k)

                        @pl.when((q == qq) & here)
                        def _():
                            local(o.at[qq, m], M.at[:, wcols(j, fq)], osem.at[qq, m]).start()

                        @pl.when((q == qq) & jnp.logical_not(here))
                        def _():
                            local(o.at[qq, m], pb.at[qq, j, 2 * (1 - ps) + m], osem.at[qq, m]).start()
                loop(2, grads)
            loop(2 * nq, unit)
        load(0)
        loop(2, one)
        ship(nw - 1)

        def finish(j):
            w = 2 * j
            for q in range(2):
                near(w, q).wait()
                for m in range(2):
                    far(w, q, m).wait_send()
                    remote(pb.at[q, j, 0], (m1, m2)[q].at[:, wcols(j, fq)], ms_s.at[q, j], pe_r.at[q, m, j], (s, pr)).wait_recv()
        loop(nq, finish)

    def sums1(wb1, wb2, ht, et, gv, qv, a, b, o, tb, dv, wsem, tsem, asem, gqsem, osem):
        def weights(j):
            return (local(w1.at[:, wcols(j, fb)], wb1.at[j % 2], wsem.at[0, j % 2]),
                    local(w2.at[wcols(j, fb), :], wb2.at[j % 2], wsem.at[1, j % 2]))

        def stream(v):
            i, sl = v % nm, v % 2
            return (local(ha.at[1, i], a.at[sl], asem.at[0, sl]), local(ea.at[1, i], b.at[sl], asem.at[1, sl]))

        def saved(j, i):
            rows = pl.ds(pl.multiple_of(i * T2, T2), T2)
            return (local(gb.at[i, :, fcols(j)], gv.at[rows], gqsem.at[0, i]),
                    local(qb.at[i, :, fcols(j)], qv.at[rows], gqsem.at[1, i]))

        for c in weights(0):
            c.start()

        cols = (chip_cols(r), chip_cols(pe))
        for q, A, dst in ((0, ha, ht), (1, ea, et)):
            def c_t(v):
                return [local(A.at[v // nm, v % nm, :, cols[c]], tb.at[v % 2, c], tsem.at[v % 2, c]) for c in range(2)]

            def start(v):
                @pl.when(v >= nm)
                def _():
                    for h in range(2):
                        got_half(n_r.at[q * nm + v - nm, h]).wait_recv()
                for c in c_t(v):
                    c.start()
            start(0)

            def build(v):
                for c in c_t(v):
                    c.wait()

                @pl.when(v + 1 < 2 * nm)
                def _():
                    start(v + 1)
                for c in range(2):
                    dst[c * dq:(c + 1) * dq, pl.ds(pl.multiple_of(v * T2, T2), T2)] = tb[v % 2, c].T
            loop(2 * nm, build)

        for c in stream(0):
            c.start()

        def kept(q, j, m):
            mine = local(o.at[q, m], (m1, m2)[q].at[:, wcols(j, fb)], osem.at[q, m])
            rest = local(o.at[q, m], pb.at[q, j, m], osem.at[q, m])
            return mine, rest

        def sends(j):
            cs = wcols(j, fb)
            out = []
            for q in range(2):
                for c in range(2):
                    out.append(remote(pb.at[q, j, 2 + c], (r1, r2)[q].at[:, cs], pe_s.at[q, c, j], pe_r.at[q, k, j], (s, pe - k + c)))
                out.append(remote(pb.at[q, j, 1 - k], (m1, m2)[q].at[:, cs], ms_s.at[q, j], ms_r.at[q, j], (s, pr)))
            return out

        def ship(j):
            for q in range(2):
                loop(4, lambda m: kept(q, j, m)[1].wait())
            for c in sends(j):
                c.start()

        def part(j):
            ws = j % 2
            loop(nm, lambda i: [c.start() for c in saved(j, i)])
            for c in weights(j):
                c.wait()

            @pl.when(j + 1 < nj)
            def _():
                for c in weights(j + 1):
                    c.start()

            @pl.when(j >= 1)
            def _():
                ship(j - 1)

            def again(i):
                v = j * nm + i
                sl = v % 2
                for c in stream(v):
                    c.wait()

                @pl.when(v + 1 < nj * nm)
                def _():
                    for c in stream(v + 1):
                        c.start()
                rows = pl.ds(pl.multiple_of((nm + i) * T2, T2), T2)
                for h in range(2):
                    part_rows = pl.ds(pl.multiple_of((nm + i) * T2 + h * T, T), T)
                    g, dv[h * T:(h + 1) * T] = gelu_both(dot(a[sl, h * T:(h + 1) * T], wb1[ws]))
                    gv[part_rows, :] = g.astype(BF16)
                p = dot_cols(b[sl], wb2[ws]).astype(BF16)
                qv[rows, :] = (p.astype(F32) * dv[...]).astype(BF16)
            loop(nm, again)
            loop(nm, lambda i: [c.wait() for c in saved(j, i)])

            def grads(m):
                rows = pl.ds(pl.multiple_of(m * dr, dr), dr)
                o[0, m] = dot(ht[rows, :], qv[...])
                o[1, m] = dot(et[rows, :], gv[...])
                for q in range(2):
                    mine, rest = kept(q, j, m)

                    @pl.when(m == k)
                    def _():
                        mine.start()

                    @pl.when(m != k)
                    def _():
                        rest.start()
            loop(4, grads)
        loop(nj, part)
        ship(nj - 1)

        def finish(j):
            for c in sends(j):
                c.wait_send()
            for q in range(2):
                remote(pb.at[q, j, 0], (m1, m2)[q].at[:, wcols(j, fb)], ms_s.at[q, j], ms_r.at[q, j], (s, pr)).wait_recv()
                for c in range(2):
                    remote(pb.at[q, j, 0], (r1, r2)[q].at[:, wcols(j, fb)], ms_s.at[q, j], pe_r.at[q, c, j], (s, pr)).wait_recv()
        loop(nj, finish)

    nr = 2 * nm * T2

    @pl.when(is0)
    def _():
        pl.run_scoped(
            all_tokens,
            VMEM((nq, D, fs), BF16), VMEM((nq, fs, D), BF16), VMEM((2, T2, D), BF16),
            VMEM((2, T2, fs), F32), VMEM((2, T2, fs), F32), VMEM((2, T2, fs), BF16),
            DMA((2, nq)), DMA((2,)), DMA((2,)), DMA((2,)), DMA((2,)),
        )
        pl.run_scoped(
            sums0,
            VMEM((2, dq, 2 * nr), BF16), VMEM((2, 2 * nr, fs), BF16), VMEM((2, 2, dr, fs), F32), VMEM((2, T2, dq), BF16),
            DMA((2,)), DMA((2,)), DMA((2, 2)),
        )

    @pl.when(is1)
    def _():
        pl.run_scoped(
            sums1,
            VMEM((2, D, fs), BF16), VMEM((2, fs, D), BF16),
            VMEM((2 * dq, nr), BF16), VMEM((2 * dq, nr), BF16), VMEM((nr, fs), BF16), VMEM((nr, fs), BF16),
            VMEM((2, T2, D), BF16), VMEM((2, T2, D), BF16), VMEM((2, 4, dr, fs), F32), VMEM((2, 2, T2, dq), BF16), VMEM((T2, fs), F32),
            DMA((2, 2)), DMA((2, 2)), DMA((2, 2)), DMA((2, nm)), DMA((2, 4)),
        )

    def settle(n):
        A = ha

        @pl.when(is0 | (n < nm))
        def _():
            for c in give(A.at[0, 0, own], A, n, 0, False):
                c.wait_send()

        @pl.when(is0)
        def _():
            remote(A.at[3, 0, own], A.at[3, 0, own], x_s.at[n], x_r.at[n], (s, dg)).wait_send()
            remote(A.at[3, 0, own], A.at[3, 0, own], h_s.at[n], h_r.at[n], (s, pr)).wait_send()
            remote(A.at[1, 0], A.at[2, 0], f_s.at[n], f_r.at[n], (s, pr)).wait_send()
    loop(nt, settle)

    @pl.when(is1)
    def _():
        def sent(d):
            @pl.when(d != 8 + r)
            def _():
                loss_copy(d).wait_send()
        loop(16, sent)
        loss_self().wait()

    def got(n):
        @pl.when(is0 | (n != r))
        def _():
            remote(lacc, lb.at[n], ls_s.at[n], ls_r.at[n], (s, r)).wait_recv()
    loop(8, got)


def solution(mesh):
    n_data = mesh.shape['data']

    def per_device(inputs, targets, w_up, w_down):
        nm, T, D = inputs.shape
        F = w_up.shape[2]
        Fk = F // 2
        fs = min(512, Fk // 4)
        nj = Fk // fs
        dr = D // 8
        inv = 1.0 / (n_data * nm * T)
        dims = (nm, T, D, Fk, fs, inv)
        sd = jax.ShapeDtypeStruct
        rows = 4 * nm * 2 * T
        out_shape = [
            sd((dr, F), F32), sd((dr, F), F32), sd((dr, F), F32), sd((dr, F), F32), sd((8, 8, 128), F32),
            sd((4, nm, 2 * T, D), BF16), sd((4, nm, 2 * T, D), BF16),
            sd((nm, 2 * T, Fk), F32), sd((nm, 2 * T, Fk), BF16), sd((nm, 2 * T, Fk), BF16),
            sd((rows, Fk // 2), F32), sd((rows, Fk // 2), BF16), sd((rows, Fk // 2), BF16),
            sd((2 * nm, T, D), F32), sd((2, nj, 4, dr, fs), F32),
        ]
        any_spec = pl.BlockSpec(memory_space=pl.ANY)
        n2 = 2 * nm
        outs = pl.pallas_call(
            functools.partial(kernel, dims),
            out_shape=out_shape,
            in_specs=[any_spec] * 4,
            out_specs=[any_spec] * len(out_shape),
            scratch_shapes=[
                VMEM((8, 128), F32),
                DMA((n2,)), DMA((n2,)), DMA((n2,)), DMA((n2,)), DMA((n2,)), DMA((n2,)), DMA((n2, 2)), DMA((n2, 2)),
                DMA((n2,)), DMA((n2,)), DMA((n2,)), DMA((n2,)), DMA((n2,)), DMA((n2,)),
                DMA((2, nj)), DMA((2, nj)), DMA((2, 2, nj)), DMA((2, 2, nj)), DMA((16,)), DMA((8,)),
            ],
            compiler_params=pltpu.CompilerParams(has_side_effects=True, vmem_limit_bytes=67_000_000),
            cost_estimate=pl.CostEstimate(flops=16 * nm * T * D * F, bytes_accessed=10**9, transcendentals=0),
            name='train_step',
        )(inputs, targets, w_up.reshape(D, F), w_down.reshape(F, D))
        m1, r1, m2, r2, lb = outs[:5]
        loss = jnp.sum(lb) * (0.5 * inv)
        whole = lax.axis_index('stage') == 0
        up = jnp.where(whole, m1, m1 + r1)
        down = jnp.where(whole, m2, m2 + r2)
        return loss, up[None], down.T[None]

    return jax.shard_map(per_device, mesh=mesh, in_specs=(P('data', None, None), P('data', None, None), P('stage', None, None), P('stage', None, None)), out_specs=(P(), P('stage', 'data', None), P('stage', None, 'data')), check_vma=False)
```

```python
import functools
import math

import jax
import jax.numpy as jnp
from jax import lax
from jax.experimental import pallas as pl
from jax.experimental.pallas import tpu as pltpu
from jax.sharding import PartitionSpec as P

F32 = jnp.float32
BF16 = jnp.bfloat16
MESH = pl.DeviceIdType.MESH
SC = jax.named_scope
COLS = (((1,), (1,)), ((), ()))
GC = math.sqrt(2.0 / math.pi)
DMA = pltpu.SemaphoreType.DMA
VMEM = pltpu.VMEM


def dot(a, b):
    return jnp.dot(a, b, preferred_element_type=F32)


def dot_cols(a, b):
    return lax.dot_general(a, b, COLS, preferred_element_type=F32)


def gelu_both(u):
    u2 = u * u
    t = jnp.tanh(GC * (u + 0.044715 * (u2 * u)))
    half = 0.5 * (1.0 + t)
    return u * half, half + (0.5 * u) * (1.0 - t * t) * (GC + (3.0 * 0.044715 * GC) * u2)


def loop(n, body):
    lax.fori_loop(0, n, lambda i, c: (body(i), c)[1], 0)


def local(src, dst, sem):
    return pltpu.make_async_copy(src, dst, sem)


def remote(src, dst, ss, rs, dev):
    return pltpu.make_async_remote_copy(src_ref=src, dst_ref=dst, send_sem=ss, recv_sem=rs, device_id=dev, device_id_type=MESH)


def kernel(dims, x, y, w1, w2, m1, r1, m2, r2, lb, ha, ea, ub, gb, qb, ua, ga, qa, vx, pb,
           lacc, z_s, z_r, d_s, d_r, v_s, v_r, n_s, n_r, x_s, x_r, f_s, f_r, h_s, h_r, ms_s, ms_r, pe_s, pe_r, ls_s, ls_r):
    nm, T, D, Fk, fs, inv = dims
    nj = Fk // fs
    nq = nj // 2
    nt = 2 * nm
    T2 = 2 * T
    dq, dr = D // 4, D // 8
    s = lax.axis_index('stage')
    r = lax.axis_index('data')
    k = r % 2
    xb = (r // 2) % 2
    yb_ = r // 4
    pr = r + 1 - 2 * k
    fx = r + 2 - 4 * xb
    fy = r + 4 - 8 * yb_
    dg = fy + 2 - 4 * xb
    ry, rx = fy - k, fx - k + 1
    nb = fy * (1 - k) + fx * k
    pe = fx * (1 - k) + fy * k
    fb = k * Fk
    fq = fb + (yb_ * (1 - k) + xb * k) * (Fk // 2)
    own = pl.ds(pl.multiple_of(k * T, T), T)
    oth = pl.ds(pl.multiple_of((1 - k) * T, T), T)
    is0, is1 = s == 0, s == 1

    def fcols(j):
        return pl.ds(pl.multiple_of(j * fs, fs), fs)

    def wcols(j, base):
        return pl.ds(pl.multiple_of(base + j * fs, fs), fs)

    def chip_cols(dev):
        return pl.ds(pl.multiple_of((dev // 2) * dq, 128), dq)

    def give(src, A, n, i, far):
        out = [
            remote(src, A.at[0, i, own], d_s.at[n], d_r.at[n], (s, pr)),
            remote(src, A.at[1, i, own], n_s.at[n, 0], n_r.at[n, k], (s, ry)),
            remote(src, A.at[1, i, own], n_s.at[n, 1], n_r.at[n, k], (s, rx)),
        ]
        if far:
            out.append(remote(src, A.at[3, i, own], x_s.at[n], x_r.at[n], (s, dg)))
        return out

    def got_half(sem):
        return remote(ha.at[0, 0, own], ha.at[0, 0, oth], x_s.at[0], sem, (s, pr))

    @pl.when(is0)
    def _():
        for i in range(nm):
            for c in give(x.at[i], ha, i, i, True):
                c.start()

    def phase1(wb1, wb2, ab, acc, uo, ui, go, tmp, yb, ob, wsem, alsem, usem, isem, gsem, psem, lsem, hsem):
        lacc[...] = jnp.zeros_like(lacc)

        def sched(t):
            mid = (t > 0) & (t < nt - 1)
            kind1 = jnp.where(mid, (t + 1) % 2, jnp.where(t == 0, 0, 1))
            i1 = jnp.where(mid, jnp.where(t % 2 == 1, (t + 1) // 2, (t - 2) // 2), jnp.where(t == 0, 0, nm - 1))
            return jnp.where(is1, kind1, 0), jnp.where(is1, i1, t)

        def c_w1(j):
            return local(w1.at[:, wcols(j, fb)], wb1.at[j % 2], wsem.at[0, j % 2])

        def c_w2(j):
            return local(w2.at[wcols(j, fb), :], wb2.at[j % 2], wsem.at[1, j % 2])

        def prep_a(t):
            kind, i = sched(t)

            @pl.when(is1 & (kind == 0))
            def _():
                with SC('w_z_h'):
                    got_half(z_r.at[i]).wait_recv()
                for c in give(ha.at[0, i, own], ha, i, i, False):
                    c.start()

        def u_in(i, j):
            return local(ub.at[i, :, fcols(j)], ui.at[j % 2], isem.at[j % 2])

        def prep_b(t):
            kind, i = sched(t)
            ap = t % 2
            for kk, A in ((0, ha), (1, ea)):
                @pl.when(kind == kk)
                def _():
                    with SC('w_d'):
                        got_half(d_r.at[kk * nm + i]).wait_recv()
                    if kk == 1:
                        local(ob.at[0], ea.at[0, i, own], lsem.at[i]).wait()
                        u_in(i, 0).start()
                    if kk == 0:
                        @pl.when(is0)
                        def _():
                            local(x.at[i], ab.at[ap, own], alsem.at[ap, 0]).start()

                    @pl.when(is1)
                    def _():
                        local(A.at[0, i, own], ab.at[ap, own], alsem.at[ap, 0]).start()
                    local(A.at[0, i, oth], ab.at[ap, oth], alsem.at[ap, 1]).start()

        def exchange(t):
            kind, i = sched(t)
            n = kind * nm + i
            return remote(acc.at[t % 2, oth], vx.at[n], v_s.at[n], v_r.at[n], (s, pr))

        def wait_out(t):
            kind, i = sched(t)

            @pl.when(is0 | (kind == 1))
            def _():
                n = kind * nm + i
                remote(ob.at[0], ea.at[0, i, own], z_s.at[n], z_r.at[n], (1 - s, r)).wait_send()

            @pl.when(is1 & (kind == 0))
            def _():
                for c in give(ob.at[0], ea, nm + i, i, False):
                    c.wait_send()

        def post_a(t):
            kind, i = sched(t)
            with SC('w_exch'):
                exchange(t).wait()
            local(vx.at[kind * nm + i], tmp, psem.at[0]).start()
            local(y.at[i], yb, psem.at[1]).start()

        def post_b(t):
            kind, i = sched(t)
            n = kind * nm + i
            ap = t % 2

            @pl.when(t >= 2)
            def _():
                with SC('w_out'):
                    wait_out(t - 2)
            local(vx.at[n], tmp, psem.at[0]).wait()
            local(y.at[i], yb, psem.at[1]).wait()
            last = is1 & (kind == 0)
            rb = min(64, T)

            def rows(b):
                lo = pl.ds(pl.multiple_of(b * rb, rb), rb)
                mine = pl.ds(pl.multiple_of(k * T + b * rb, rb), rb)
                h = (ab[ap, mine, :].astype(F32) + (acc[ap, mine, :] + tmp[lo, :])).astype(BF16)

                @pl.when(last)
                def _():
                    d = h.astype(F32) - yb[lo, :].astype(F32)
                    ob[ap, lo, :] = (d * inv).astype(BF16)
                    sq = jnp.sum((d * d).reshape(rb // 8, 8, D), axis=0)
                    part = lacc[...]
                    for c in range(D // 128):
                        part = part + sq[:, c * 128:(c + 1) * 128]
                    lacc[...] = part

                @pl.when(jnp.logical_not(last))
                def _():
                    ob[ap, lo, :] = h
            with SC('post_rows'):
                loop(T // rb, rows)

            @pl.when(is0)
            def _():
                remote(ob.at[ap], ha.at[0, i, own], z_s.at[n], z_r.at[n], (1 - s, r)).start()

            @pl.when(is1 & (kind == 1))
            def _():
                remote(ob.at[ap], ea.at[0, i, own], z_s.at[n], z_r.at[n], (1 - s, r)).start()

            @pl.when(last)
            def _():
                for c in give(ob.at[ap], ea, nm + i, i, False):
                    c.start()
                local(ob.at[ap], ea.at[0, i, own], lsem.at[i]).start()

        j_a = max(0, nj // 2 - 2)
        j_b = j_a + 1
        j_c = min(j_b + 1, nj - 2)
        j_d = nj - 2

        def slot(t):
            kind, i = sched(t)
            ap = t % 2
            more = t + 1 < nm + nm * s

            @pl.when(is0 | (t == 0))
            def _():
                prep_a(t)
                prep_b(t)

            local(ha.at[0, i, own], ab.at[ap, own], alsem.at[ap, 0]).wait()
            local(ha.at[0, i, oth], ab.at[ap, oth], alsem.at[ap, 1]).wait()

            @pl.when(is0)
            def _():
                local(ab.at[ap, own], ha.at[0, i, own], hsem).start()

            def hooks(j):
                late = is1 & (t > 0)

                @pl.when(late & (j == j_a))
                def _():
                    post_a(t - 1)

                @pl.when(late & (j == j_b))
                def _():
                    post_b(t - 1)

                @pl.when(is1 & more & (j == jnp.where(t == 0, j_d, j_c)))
                def _():
                    prep_a(t + 1)

                @pl.when(is1 & more & (j == j_d))
                def _():
                    prep_b(t + 1)

            def run(c1, c2, before, first, second, after):
                c1(0).wait()
                c1(1).start()
                before(0)
                acc[ap] = jnp.zeros((T2, D), F32)
                first(0)
                after(0)

                def step(j):
                    c1(j + 1).wait()
                    c2(j).wait()

                    @pl.when(j + 2 < nj)
                    def _():
                        c1(j + 2).start()
                    c2(j + 1).start()
                    hooks(j)
                    before(j + 1)
                    first(j + 1)
                    acc[ap] += second(j)
                    after(j + 1)
                loop(nj - 1, step)
                c2(nj - 1).wait()

                @pl.when(more)
                def _():
                    c_w1(0).start()
                    c_w2(0).start()
                acc[ap] += second(nj - 1)

            def g_out(j, dst):
                return local(go.at[j % 2], dst.at[i, :, fcols(j)], gsem.at[j % 2])

            def u_out(j):
                return local(uo.at[j % 2], ub.at[i, :, fcols(j)], usem.at[j % 2])

            @pl.when(kind == 0)
            def _():
                def before(j):
                    @pl.when(j >= 2)
                    def _():
                        u_out(j - 2).wait()
                        g_out(j - 2, gb).wait()

                def first(j):
                    for h in (slice(0, T), slice(T, T2)):
                        g, uo[j % 2, h] = gelu_both(dot(ab[ap, h], wb1[j % 2]))
                        go[j % 2, h] = g.astype(BF16)

                def after(j):
                    u_out(j).start()
                    g_out(j, gb).start()
                with SC('slotF'):
                    run(c_w1, c_w2, before, first, lambda j: dot(go[j % 2], wb2[j % 2]), after)
                for j in (nj - 2, nj - 1):
                    u_out(j).wait()
                    g_out(j, gb).wait()

            @pl.when(kind == 1)
            def _():
                def before(j):
                    @pl.when(j >= 2)
                    def _():
                        g_out(j - 2, qb).wait()
                    u_in(i, j).wait()

                    @pl.when(j + 1 < nj)
                    def _():
                        u_in(i, j + 1).start()

                def first(j):
                    p = dot_cols(ab[ap], wb2[j % 2]).astype(BF16)
                    go[j % 2] = (p.astype(F32) * ui[j % 2]).astype(BF16)
                with SC('slotB'):
                    run(c_w2, c_w1, before, first, lambda j: dot_cols(go[j % 2], wb1[j % 2]), lambda j: g_out(j, qb).start())
                for j in (nj - 2, nj - 1):
                    g_out(j, qb).wait()

            @pl.when(is0)
            def _():
                local(ab.at[ap, own], ha.at[0, i, own], hsem).wait()
            exchange(t).start()

            @pl.when(is0 | (t == nt - 1))
            def _():
                post_a(t)
                post_b(t)

        c_w1(0).start()
        c_w2(0).start()
        n_slots = nm + nm * s
        lax.fori_loop(0, n_slots, lambda t, c: (slot(t), c)[1], 0)
        wait_out(n_slots - 2)
        wait_out(n_slots - 1)

    pl.run_scoped(
        phase1,
        VMEM((2, D, fs), BF16), VMEM((2, fs, D), BF16), VMEM((2, T2, D), BF16), VMEM((2, T2, D), F32),
        VMEM((2, T2, fs), F32), VMEM((2, T2, fs), F32), VMEM((2, T2, fs), BF16),
        VMEM((T, D), F32), VMEM((T, D), BF16), VMEM((2, T, D), BF16),
        DMA((2, 2)), DMA((2, 2)), DMA((2,)), DMA((2,)), DMA((2,)), DMA((2,)), DMA((nm,)), DMA,
    )

    def loss_copy(d):
        return remote(lacc, lb.at[r], ls_s.at[d], ls_r.at[r], (d // 8, d % 8))

    def loss_self():
        return local(lacc, lb.at[r], ls_s.at[8 + r])

    @pl.when(is1)
    def _():
        def send(d):
            @pl.when(d != 8 + r)
            def _():
                loss_copy(d).start()
        loop(16, send)
        loss_self().start()

    nc = 4 * nm

    def all_tokens(wq1, wq2, ab, uo, ui, go, qsem, alsem, usem, isem, gsem):
        def c_q1(j):
            return local(w1.at[:, wcols(j, fq)], wq1.at[j], qsem.at[0, j])

        def c_q2(j):
            return local(w2.at[wcols(j, fq), :], wq2.at[j], qsem.at[1, j])
        for j in range(nq):
            c_q1(j).start()

        def arrive(A, n, c, i):
            @pl.when(c == 1)
            def _():
                for h in range(2):
                    with SC('a_c1'):
                        got_half(n_r.at[n, h]).wait_recv()
                remote(A.at[1, i], A.at[2, i], f_s.at[n], f_r.at[n], (s, pr)).start()

            @pl.when(c == 2)
            def _():
                with SC('a_c2'):
                    remote(A.at[1, i], A.at[2, i], f_s.at[n], f_r.at[n], (s, pr)).wait_recv()

            @pl.when(c == 3)
            def _():
                with SC('a_c3'):
                    got_half(x_r.at[n]).wait_recv()
                remote(A.at[3, i, own], A.at[3, i, own], h_s.at[n], h_r.at[n], (s, pr)).start()
                with SC('a_c3b'):
                    got_half(h_r.at[n]).wait_recv()

        def c_ab(A, c, i, v):
            return local(A.at[c, i], ab.at[v % 2], alsem.at[v % 2])

        def block(c, i):
            return pl.ds(pl.multiple_of((c * nm + i) * T2, T2), T2)

        def run(A, at, ready, before, first, outs):
            def load(v):
                c, i = at(v)
                ready(c, i)
                c_ab(A, c, i, v).start()
            load(0)

            def chunk(v):
                c, i = at(v)
                c_ab(A, c, i, v).wait()

                def step(j):
                    g = v * nq + j

                    @pl.when((j == nq - 1) & (v + 1 < nc))
                    def _():
                        load(v + 1)

                    @pl.when(g >= 2)
                    def _():
                        for o in outs(g - 2):
                            o.wait()
                    before(g)
                    first(v, j, g % 2)
                    for o in outs(g):
                        o.start()
                with SC('uchunk'):
                    loop(nq, step)
            loop(nc, chunk)
            for g in (nc * nq - 2, nc * nq - 1):
                for o in outs(g):
                    o.wait()

        def at_h(v):
            return v // nm, v % nm

        def outs_h(g):
            c, i = at_h(g // nq)
            return [local(uo.at[g % 2], ua.at[block(c, i), fcols(g % nq)], usem.at[g % 2]),
                    local(go.at[g % 2], ga.at[block(c, i), fcols(g % nq)], gsem.at[g % 2])]

        def before_h(g):
            @pl.when(g < nq)
            def _():
                c_q1(g).wait()
                c_q2(g).start()

        def first_h(v, j, sl):
            for h in (slice(0, T), slice(T, T2)):
                g, uo[sl, h] = gelu_both(dot(ab[v % 2, h], wq1[j]))
                go[sl, h] = g.astype(BF16)
        run(ha, at_h, lambda c, i: arrive(ha, i, c, i), before_h, first_h, outs_h)

        def at_e(v):
            return v % 4, v // 4

        def outs_e(g):
            c, i = at_e(g // nq)
            return [local(go.at[g % 2], qa.at[block(c, i), fcols(g % nq)], gsem.at[g % 2])]

        def u_in(g):
            c, i = at_e(g // nq)
            return local(ua.at[block(c, i), fcols(g % nq)], ui.at[g % 2], isem.at[g % 2])

        def before_e(g):
            @pl.when(g < nq)
            def _():
                c_q2(g).wait()
            u_in(g).wait()

            @pl.when(g + 1 < nc * nq)
            def _():
                u_in(g + 1).start()

        def ready_e(c, i):
            n = nm + i

            @pl.when(c == 0)
            def _():
                with SC('a_z'):
                    got_half(z_r.at[n]).wait_recv()
                for cp in give(ea.at[0, i, own], ea, n, i, True):
                    cp.start()
                with SC('a_d'):
                    got_half(d_r.at[n]).wait_recv()
            arrive(ea, n, c, i)

        def first_e(v, j, sl):
            p = dot_cols(ab[v % 2], wq2[j]).astype(BF16)
            go[sl] = (p.astype(F32) * ui[sl]).astype(BF16)
        u_in(0).start()
        run(ea, at_e, ready_e, before_e, first_e, outs_e)

    def sums0(hv, bv, o, tb, tsem, bsem, osem):
        nw = 4 * nq

        def at(w):
            return w // (2 * nq), (w // 2) % nq, w % 2

        def load(w):
            _, j, q = at(w)
            for qq, A in ((0, qa), (1, ga)):
                @pl.when(q == qq)
                def _():
                    local(A.at[:, fcols(j)], bv.at[w % 2], bsem.at[w % 2]).start()

        def far(w, q, m):
            j = at(w)[1]
            return remote(pb.at[q, j, 2 + m], (m1, m2)[q].at[:, wcols(j, fq)], pe_s.at[q, m, j], pe_r.at[q, k, j], (s, nb - k + m))

        def near(w, q):
            j = at(w)[1]
            return remote(pb.at[q, j, 1 - k], (m1, m2)[q].at[:, wcols(j, fq)], ms_s.at[q, j], ms_r.at[q, j], (s, pr))

        def ship(w):
            ps, j, q = at(w)
            for qq in range(2):
                @pl.when(q == qq)
                def _():
                    for m in range(2):
                        local(o.at[qq, m], pb.at[qq, j, m], osem.at[qq, m]).wait()

                    @pl.when(ps == 0)
                    def _():
                        for m in range(2):
                            far(w, qq, m).start()

                    @pl.when(ps == 1)
                    def _():
                        near(w, qq).start()

        def one(ps):
            cols = pl.ds(pl.multiple_of((nb // 2) * dq * (1 - ps) + (r // 2) * dq * ps, 128), dq)
            for qq, A in ((0, ha), (1, ea)):
                def c_t(v):
                    return local(A.at[v // nm, v % nm, :, cols], tb.at[v % 2], tsem.at[v % 2])
                c_t(0).start()

                def build(v):
                    c_t(v).wait()

                    @pl.when(v + 1 < nc)
                    def _():
                        c_t(v + 1).start()
                    hv[qq, :, pl.ds(pl.multiple_of(v * T2, T2), T2)] = tb[v % 2].T
                with SC('build0'):
                    loop(nc, build)

            def unit(ww):
                w = ps * 2 * nq + ww
                _, j, q = at(w)
                local(qa.at[:, fcols(j)], bv.at[w % 2], bsem.at[w % 2]).wait()

                @pl.when(w + 1 < nw)
                def _():
                    load(w + 1)

                @pl.when(w >= 1)
                def _():
                    ship(w - 1)

                def grads(m):
                    rows = pl.ds(pl.multiple_of(m * dr, dr), dr)
                    o[q, m] = dot(hv[q, rows, :], bv[w % 2])
                    for qq, M in ((0, m1), (1, m2)):
                        here = (ps == 1) & (m == k)

                        @pl.when((q == qq) & here)
                        def _():
                            local(o.at[qq, m], M.at[:, wcols(j, fq)], osem.at[qq, m]).start()

                        @pl.when((q == qq) & jnp.logical_not(here))
                        def _():
                            local(o.at[qq, m], pb.at[qq, j, 2 * (1 - ps) + m], osem.at[qq, m]).start()
                with SC('grads0'):
                    loop(2, grads)
            loop(2 * nq, unit)
        load(0)
        loop(2, one)
        ship(nw - 1)

        def finish(j):
            w = 2 * j
            for q in range(2):
                near(w, q).wait()
                for m in range(2):
                    far(w, q, m).wait_send()
                    remote(pb.at[q, j, 0], (m1, m2)[q].at[:, wcols(j, fq)], ms_s.at[q, j], pe_r.at[q, m, j], (s, pr)).wait_recv()
        with SC('finish0'):
            loop(nq, finish)

    def sums1(wb1, wb2, ht, et, gv, qv, a, b, o, tb, dv, wsem, tsem, asem, gqsem, osem):
        def weights(j):
            return (local(w1.at[:, wcols(j, fb)], wb1.at[j % 2], wsem.at[0, j % 2]),
                    local(w2.at[wcols(j, fb), :], wb2.at[j % 2], wsem.at[1, j % 2]))

        def stream(v):
            i, sl = v % nm, v % 2
            return (local(ha.at[1, i], a.at[sl], asem.at[0, sl]), local(ea.at[1, i], b.at[sl], asem.at[1, sl]))

        def saved(j, i):
            rows = pl.ds(pl.multiple_of(i * T2, T2), T2)
            return (local(gb.at[i, :, fcols(j)], gv.at[rows], gqsem.at[0, i]),
                    local(qb.at[i, :, fcols(j)], qv.at[rows], gqsem.at[1, i]))

        for c in weights(0):
            c.start()

        cols = (chip_cols(r), chip_cols(pe))
        for q, A, dst in ((0, ha, ht), (1, ea, et)):
            def c_t(v):
                return [local(A.at[v // nm, v % nm, :, cols[c]], tb.at[v % 2, c], tsem.at[v % 2, c]) for c in range(2)]

            def start(v):
                @pl.when(v >= nm)
                def _():
                    for h in range(2):
                        got_half(n_r.at[q * nm + v - nm, h]).wait_recv()
                for c in c_t(v):
                    c.start()
            start(0)

            def build(v):
                for c in c_t(v):
                    c.wait()

                @pl.when(v + 1 < 2 * nm)
                def _():
                    start(v + 1)
                for c in range(2):
                    dst[c * dq:(c + 1) * dq, pl.ds(pl.multiple_of(v * T2, T2), T2)] = tb[v % 2, c].T
            with SC('build1'):
                loop(2 * nm, build)

        for c in stream(0):
            c.start()

        def kept(q, j, m):
            mine = local(o.at[q, m], (m1, m2)[q].at[:, wcols(j, fb)], osem.at[q, m])
            rest = local(o.at[q, m], pb.at[q, j, m], osem.at[q, m])
            return mine, rest

        def sends(j):
            cs = wcols(j, fb)
            out = []
            for q in range(2):
                for c in range(2):
                    out.append(remote(pb.at[q, j, 2 + c], (r1, r2)[q].at[:, cs], pe_s.at[q, c, j], pe_r.at[q, k, j], (s, pe - k + c)))
                out.append(remote(pb.at[q, j, 1 - k], (m1, m2)[q].at[:, cs], ms_s.at[q, j], ms_r.at[q, j], (s, pr)))
            return out

        def ship(j):
            for q in range(2):
                loop(4, lambda m: kept(q, j, m)[1].wait())
            for c in sends(j):
                c.start()

        def part(j):
            ws = j % 2
            loop(nm, lambda i: [c.start() for c in saved(j, i)])
            for c in weights(j):
                c.wait()

            @pl.when(j + 1 < nj)
            def _():
                for c in weights(j + 1):
                    c.start()

            @pl.when(j >= 1)
            def _():
                ship(j - 1)

            def again(i):
                v = j * nm + i
                sl = v % 2
                for c in stream(v):
                    c.wait()

                @pl.when(v + 1 < nj * nm)
                def _():
                    for c in stream(v + 1):
                        c.start()
                rows = pl.ds(pl.multiple_of((nm + i) * T2, T2), T2)
                for h in range(2):
                    part_rows = pl.ds(pl.multiple_of((nm + i) * T2 + h * T, T), T)
                    g, dv[h * T:(h + 1) * T] = gelu_both(dot(a[sl, h * T:(h + 1) * T], wb1[ws]))
                    gv[part_rows, :] = g.astype(BF16)
                p = dot_cols(b[sl], wb2[ws]).astype(BF16)
                qv[rows, :] = (p.astype(F32) * dv[...]).astype(BF16)
            with SC('again'):
                loop(nm, again)
            loop(nm, lambda i: [c.wait() for c in saved(j, i)])

            def grads(m):
                rows = pl.ds(pl.multiple_of(m * dr, dr), dr)
                o[0, m] = dot(ht[rows, :], qv[...])
                o[1, m] = dot(et[rows, :], gv[...])
                for q in range(2):
                    mine, rest = kept(q, j, m)

                    @pl.when(m == k)
                    def _():
                        mine.start()

                    @pl.when(m != k)
                    def _():
                        rest.start()
            with SC('grads1'):
                loop(4, grads)
        loop(nj, part)
        ship(nj - 1)

        def finish(j):
            for c in sends(j):
                c.wait_send()
            for q in range(2):
                remote(pb.at[q, j, 0], (m1, m2)[q].at[:, wcols(j, fb)], ms_s.at[q, j], ms_r.at[q, j], (s, pr)).wait_recv()
                for c in range(2):
                    remote(pb.at[q, j, 0], (r1, r2)[q].at[:, wcols(j, fb)], ms_s.at[q, j], pe_r.at[q, c, j], (s, pr)).wait_recv()
        with SC('finish1'):
            loop(nj, finish)

    nr = 2 * nm * T2

    @pl.when(is0)
    def _():
        pl.run_scoped(
            all_tokens,
            VMEM((nq, D, fs), BF16), VMEM((nq, fs, D), BF16), VMEM((2, T2, D), BF16),
            VMEM((2, T2, fs), F32), VMEM((2, T2, fs), F32), VMEM((2, T2, fs), BF16),
            DMA((2, nq)), DMA((2,)), DMA((2,)), DMA((2,)), DMA((2,)),
        )
        pl.run_scoped(
            sums0,
            VMEM((2, dq, 2 * nr), BF16), VMEM((2, 2 * nr, fs), BF16), VMEM((2, 2, dr, fs), F32), VMEM((2, T2, dq), BF16),
            DMA((2,)), DMA((2,)), DMA((2, 2)),
        )

    @pl.when(is1)
    def _():
        pl.run_scoped(
            sums1,
            VMEM((2, D, fs), BF16), VMEM((2, fs, D), BF16),
            VMEM((2 * dq, nr), BF16), VMEM((2 * dq, nr), BF16), VMEM((nr, fs), BF16), VMEM((nr, fs), BF16),
            VMEM((2, T2, D), BF16), VMEM((2, T2, D), BF16), VMEM((2, 4, dr, fs), F32), VMEM((2, 2, T2, dq), BF16), VMEM((T2, fs), F32),
            DMA((2, 2)), DMA((2, 2)), DMA((2, 2)), DMA((2, nm)), DMA((2, 4)),
        )

    def settle(n):
        A = ha

        @pl.when(is0 | (n < nm))
        def _():
            for c in give(A.at[0, 0, own], A, n, 0, False):
                c.wait_send()

        @pl.when(is0)
        def _():
            remote(A.at[3, 0, own], A.at[3, 0, own], x_s.at[n], x_r.at[n], (s, dg)).wait_send()
            remote(A.at[3, 0, own], A.at[3, 0, own], h_s.at[n], h_r.at[n], (s, pr)).wait_send()
            remote(A.at[1, 0], A.at[2, 0], f_s.at[n], f_r.at[n], (s, pr)).wait_send()
    with SC('settle'):
        loop(nt, settle)

    @pl.when(is1)
    def _():
        def sent(d):
            @pl.when(d != 8 + r)
            def _():
                loss_copy(d).wait_send()
        loop(16, sent)
        loss_self().wait()

    def got(n):
        @pl.when(is0 | (n != r))
        def _():
            remote(lacc, lb.at[n], ls_s.at[n], ls_r.at[n], (s, r)).wait_recv()
    loop(8, got)


def solution(mesh):
    n_data = mesh.shape['data']

    def per_device(inputs, targets, w_up, w_down):
        nm, T, D = inputs.shape
        F = w_up.shape[2]
        Fk = F // 2
        fs = min(512, Fk // 4)
        nj = Fk // fs
        dr = D // 8
        inv = 1.0 / (n_data * nm * T)
        dims = (nm, T, D, Fk, fs, inv)
        sd = jax.ShapeDtypeStruct
        rows = 4 * nm * 2 * T
        out_shape = [
            sd((dr, F), F32), sd((dr, F), F32), sd((dr, F), F32), sd((dr, F), F32), sd((8, 8, 128), F32),
            sd((4, nm, 2 * T, D), BF16), sd((4, nm, 2 * T, D), BF16),
            sd((nm, 2 * T, Fk), F32), sd((nm, 2 * T, Fk), BF16), sd((nm, 2 * T, Fk), BF16),
            sd((rows, Fk // 2), F32), sd((rows, Fk // 2), BF16), sd((rows, Fk // 2), BF16),
            sd((2 * nm, T, D), F32), sd((2, nj, 4, dr, fs), F32),
        ]
        any_spec = pl.BlockSpec(memory_space=pl.ANY)
        n2 = 2 * nm
        outs = pl.pallas_call(
            functools.partial(kernel, dims),
            out_shape=out_shape,
            in_specs=[any_spec] * 4,
            out_specs=[any_spec] * len(out_shape),
            scratch_shapes=[
                VMEM((8, 128), F32),
                DMA((n2,)), DMA((n2,)), DMA((n2,)), DMA((n2,)), DMA((n2,)), DMA((n2,)), DMA((n2, 2)), DMA((n2, 2)),
                DMA((n2,)), DMA((n2,)), DMA((n2,)), DMA((n2,)), DMA((n2,)), DMA((n2,)),
                DMA((2, nj)), DMA((2, nj)), DMA((2, 2, nj)), DMA((2, 2, nj)), DMA((16,)), DMA((8,)),
            ],
            compiler_params=pltpu.CompilerParams(has_side_effects=True, vmem_limit_bytes=67_000_000),
            cost_estimate=pl.CostEstimate(flops=16 * nm * T * D * F, bytes_accessed=10**9, transcendentals=0),
            name='train_step',
        )(inputs, targets, w_up.reshape(D, F), w_down.reshape(F, D))
        m1, r1, m2, r2, lb = outs[:5]
        loss = jnp.sum(lb) * (0.5 * inv)
        whole = lax.axis_index('stage') == 0
        up = jnp.where(whole, m1, m1 + r1)
        down = jnp.where(whole, m2, m2 + r2)
        return loss, up[None], down.T[None]

    return jax.shard_map(per_device, mesh=mesh, in_specs=(P('data', None, None), P('data', None, None), P('stage', None, None), P('stage', None, None)), out_specs=(P(), P('stage', 'data', None), P('stage', None, 'data')), check_vma=False)
```

```python
import functools
import math

import jax
import jax.numpy as jnp
from jax import lax
from jax.experimental import pallas as pl
from jax.experimental.pallas import tpu as pltpu
from jax.sharding import PartitionSpec as P

F32 = jnp.float32
BF16 = jnp.bfloat16
MESH = pl.DeviceIdType.MESH
SC = jax.named_scope
COLS = (((1,), (1,)), ((), ()))
GC = math.sqrt(2.0 / math.pi)
DMA = pltpu.SemaphoreType.DMA
VMEM = pltpu.VMEM


def dot(a, b):
    return jnp.dot(a, b, preferred_element_type=F32)


def dot_cols(a, b):
    return lax.dot_general(a, b, COLS, preferred_element_type=F32)


def gelu_both(u):
    u2 = u * u
    t = jnp.tanh(GC * (u + 0.044715 * (u2 * u)))
    half = 0.5 * (1.0 + t)
    return u * half, half + (0.5 * u) * (1.0 - t * t) * (GC + (3.0 * 0.044715 * GC) * u2)


def loop(n, body):
    lax.fori_loop(0, n, lambda i, c: (body(i), c)[1], 0)


def local(src, dst, sem):
    return pltpu.make_async_copy(src, dst, sem)


def remote(src, dst, ss, rs, dev):
    return pltpu.make_async_remote_copy(src_ref=src, dst_ref=dst, send_sem=ss, recv_sem=rs, device_id=dev, device_id_type=MESH)


def kernel(dims, x, y, w1, w2, m1, r1, m2, r2, lb, ha, ea, ub, gb, qb, ua, ga, qa, vx, pb,
           lacc, ob, z_s, z_r, d_s, d_r, v_s, v_r, n_s, n_r, x_s, x_r, f_s, f_r, h_s, h_r, ms_s, ms_r, pe_s, pe_r, ls_s, ls_r):
    nm, T, D, Fk, fs, inv = dims
    nj = Fk // fs
    nq = nj // 2
    nt = 2 * nm
    T2 = 2 * T
    dq, dr = D // 4, D // 8
    s = lax.axis_index('stage')
    r = lax.axis_index('data')
    k = r % 2
    xb = (r // 2) % 2
    yb_ = r // 4
    pr = r + 1 - 2 * k
    fx = r + 2 - 4 * xb
    fy = r + 4 - 8 * yb_
    dg = fy + 2 - 4 * xb
    ry, rx = fy - k, fx - k + 1
    nb = fy * (1 - k) + fx * k
    pe = fx * (1 - k) + fy * k
    fb = k * Fk
    q0 = (yb_ * (1 - k) + xb * k) * nq
    fq = fb + q0 * fs
    own = pl.ds(pl.multiple_of(k * T, T), T)
    oth = pl.ds(pl.multiple_of((1 - k) * T, T), T)
    is0, is1 = s == 0, s == 1

    def fcols(j):
        return pl.ds(pl.multiple_of(j * fs, fs), fs)

    def wcols(j, base):
        return pl.ds(pl.multiple_of(base + j * fs, fs), fs)

    def chip_cols(dev):
        return pl.ds(pl.multiple_of((dev // 2) * dq, 128), dq)

    def give(src, A, n, i, far):
        out = [
            remote(src, A.at[0, i, own], d_s.at[n], d_r.at[n], (s, pr)),
            remote(src, A.at[1, i, own], n_s.at[n, 0], n_r.at[n, k], (s, ry)),
            remote(src, A.at[1, i, own], n_s.at[n, 1], n_r.at[n, k], (s, rx)),
        ]
        if far:
            out.append(remote(src, A.at[3, i, own], x_s.at[n], x_r.at[n], (s, dg)))
        return out

    def got_half(sem):
        return remote(ha.at[0, 0, own], ha.at[0, 0, oth], x_s.at[0], sem, (s, pr))

    @pl.when(is0)
    def _():
        for i in range(nm):
            for c in give(x.at[i], ha, i, i, True):
                c.start()

    def phase1(wb1, wb2, ab, acc, uo, ui, go, tmp, yb, wsem, alsem, usem, isem, gsem, psem, lsem, hsem):
        lacc[...] = jnp.zeros_like(lacc)

        def sched(t):
            mid = (t > 0) & (t < nt - 1)
            kind1 = jnp.where(mid, (t + 1) % 2, jnp.where(t == 0, 0, 1))
            i1 = jnp.where(mid, jnp.where(t % 2 == 1, (t + 1) // 2, (t - 2) // 2), jnp.where(t == 0, 0, nm - 1))
            return jnp.where(is1, kind1, 0), jnp.where(is1, i1, t)

        def c_w1(j):
            return local(w1.at[:, wcols(j, fb)], wb1.at[j % 2], wsem.at[0, j % 2])

        def c_w2(j):
            return local(w2.at[wcols(j, fb), :], wb2.at[j % 2], wsem.at[1, j % 2])

        def prep_a(t):
            kind, i = sched(t)

            @pl.when(is1 & (kind == 0))
            def _():
                with SC('w_z_h'):
                    got_half(z_r.at[i]).wait_recv()
                for c in give(ha.at[0, i, own], ha, i, i, False):
                    c.start()

        def u_in(i, j):
            return local(ub.at[i, :, fcols(j)], ui.at[j % 2], isem.at[j % 2])

        def prep_b(t):
            kind, i = sched(t)
            ap = t % 2
            for kk, A in ((0, ha), (1, ea)):
                @pl.when(kind == kk)
                def _():
                    with SC('w_d'):
                        got_half(d_r.at[kk * nm + i]).wait_recv()
                    if kk == 1:
                        local(ob.at[0], ea.at[0, i, own], lsem.at[i]).wait()
                        u_in(i, 0).start()
                    if kk == 0:
                        @pl.when(is0)
                        def _():
                            local(x.at[i], ab.at[ap, own], alsem.at[ap, 0]).start()

                    @pl.when(is1)
                    def _():
                        local(A.at[0, i, own], ab.at[ap, own], alsem.at[ap, 0]).start()
                    local(A.at[0, i, oth], ab.at[ap, oth], alsem.at[ap, 1]).start()

        def exchange(t):
            kind, i = sched(t)
            n = kind * nm + i
            return remote(acc.at[t % 2, oth], vx.at[n], v_s.at[n], v_r.at[n], (s, pr))

        def wait_out(t):
            kind, i = sched(t)

            @pl.when(is0 | (kind == 1))
            def _():
                n = kind * nm + i
                remote(ob.at[0], ea.at[0, i, own], z_s.at[n], z_r.at[n], (1 - s, r)).wait_send()

            @pl.when(is1 & (kind == 0))
            def _():
                for c in give(ob.at[0], ea, nm + i, i, False):
                    c.wait_send()

        def post_a(t):
            kind, i = sched(t)
            with SC('w_exch'):
                exchange(t).wait()
            local(vx.at[kind * nm + i], tmp, psem.at[0]).start()
            local(y.at[i], yb, psem.at[1]).start()

        def post_b(t):
            kind, i = sched(t)
            n = kind * nm + i
            ap = t % 2

            @pl.when(t >= 2)
            def _():
                with SC('w_out'):
                    wait_out(t - 2)
            local(vx.at[n], tmp, psem.at[0]).wait()
            local(y.at[i], yb, psem.at[1]).wait()
            last = is1 & (kind == 0)
            rb = min(64, T)

            def rows(b):
                lo = pl.ds(pl.multiple_of(b * rb, rb), rb)
                mine = pl.ds(pl.multiple_of(k * T + b * rb, rb), rb)
                h = (ab[ap, mine, :].astype(F32) + (acc[ap, mine, :] + tmp[lo, :])).astype(BF16)

                @pl.when(last)
                def _():
                    d = h.astype(F32) - yb[lo, :].astype(F32)
                    ob[ap, lo, :] = (d * inv).astype(BF16)
                    sq = jnp.sum((d * d).reshape(rb // 8, 8, D), axis=0)
                    part = lacc[...]
                    for c in range(D // 128):
                        part = part + sq[:, c * 128:(c + 1) * 128]
                    lacc[...] = part

                @pl.when(jnp.logical_not(last))
                def _():
                    ob[ap, lo, :] = h
            with SC('post_rows'):
                loop(T // rb, rows)

            @pl.when(is0)
            def _():
                remote(ob.at[ap], ha.at[0, i, own], z_s.at[n], z_r.at[n], (1 - s, r)).start()

            @pl.when(is1 & (kind == 1))
            def _():
                remote(ob.at[ap], ea.at[0, i, own], z_s.at[n], z_r.at[n], (1 - s, r)).start()

            @pl.when(last)
            def _():
                for c in give(ob.at[ap], ea, nm + i, i, False):
                    c.start()
                local(ob.at[ap], ea.at[0, i, own], lsem.at[i]).start()

        j_a = max(0, nj // 2 - 2)
        j_b = j_a + 1
        j_c = min(j_b + 1, nj - 2)
        j_d = nj - 2

        def slot(t):
            kind, i = sched(t)
            ap = t % 2
            more = t + 1 < nm + nm * s

            @pl.when(is0 | (t == 0))
            def _():
                prep_a(t)
                prep_b(t)

            local(ha.at[0, i, own], ab.at[ap, own], alsem.at[ap, 0]).wait()
            local(ha.at[0, i, oth], ab.at[ap, oth], alsem.at[ap, 1]).wait()

            @pl.when(is0)
            def _():
                local(ab.at[ap, own], ha.at[0, i, own], hsem).start()

            def hooks(j):
                late = is1 & (t > 0)

                @pl.when(late & (j == j_a))
                def _():
                    post_a(t - 1)

                @pl.when(late & (j == j_b))
                def _():
                    post_b(t - 1)

                @pl.when(is1 & more & (j == jnp.where(t == 0, j_d, j_c)))
                def _():
                    prep_a(t + 1)

                @pl.when(is1 & more & (j == j_d))
                def _():
                    prep_b(t + 1)

            def run(c1, c2, before, first, second, after):
                c1(0).wait()
                c1(1).start()
                before(0)
                acc[ap] = jnp.zeros((T2, D), F32)
                first(0)
                after(0)

                def step(j):
                    c1(j + 1).wait()
                    c2(j).wait()

                    @pl.when(j + 2 < nj)
                    def _():
                        c1(j + 2).start()
                    c2(j + 1).start()
                    hooks(j)
                    before(j + 1)
                    first(j + 1)
                    acc[ap] += second(j)
                    after(j + 1)
                loop(nj - 1, step)
                c2(nj - 1).wait()

                @pl.when(more)
                def _():
                    c_w1(0).start()
                    c_w2(0).start()
                acc[ap] += second(nj - 1)

            def g_out(j, dst):
                return local(go.at[j % 2], dst.at[i, :, fcols(j)], gsem.at[j % 2])

            def u_out(j):
                return local(uo.at[j % 2], ub.at[i, :, fcols(j)], usem.at[j % 2])

            def mine(j):
                return (j >= q0) & (j < q0 + nq)

            def keep(j):
                @pl.when(is1)
                def _():
                    u_out(j).start()
                    g_out(j, gb).start()

                @pl.when(is0 & mine(j))
                def _():
                    rows = pl.ds(pl.multiple_of(i * T2, T2), T2)
                    local(uo.at[j % 2], ua.at[rows, fcols(j - q0)], usem.at[j % 2]).start()
                    local(go.at[j % 2], ga.at[rows, fcols(j - q0)], gsem.at[j % 2]).start()

            def kept(j):
                @pl.when(is1 | mine(j))
                def _():
                    u_out(j).wait()
                    g_out(j, gb).wait()

            @pl.when(kind == 0)
            def _():
                def before(j):
                    @pl.when(j >= 2)
                    def _():
                        kept(j - 2)

                def first(j):
                    for h in (slice(0, T), slice(T, T2)):
                        g, uo[j % 2, h] = gelu_both(dot(ab[ap, h], wb1[j % 2]))
                        go[j % 2, h] = g.astype(BF16)

                with SC('slotF'):
                    run(c_w1, c_w2, before, first, lambda j: dot(go[j % 2], wb2[j % 2]), keep)
                for j in (nj - 2, nj - 1):
                    kept(j)

            @pl.when(kind == 1)
            def _():
                def before(j):
                    @pl.when(j >= 2)
                    def _():
                        g_out(j - 2, qb).wait()
                    u_in(i, j).wait()

                    @pl.when(j + 1 < nj)
                    def _():
                        u_in(i, j + 1).start()

                def first(j):
                    p = dot_cols(ab[ap], wb2[j % 2]).astype(BF16)
                    go[j % 2] = (p.astype(F32) * ui[j % 2]).astype(BF16)
                with SC('slotB'):
                    run(c_w2, c_w1, before, first, lambda j: dot_cols(go[j % 2], wb1[j % 2]), lambda j: g_out(j, qb).start())
                for j in (nj - 2, nj - 1):
                    g_out(j, qb).wait()

            @pl.when(is0)
            def _():
                local(ab.at[ap, own], ha.at[0, i, own], hsem).wait()
            exchange(t).start()

            @pl.when(is0 | (t == nt - 1))
            def _():
                post_a(t)
                post_b(t)

        c_w1(0).start()
        c_w2(0).start()
        n_slots = nm + nm * s
        lax.fori_loop(0, n_slots, lambda t, c: (slot(t), c)[1], 0)

    pl.run_scoped(
        phase1,
        VMEM((2, D, fs), BF16), VMEM((2, fs, D), BF16), VMEM((2, T2, D), BF16), VMEM((2, T2, D), F32),
        VMEM((2, T2, fs), F32), VMEM((2, T2, fs), F32), VMEM((2, T2, fs), BF16),
        VMEM((T, D), F32), VMEM((T, D), BF16),
        DMA((2, 2)), DMA((2, 2)), DMA((2,)), DMA((2,)), DMA((2,)), DMA((2,)), DMA((nm,)), DMA,
    )

    def loss_copy(d):
        return remote(lacc, lb.at[r], ls_s.at[d], ls_r.at[r], (d // 8, d % 8))

    def loss_self():
        return local(lacc, lb.at[r], ls_s.at[8 + r])

    @pl.when(is1)
    def _():
        def send(d):
            @pl.when(d != 8 + r)
            def _():
                loss_copy(d).start()
        loop(16, send)
        loss_self().start()

    nc = 4 * nm

    def all_tokens(wq1, wq2, ab, uo, ui, go, qsem, alsem, usem, isem, gsem):
        def c_q1(j):
            return local(w1.at[:, wcols(j, fq)], wq1.at[j], qsem.at[0, j])

        def c_q2(j):
            return local(w2.at[wcols(j, fq), :], wq2.at[j], qsem.at[1, j])
        for j in range(nq):
            c_q1(j).start()

        def arrive(A, n, c, i):
            @pl.when(c == 1)
            def _():
                for h in range(2):
                    with SC('a_c1'):
                        got_half(n_r.at[n, h]).wait_recv()
                remote(A.at[1, i], A.at[2, i], f_s.at[n], f_r.at[n], (s, pr)).start()

            @pl.when(c == 2)
            def _():
                with SC('a_c2'):
                    remote(A.at[1, i], A.at[2, i], f_s.at[n], f_r.at[n], (s, pr)).wait_recv()

            @pl.when(c == 3)
            def _():
                with SC('a_c3'):
                    got_half(x_r.at[n]).wait_recv()
                remote(A.at[3, i, own], A.at[3, i, own], h_s.at[n], h_r.at[n], (s, pr)).start()
                with SC('a_c3b'):
                    got_half(h_r.at[n]).wait_recv()

        def c_ab(A, c, i, v):
            return local(A.at[c, i], ab.at[v % 2], alsem.at[v % 2])

        def block(c, i):
            return pl.ds(pl.multiple_of((c * nm + i) * T2, T2), T2)

        def pass_on(i):
            n = nm + i
            with SC('a_z'):
                got_half(z_r.at[n]).wait_recv()
            for cp in give(ea.at[0, i, own], ea, n, i, True):
                cp.start()

        def run(nc, A, at, ready, before, first, outs):
            def load(v):
                c, i = at(v)
                ready(c, i)
                c_ab(A, c, i, v).start()
            load(0)

            def chunk(v):
                c, i = at(v)
                c_ab(A, c, i, v).wait()

                def step(j):
                    g = v * nq + j

                    @pl.when((j == nq - 2) & (v + 1 < nc))
                    def _():
                        load(v + 1)

                    @pl.when(g >= 2)
                    def _():
                        for o in outs(g - 2):
                            o.wait()
                    before(g)
                    first(v, j, g % 2)
                    for o in outs(g):
                        o.start()
                with SC('uchunk'):
                    loop(nq, step)
            loop(nc, chunk)
            for g in (nc * nq - 2, nc * nq - 1):
                for o in outs(g):
                    o.wait()

        def at_h(v):
            return 1 + v // nm, v % nm

        def outs_h(g):
            c, i = at_h(g // nq)
            return [local(uo.at[g % 2], ua.at[block(c, i), fcols(g % nq)], usem.at[g % 2]),
                    local(go.at[g % 2], ga.at[block(c, i), fcols(g % nq)], gsem.at[g % 2])]

        def before_h(g):
            @pl.when(g < nq)
            def _():
                c_q1(g).wait()
                c_q2(g).start()

        def first_h(v, j, sl):
            for h in (slice(0, T), slice(T, T2)):
                g, uo[sl, h] = gelu_both(dot(ab[v % 2, h], wq1[j]))
                go[sl, h] = g.astype(BF16)

        def ready_h(c, i):
            @pl.when((c == 2) & (i == nm // 2))
            def _():
                pass_on(0)
            arrive(ha, i, c, i)
        run(3 * nm, ha, at_h, ready_h, before_h, first_h, outs_h)

        def at_e(v):
            return v % 4, v // 4

        def outs_e(g):
            c, i = at_e(g // nq)
            return [local(go.at[g % 2], qa.at[block(c, i), fcols(g % nq)], gsem.at[g % 2])]

        def u_in(g):
            c, i = at_e(g // nq)
            return local(ua.at[block(c, i), fcols(g % nq)], ui.at[g % 4], isem.at[g % 4])

        def before_e(g):
            @pl.when(g < nq)
            def _():
                c_q2(g).wait()
            u_in(g).wait()

            @pl.when(g + 3 < nc * nq)
            def _():
                u_in(g + 3).start()

        def ready_e(c, i):
            n = nm + i

            @pl.when(c == 0)
            def _():
                with SC('a_d'):
                    got_half(d_r.at[n]).wait_recv()
            arrive(ea, n, c, i)

            @pl.when((c == 1) & (i + 1 < nm))
            def _():
                pass_on(i + 1)

        def first_e(v, j, sl):
            p = dot_cols(ab[v % 2], wq2[j]).astype(BF16)
            go[sl] = (p.astype(F32) * ui[(v * nq + j) % 4]).astype(BF16)
        for g in range(3):
            u_in(g).start()
        run(nc, ea, at_e, ready_e, before_e, first_e, outs_e)

    def sums0(hv, bv, o, tb, tsem, bsem, osem):
        nw = 4 * nq

        def at(w):
            return w // (2 * nq), (w // 2) % nq, w % 2

        def load(w):
            _, j, q = at(w)
            for qq, A in ((0, qa), (1, ga)):
                @pl.when(q == qq)
                def _():
                    local(A.at[:, fcols(j)], bv.at[w % 2], bsem.at[w % 2]).start()

        def far(w, q, m):
            j = at(w)[1]
            return remote(pb.at[q, j, 2 + m], (m1, m2)[q].at[:, wcols(j, fq)], pe_s.at[q, m, j], pe_r.at[q, k, j], (s, nb - k + m))

        def near(w, q):
            j = at(w)[1]
            return remote(pb.at[q, j, 1 - k], (m1, m2)[q].at[:, wcols(j, fq)], ms_s.at[q, j], ms_r.at[q, j], (s, pr))

        def ship(w):
            ps, j, q = at(w)
            for qq in range(2):
                @pl.when(q == qq)
                def _():
                    for m in range(2):
                        local(o.at[qq, m], pb.at[qq, j, m], osem.at[qq, m]).wait()

                    @pl.when(ps == 0)
                    def _():
                        for m in range(2):
                            far(w, qq, m).start()

                    @pl.when(ps == 1)
                    def _():
                        near(w, qq).start()

        def one(ps):
            cols = pl.ds(pl.multiple_of((nb // 2) * dq * (1 - ps) + (r // 2) * dq * ps, 128), dq)
            for qq, A in ((0, ha), (1, ea)):
                def c_t(v):
                    return local(A.at[v // nm, v % nm, :, cols], tb.at[v % 8], tsem.at[v % 8])
                for v in range(7):
                    c_t(v).start()

                def build(v):
                    c_t(v).wait()

                    @pl.when(v + 7 < nc)
                    def _():
                        c_t(v + 7).start()
                    hv[qq, :, pl.ds(pl.multiple_of(v * T2, T2), T2)] = tb[v % 8].T
                with SC('build0'):
                    loop(nc, build)

            def unit(ww):
                w = ps * 2 * nq + ww
                _, j, q = at(w)
                local(qa.at[:, fcols(j)], bv.at[w % 2], bsem.at[w % 2]).wait()

                @pl.when(w + 1 < nw)
                def _():
                    load(w + 1)

                def grads(m):
                    rows = pl.ds(pl.multiple_of(m * dr, dr), dr)

                    @pl.when((w >= 1) & (m == 1))
                    def _():
                        ship(w - 1)
                    o[q, m] = dot(hv[q, rows, :], bv[w % 2])
                    for qq, M in ((0, m1), (1, m2)):
                        here = (ps == 1) & (m == k)

                        @pl.when((q == qq) & here)
                        def _():
                            local(o.at[qq, m], M.at[:, wcols(j, fq)], osem.at[qq, m]).start()

                        @pl.when((q == qq) & jnp.logical_not(here))
                        def _():
                            local(o.at[qq, m], pb.at[qq, j, 2 * (1 - ps) + m], osem.at[qq, m]).start()
                with SC('grads0'):
                    loop(2, grads)
            loop(2 * nq, unit)
        load(0)
        loop(2, one)
        ship(nw - 1)

        def finish(j):
            w = 2 * j
            for q in range(2):
                near(w, q).wait()
                for m in range(2):
                    far(w, q, m).wait_send()
                    remote(pb.at[q, j, 0], (m1, m2)[q].at[:, wcols(j, fq)], ms_s.at[q, j], pe_r.at[q, m, j], (s, pr)).wait_recv()
        with SC('finish0'):
            loop(nq, finish)

    def sums1(wb1, wb2, ht, et, gv, qv, ab, o, dv, wsem, tsem, asem, gqsem, osem):
        def weights(j):
            return (local(w1.at[:, wcols(j, fb)], wb1.at[j % 2], wsem.at[0, j % 2]),
                    local(w2.at[wcols(j, fb), :], wb2.at[j % 2], wsem.at[1, j % 2]))

        def stream(v):
            i, sl = v % nm, v % 2
            return (local(ha.at[1, i], ab.at[sl], asem.at[0, sl]), local(ea.at[1, i], ab.at[2 + sl], asem.at[1, sl]))

        def saved(j, i):
            rows = pl.ds(pl.multiple_of(i * T2, T2), T2)
            return (local(gb.at[i, :, fcols(j)], gv.at[rows], gqsem.at[0, i]),
                    local(qb.at[i, :, fcols(j)], qv.at[rows], gqsem.at[1, i]))

        for c in weights(0):
            c.start()

        cols = (chip_cols(r), chip_cols(pe))
        for q, A, dst in ((0, ha, ht), (1, ea, et)):
            def c_t(v):
                return [local(A.at[v // nm, v % nm, :, cols[c]], ab.at[v % 4, :, c * dq:(c + 1) * dq], tsem.at[v % 4, c]) for c in range(2)]

            def start(v):
                @pl.when(v >= nm)
                def _():
                    for h in range(2):
                        got_half(n_r.at[q * nm + v - nm, h]).wait_recv()
                for c in c_t(v):
                    c.start()
            for v in range(3):
                start(v)

            def build(v):
                for c in c_t(v):
                    c.wait()

                @pl.when(v + 3 < 2 * nm)
                def _():
                    start(v + 3)
                for c in range(2):
                    dst[c * dq:(c + 1) * dq, pl.ds(pl.multiple_of(v * T2, T2), T2)] = ab[v % 4, :, c * dq:(c + 1) * dq].T
            with SC('build1'):
                loop(2 * nm, build)

        for c in stream(0):
            c.start()

        def kept(q, j, m):
            mine = local(o.at[q, m], (m1, m2)[q].at[:, wcols(j, fb)], osem.at[q, m])
            rest = local(o.at[q, m], pb.at[q, j, m], osem.at[q, m])
            return mine, rest

        def sends(j):
            cs = wcols(j, fb)
            out = []
            for q in range(2):
                for c in range(2):
                    out.append(remote(pb.at[q, j, 2 + c], (r1, r2)[q].at[:, cs], pe_s.at[q, c, j], pe_r.at[q, k, j], (s, pe - k + c)))
                out.append(remote(pb.at[q, j, 1 - k], (m1, m2)[q].at[:, cs], ms_s.at[q, j], ms_r.at[q, j], (s, pr)))
            return out

        def ship(j):
            for q in range(2):
                loop(4, lambda m: kept(q, j, m)[1].wait())
            for c in sends(j):
                c.start()

        def part(j):
            ws = j % 2
            for c in weights(j):
                c.wait()

            @pl.when(j >= 1)
            def _():
                ship(j - 1)

            def again(i):
                v = j * nm + i
                sl = v % 2
                for c in stream(v):
                    c.wait()

                @pl.when(v + 1 < nj * nm)
                def _():
                    for c in stream(v + 1):
                        c.start()
                for c in saved(j, i):
                    c.start()
                rows = pl.ds(pl.multiple_of((nm + i) * T2, T2), T2)
                for h in range(2):
                    part_rows = pl.ds(pl.multiple_of((nm + i) * T2 + h * T, T), T)
                    g, dv[h * T:(h + 1) * T] = gelu_both(dot(ab[sl, h * T:(h + 1) * T], wb1[ws]))
                    gv[part_rows, :] = g.astype(BF16)
                p = dot_cols(ab[2 + sl], wb2[ws]).astype(BF16)
                qv[rows, :] = (p.astype(F32) * dv[...]).astype(BF16)
            with SC('again'):
                loop(nm, again)

            @pl.when(j + 1 < nj)
            def _():
                for c in weights(j + 1):
                    c.start()
            loop(nm, lambda i: [c.wait() for c in saved(j, i)])

            def grads(m):
                rows = pl.ds(pl.multiple_of(m * dr, dr), dr)
                o[0, m] = dot(ht[rows, :], qv[...])
                o[1, m] = dot(et[rows, :], gv[...])
                for q in range(2):
                    mine, rest = kept(q, j, m)

                    @pl.when(m == k)
                    def _():
                        mine.start()

                    @pl.when(m != k)
                    def _():
                        rest.start()
            with SC('grads1'):
                loop(4, grads)
        loop(nj, part)
        ship(nj - 1)

        def finish(j):
            for c in sends(j):
                c.wait_send()
            for q in range(2):
                remote(pb.at[q, j, 0], (m1, m2)[q].at[:, wcols(j, fb)], ms_s.at[q, j], ms_r.at[q, j], (s, pr)).wait_recv()
                for c in range(2):
                    remote(pb.at[q, j, 0], (r1, r2)[q].at[:, wcols(j, fb)], ms_s.at[q, j], pe_r.at[q, c, j], (s, pr)).wait_recv()
        with SC('finish1'):
            loop(nj, finish)

    nr = 2 * nm * T2

    @pl.when(is0)
    def _():
        pl.run_scoped(
            all_tokens,
            VMEM((nq, D, fs), BF16), VMEM((nq, fs, D), BF16), VMEM((2, T2, D), BF16),
            VMEM((2, T2, fs), F32), VMEM((4, T2, fs), F32), VMEM((2, T2, fs), BF16),
            DMA((2, nq)), DMA((2,)), DMA((2,)), DMA((4,)), DMA((2,)),
        )
        pl.run_scoped(
            sums0,
            VMEM((2, dq, 2 * nr), BF16), VMEM((2, 2 * nr, fs), BF16), VMEM((2, 2, dr, fs), F32), VMEM((8, T2, dq), BF16),
            DMA((8,)), DMA((2,)), DMA((2, 2)),
        )

    @pl.when(is1)
    def _():
        pl.run_scoped(
            sums1,
            VMEM((2, D, fs), BF16), VMEM((2, fs, D), BF16),
            VMEM((2 * dq, nr), BF16), VMEM((2 * dq, nr), BF16), VMEM((nr, fs), BF16), VMEM((nr, fs), BF16),
            VMEM((4, T2, D), BF16), VMEM((2, 4, dr, fs), F32), VMEM((T2, fs), F32),
            DMA((2, 2)), DMA((4, 2)), DMA((2, 2)), DMA((2, nm)), DMA((2, 4)),
        )

    for i in (nm - 2, nm - 1):
        n = i + nm * s
        remote(ob.at[0], ea.at[0, i, own], z_s.at[n], z_r.at[n], (1 - s, r)).wait_send()

    def settle(n):
        A = ha

        @pl.when(is0 | (n < nm))
        def _():
            for c in give(A.at[0, 0, own], A, n, 0, False):
                c.wait_send()

        @pl.when(is0)
        def _():
            remote(A.at[3, 0, own], A.at[3, 0, own], x_s.at[n], x_r.at[n], (s, dg)).wait_send()
            remote(A.at[3, 0, own], A.at[3, 0, own], h_s.at[n], h_r.at[n], (s, pr)).wait_send()
            remote(A.at[1, 0], A.at[2, 0], f_s.at[n], f_r.at[n], (s, pr)).wait_send()
    with SC('settle'):
        loop(nt, settle)

    @pl.when(is1)
    def _():
        def sent(d):
            @pl.when(d != 8 + r)
            def _():
                loss_copy(d).wait_send()
        loop(16, sent)
        loss_self().wait()

    def got(n):
        @pl.when(is0 | (n != r))
        def _():
            remote(lacc, lb.at[n], ls_s.at[n], ls_r.at[n], (s, r)).wait_recv()
    loop(8, got)


def solution(mesh):
    n_data = mesh.shape['data']

    def per_device(inputs, targets, w_up, w_down):
        nm, T, D = inputs.shape
        F = w_up.shape[2]
        Fk = F // 2
        fs = min(512, Fk // 4)
        nj = Fk // fs
        dr = D // 8
        inv = 1.0 / (n_data * nm * T)
        dims = (nm, T, D, Fk, fs, inv)
        sd = jax.ShapeDtypeStruct
        rows = 4 * nm * 2 * T
        out_shape = [
            sd((dr, F), F32), sd((dr, F), F32), sd((dr, F), F32), sd((dr, F), F32), sd((8, 8, 128), F32),
            sd((4, nm, 2 * T, D), BF16), sd((4, nm, 2 * T, D), BF16),
            sd((nm, 2 * T, Fk), F32), sd((nm, 2 * T, Fk), BF16), sd((nm, 2 * T, Fk), BF16),
            sd((rows, Fk // 2), F32), sd((rows, Fk // 2), BF16), sd((rows, Fk // 2), BF16),
            sd((2 * nm, T, D), F32), sd((2, nj, 4, dr, fs), F32),
        ]
        any_spec = pl.BlockSpec(memory_space=pl.ANY)
        n2 = 2 * nm
        outs = pl.pallas_call(
            functools.partial(kernel, dims),
            out_shape=out_shape,
            in_specs=[any_spec] * 4,
            out_specs=[any_spec] * len(out_shape),
            scratch_shapes=[
                VMEM((8, 128), F32), VMEM((2, T, D), BF16),
                DMA((n2,)), DMA((n2,)), DMA((n2,)), DMA((n2,)), DMA((n2,)), DMA((n2,)), DMA((n2, 2)), DMA((n2, 2)),
                DMA((n2,)), DMA((n2,)), DMA((n2,)), DMA((n2,)), DMA((n2,)), DMA((n2,)),
                DMA((2, nj)), DMA((2, nj)), DMA((2, 2, nj)), DMA((2, 2, nj)), DMA((16,)), DMA((8,)),
            ],
            compiler_params=pltpu.CompilerParams(has_side_effects=True, vmem_limit_bytes=67_000_000),
            cost_estimate=pl.CostEstimate(flops=16 * nm * T * D * F, bytes_accessed=10**9, transcendentals=0),
            name='train_step',
        )(inputs, targets, w_up.reshape(D, F), w_down.reshape(F, D))
        m1, r1, m2, r2, lb = outs[:5]
        loss = jnp.sum(lb) * (0.5 * inv)
        whole = lax.axis_index('stage') == 0
        up = jnp.where(whole, m1, m1 + r1)
        down = jnp.where(whole, m2, m2 + r2)
        return loss, up[None], down.T[None]

    return jax.shard_map(per_device, mesh=mesh, in_specs=(P('data', None, None), P('data', None, None), P('stage', None, None), P('stage', None, None)), out_specs=(P(), P('stage', 'data', None), P('stage', None, 'data')), check_vma=False)
```

```python
import functools
import math

import jax
import jax.numpy as jnp
from jax import lax
from jax.experimental import pallas as pl
from jax.experimental.pallas import tpu as pltpu
from jax.sharding import PartitionSpec as P

F32 = jnp.float32
BF16 = jnp.bfloat16
MESH = pl.DeviceIdType.MESH
SC = jax.named_scope
COLS = (((1,), (1,)), ((), ()))
GC = math.sqrt(2.0 / math.pi)
DMA = pltpu.SemaphoreType.DMA
VMEM = pltpu.VMEM


def dot(a, b):
    return jnp.dot(a, b, preferred_element_type=F32)


def dot_cols(a, b):
    return lax.dot_general(a, b, COLS, preferred_element_type=F32)


def gelu_both(u):
    u2 = u * u
    t = jnp.tanh(GC * (u + 0.044715 * (u2 * u)))
    half = 0.5 * (1.0 + t)
    return u * half, half + (0.5 * u) * (1.0 - t * t) * (GC + (3.0 * 0.044715 * GC) * u2)


def loop(n, body):
    lax.fori_loop(0, n, lambda i, c: (body(i), c)[1], 0)


def local(src, dst, sem):
    return pltpu.make_async_copy(src, dst, sem)


def remote(src, dst, ss, rs, dev):
    return pltpu.make_async_remote_copy(src_ref=src, dst_ref=dst, send_sem=ss, recv_sem=rs, device_id=dev, device_id_type=MESH)


def kernel(dims, x, y, w1, w2, m1, r1, m2, r2, lb, ha, ea, ub, gb, qb, ua, ga, qa, vx, pb,
           lacc, ob, z_s, z_r, d_s, d_r, v_s, v_r, n_s, n_r, x_s, x_r, f_s, f_r, h_s, h_r, ms_s, ms_r, pe_s, pe_r, ls_s, ls_r):
    nm, T, D, Fk, fs, inv = dims
    nj = Fk // fs
    nq = nj // 2
    nt = 2 * nm
    T2 = 2 * T
    dq, dr = D // 4, D // 8
    s = lax.axis_index('stage')
    r = lax.axis_index('data')
    k = r % 2
    xb = (r // 2) % 2
    yb_ = r // 4
    pr = r + 1 - 2 * k
    fx = r + 2 - 4 * xb
    fy = r + 4 - 8 * yb_
    dg = fy + 2 - 4 * xb
    ry, rx = fy - k, fx - k + 1
    nb = fy * (1 - k) + fx * k
    pe = fx * (1 - k) + fy * k
    fb = k * Fk
    q0 = (yb_ * (1 - k) + xb * k) * nq
    fq = fb + q0 * fs
    own = pl.ds(pl.multiple_of(k * T, T), T)
    oth = pl.ds(pl.multiple_of((1 - k) * T, T), T)
    is0, is1 = s == 0, s == 1

    def fcols(j):
        return pl.ds(pl.multiple_of(j * fs, fs), fs)

    def wcols(j, base):
        return pl.ds(pl.multiple_of(base + j * fs, fs), fs)

    def chip_cols(dev):
        return pl.ds(pl.multiple_of((dev // 2) * dq, 128), dq)

    def give(src, A, n, i, far):
        out = [
            remote(src, A.at[0, i, own], d_s.at[n], d_r.at[n], (s, pr)),
            remote(src, A.at[1, i, own], n_s.at[n, 0], n_r.at[n, k], (s, ry)),
            remote(src, A.at[1, i, own], n_s.at[n, 1], n_r.at[n, k], (s, rx)),
        ]
        if far:
            out.append(remote(src, A.at[3, i, own], x_s.at[n], x_r.at[n], (s, dg)))
        return out

    def got_half(sem):
        return remote(ha.at[0, 0, own], ha.at[0, 0, oth], x_s.at[0], sem, (s, pr))

    @pl.when(is0)
    def _():
        for i in range(nm):
            for c in give(x.at[i], ha, i, i, True):
                c.start()

    def phase1(wb1, wb2, ab, acc, uo, ui, go, tmp, yb, wsem, alsem, usem, isem, gsem, psem, lsem, hsem):
        lacc[...] = jnp.zeros_like(lacc)

        def sched(t):
            mid = (t > 0) & (t < nt - 1)
            kind1 = jnp.where(mid, (t + 1) % 2, jnp.where(t == 0, 0, 1))
            i1 = jnp.where(mid, jnp.where(t % 2 == 1, (t + 1) // 2, (t - 2) // 2), jnp.where(t == 0, 0, nm - 1))
            return jnp.where(is1, kind1, 0), jnp.where(is1, i1, t)

        def wslot(t, j):
            return (t * nj + j) % 4

        def c_w1(t, j):
            return local(w1.at[:, wcols(j, fb)], wb1.at[wslot(t, j)], wsem.at[0, wslot(t, j)])

        def c_w2(t, j):
            return local(w2.at[wcols(j, fb), :], wb2.at[wslot(t, j)], wsem.at[1, wslot(t, j)])

        def first_weights(t):
            for j in range(3):
                c_w1(t, j).start()
                c_w2(t, j).start()

        def prep_a(t):
            kind, i = sched(t)

            @pl.when(is1 & (kind == 0))
            def _():
                with SC('w_z_h'):
                    got_half(z_r.at[i]).wait_recv()
                for c in give(ha.at[0, i, own], ha, i, i, False):
                    c.start()

        def u_in(i, j):
            return local(ub.at[i, :, fcols(j)], ui.at[j % 2], isem.at[j % 2])

        def prep_b(t):
            kind, i = sched(t)
            ap = t % 2
            for kk, A in ((0, ha), (1, ea)):
                @pl.when(kind == kk)
                def _():
                    with SC('w_d'):
                        got_half(d_r.at[kk * nm + i]).wait_recv()
                    if kk == 1:
                        local(ob.at[0], ea.at[0, i, own], lsem.at[i]).wait()
                        u_in(i, 0).start()
                    if kk == 0:
                        @pl.when(is0)
                        def _():
                            local(x.at[i], ab.at[ap, own], alsem.at[ap, 0]).start()

                    @pl.when(is1)
                    def _():
                        local(A.at[0, i, own], ab.at[ap, own], alsem.at[ap, 0]).start()
                    local(A.at[0, i, oth], ab.at[ap, oth], alsem.at[ap, 1]).start()

        def exchange(t):
            kind, i = sched(t)
            n = kind * nm + i
            return remote(acc.at[t % 2, oth], vx.at[n], v_s.at[n], v_r.at[n], (s, pr))

        def wait_out(t):
            kind, i = sched(t)

            @pl.when(is0 | (kind == 1))
            def _():
                n = kind * nm + i
                remote(ob.at[0], ea.at[0, i, own], z_s.at[n], z_r.at[n], (1 - s, r)).wait_send()

            @pl.when(is1 & (kind == 0))
            def _():
                for c in give(ob.at[0], ea, nm + i, i, False):
                    c.wait_send()

        def post_a(t):
            kind, i = sched(t)
            with SC('w_exch'):
                exchange(t).wait()
            local(vx.at[kind * nm + i], tmp, psem.at[0]).start()
            local(y.at[i], yb, psem.at[1]).start()

        def post_b(t):
            kind, i = sched(t)
            n = kind * nm + i
            ap = t % 2

            @pl.when(t >= 2)
            def _():
                with SC('w_out'):
                    wait_out(t - 2)
            local(vx.at[n], tmp, psem.at[0]).wait()
            local(y.at[i], yb, psem.at[1]).wait()
            last = is1 & (kind == 0)
            rb = min(64, T)

            def rows(b):
                lo = pl.ds(pl.multiple_of(b * rb, rb), rb)
                mine = pl.ds(pl.multiple_of(k * T + b * rb, rb), rb)
                h = (ab[ap, mine, :].astype(F32) + (acc[ap, mine, :] + tmp[lo, :])).astype(BF16)

                @pl.when(last)
                def _():
                    d = h.astype(F32) - yb[lo, :].astype(F32)
                    ob[ap, lo, :] = (d * inv).astype(BF16)
                    sq = jnp.sum((d * d).reshape(rb // 8, 8, D), axis=0)
                    part = lacc[...]
                    for c in range(D // 128):
                        part = part + sq[:, c * 128:(c + 1) * 128]
                    lacc[...] = part

                @pl.when(jnp.logical_not(last))
                def _():
                    ob[ap, lo, :] = h
            with SC('post_rows'):
                loop(T // rb, rows)

            @pl.when(is0)
            def _():
                remote(ob.at[ap], ha.at[0, i, own], z_s.at[n], z_r.at[n], (1 - s, r)).start()

            @pl.when(is1 & (kind == 1))
            def _():
                remote(ob.at[ap], ea.at[0, i, own], z_s.at[n], z_r.at[n], (1 - s, r)).start()

            @pl.when(last)
            def _():
                for c in give(ob.at[ap], ea, nm + i, i, False):
                    c.start()
                local(ob.at[ap], ea.at[0, i, own], lsem.at[i]).start()

        j_a = max(0, nj // 2 - 2)
        j_b = j_a + 1
        j_c = min(j_b + 1, nj - 2)
        j_d = nj - 2

        def slot(t):
            kind, i = sched(t)
            ap = t % 2
            more = t + 1 < nm + nm * s

            @pl.when(is0 | (t == 0))
            def _():
                prep_a(t)
                prep_b(t)

            local(ha.at[0, i, own], ab.at[ap, own], alsem.at[ap, 0]).wait()
            local(ha.at[0, i, oth], ab.at[ap, oth], alsem.at[ap, 1]).wait()

            @pl.when(is0)
            def _():
                local(ab.at[ap, own], ha.at[0, i, own], hsem).start()

            def hooks(j):
                late = is1 & (t > 0)

                @pl.when(late & (j == j_a))
                def _():
                    post_a(t - 1)

                @pl.when(late & (j == j_b))
                def _():
                    post_b(t - 1)

                @pl.when(is1 & more & (j == jnp.where(t == 0, j_d, j_c)))
                def _():
                    prep_a(t + 1)

                @pl.when(is1 & more & (j == j_d))
                def _():
                    prep_b(t + 1)

            def run(c1, c2, before, first, second, after):
                c1(t, 0).wait()
                c1(t, 3).start()
                before(0)
                acc[ap] = jnp.zeros((T2, D), F32)
                first(0)
                after(0)

                def step(j):
                    c1(t, j + 1).wait()
                    c2(t, j).wait()

                    @pl.when(j + 4 < nj)
                    def _():
                        c1(t, j + 4).start()

                    @pl.when(j + 3 < nj)
                    def _():
                        c2(t, j + 3).start()
                    hooks(j)
                    before(j + 1)
                    first(j + 1)
                    acc[ap] += second(j)
                    after(j + 1)
                loop(nj - 1, step)
                c2(t, nj - 1).wait()

                @pl.when(more)
                def _():
                    first_weights(t + 1)
                acc[ap] += second(nj - 1)

            def g_out(j, dst):
                return local(go.at[j % 2], dst.at[i, :, fcols(j)], gsem.at[j % 2])

            def u_out(j):
                return local(uo.at[j % 2], ub.at[i, :, fcols(j)], usem.at[j % 2])

            def mine(j):
                return (j >= q0) & (j < q0 + nq)

            def keep(j):
                @pl.when(is1)
                def _():
                    u_out(j).start()
                    g_out(j, gb).start()

                @pl.when(is0 & mine(j))
                def _():
                    rows = pl.ds(pl.multiple_of(i * T2, T2), T2)
                    local(uo.at[j % 2], ua.at[rows, fcols(j - q0)], usem.at[j % 2]).start()
                    local(go.at[j % 2], ga.at[rows, fcols(j - q0)], gsem.at[j % 2]).start()

            def kept(j):
                @pl.when(is1 | mine(j))
                def _():
                    u_out(j).wait()
                    g_out(j, gb).wait()

            @pl.when(kind == 0)
            def _():
                def before(j):
                    @pl.when(j >= 2)
                    def _():
                        kept(j - 2)

                def first(j):
                    for hq in range(4):
                        h = slice(hq * T // 2, (hq + 1) * T // 2)
                        g, uo[j % 2, h] = gelu_both(dot(ab[ap, h], wb1[wslot(t, j)]))
                        go[j % 2, h] = g.astype(BF16)

                with SC('slotF'):
                    run(c_w1, c_w2, before, first, lambda j: dot(go[j % 2], wb2[wslot(t, j)]), keep)
                for j in (nj - 2, nj - 1):
                    kept(j)

            @pl.when(kind == 1)
            def _():
                def before(j):
                    @pl.when(j >= 2)
                    def _():
                        g_out(j - 2, qb).wait()
                    u_in(i, j).wait()

                    @pl.when(j + 1 < nj)
                    def _():
                        u_in(i, j + 1).start()

                def first(j):
                    p = dot_cols(ab[ap], wb2[wslot(t, j)]).astype(BF16)
                    go[j % 2] = (p.astype(F32) * ui[j % 2]).astype(BF16)
                with SC('slotB'):
                    run(c_w2, c_w1, before, first, lambda j: dot_cols(go[j % 2], wb1[wslot(t, j)]), lambda j: g_out(j, qb).start())
                for j in (nj - 2, nj - 1):
                    g_out(j, qb).wait()

            @pl.when(is0)
            def _():
                local(ab.at[ap, own], ha.at[0, i, own], hsem).wait()
            exchange(t).start()

            @pl.when(is0 | (t == nt - 1))
            def _():
                post_a(t)
                post_b(t)

        first_weights(0)
        n_slots = nm + nm * s
        lax.fori_loop(0, n_slots, lambda t, c: (slot(t), c)[1], 0)

    pl.run_scoped(
        phase1,
        VMEM((4, D, fs), BF16), VMEM((4, fs, D), BF16), VMEM((2, T2, D), BF16), VMEM((2, T2, D), F32),
        VMEM((2, T2, fs), F32), VMEM((2, T2, fs), F32), VMEM((2, T2, fs), BF16),
        VMEM((T, D), F32), VMEM((T, D), BF16),
        DMA((2, 4)), DMA((2, 2)), DMA((2,)), DMA((2,)), DMA((2,)), DMA((2,)), DMA((nm,)), DMA,
    )

    def loss_copy(d):
        return remote(lacc, lb.at[r], ls_s.at[d], ls_r.at[r], (d // 8, d % 8))

    def loss_self():
        return local(lacc, lb.at[r], ls_s.at[8 + r])

    @pl.when(is1)
    def _():
        def send(d):
            @pl.when(d != 8 + r)
            def _():
                loss_copy(d).start()
        loop(16, send)
        loss_self().start()

    nc = 4 * nm

    def all_tokens(wq1, wq2, ab, uo, ui, go, qsem, alsem, usem, isem, gsem):
        def c_q1(j):
            return local(w1.at[:, wcols(j, fq)], wq1.at[j], qsem.at[0, j])

        def c_q2(j):
            return local(w2.at[wcols(j, fq), :], wq2.at[j], qsem.at[1, j])
        for j in range(nq):
            c_q1(j).start()

        def arrive(A, n, c, i):
            @pl.when(c == 1)
            def _():
                for h in range(2):
                    with SC('a_c1'):
                        got_half(n_r.at[n, h]).wait_recv()
                remote(A.at[1, i], A.at[2, i], f_s.at[n], f_r.at[n], (s, pr)).start()

            @pl.when(c == 2)
            def _():
                with SC('a_c2'):
                    remote(A.at[1, i], A.at[2, i], f_s.at[n], f_r.at[n], (s, pr)).wait_recv()

            @pl.when(c == 3)
            def _():
                with SC('a_c3'):
                    got_half(x_r.at[n]).wait_recv()
                remote(A.at[3, i, own], A.at[3, i, own], h_s.at[n], h_r.at[n], (s, pr)).start()
                with SC('a_c3b'):
                    got_half(h_r.at[n]).wait_recv()

        def c_ab(A, c, i, v):
            return local(A.at[c, i], ab.at[v % 2], alsem.at[v % 2])

        def block(c, i):
            return pl.ds(pl.multiple_of((c * nm + i) * T2, T2), T2)

        def pass_on(i):
            n = nm + i
            with SC('a_z'):
                got_half(z_r.at[n]).wait_recv()
            for cp in give(ea.at[0, i, own], ea, n, i, True):
                cp.start()

        def run(nc, A, at, ready, before, first, outs):
            def load(v):
                c, i = at(v)
                ready(c, i)
                c_ab(A, c, i, v).start()
            load(0)

            def chunk(v):
                c, i = at(v)
                c_ab(A, c, i, v).wait()

                def step(j):
                    g = v * nq + j

                    @pl.when((j == nq - 2) & (v + 1 < nc))
                    def _():
                        load(v + 1)

                    @pl.when(g >= 2)
                    def _():
                        for o in outs(g - 2):
                            o.wait()
                    before(g)
                    first(v, j, g % 2)
                    for o in outs(g):
                        o.start()
                with SC('uchunk'):
                    loop(nq, step)
            loop(nc, chunk)
            for g in (nc * nq - 2, nc * nq - 1):
                for o in outs(g):
                    o.wait()

        def at_h(v):
            return 1 + v // nm, v % nm

        def outs_h(g):
            c, i = at_h(g // nq)
            return [local(uo.at[g % 2], ua.at[block(c, i), fcols(g % nq)], usem.at[g % 2]),
                    local(go.at[g % 2], ga.at[block(c, i), fcols(g % nq)], gsem.at[g % 2])]

        def before_h(g):
            @pl.when(g < nq)
            def _():
                c_q1(g).wait()
                c_q2(g).start()

        def first_h(v, j, sl):
            for hq in range(4):
                h = slice(hq * T // 2, (hq + 1) * T // 2)
                g, uo[sl, h] = gelu_both(dot(ab[v % 2, h], wq1[j]))
                go[sl, h] = g.astype(BF16)

        def ready_h(c, i):
            @pl.when((c == 2) & (i == nm // 2))
            def _():
                pass_on(0)
            arrive(ha, i, c, i)
        run(3 * nm, ha, at_h, ready_h, before_h, first_h, outs_h)

        def at_e(v):
            return v % 4, v // 4

        def outs_e(g):
            c, i = at_e(g // nq)
            return [local(go.at[g % 2], qa.at[block(c, i), fcols(g % nq)], gsem.at[g % 2])]

        def u_in(g):
            c, i = at_e(g // nq)
            return local(ua.at[block(c, i), fcols(g % nq)], ui.at[g % 4], isem.at[g % 4])

        def before_e(g):
            @pl.when(g < nq)
            def _():
                c_q2(g).wait()
            u_in(g).wait()

            @pl.when(g + 3 < nc * nq)
            def _():
                u_in(g + 3).start()

        def ready_e(c, i):
            n = nm + i

            @pl.when(c == 0)
            def _():
                with SC('a_d'):
                    got_half(d_r.at[n]).wait_recv()
            arrive(ea, n, c, i)

            @pl.when((c == 1) & (i + 1 < nm))
            def _():
                pass_on(i + 1)

        def first_e(v, j, sl):
            p = dot_cols(ab[v % 2], wq2[j]).astype(BF16)
            go[sl] = (p.astype(F32) * ui[(v * nq + j) % 4]).astype(BF16)
        for g in range(3):
            u_in(g).start()
        run(nc, ea, at_e, ready_e, before_e, first_e, outs_e)

    def sums0(hv, bv, o, tb, tsem, bsem, osem):
        nw = 4 * nq

        def at(w):
            return w // (2 * nq), (w // 2) % nq, w % 2

        def load(w):
            _, j, q = at(w)
            for qq, A in ((0, qa), (1, ga)):
                @pl.when(q == qq)
                def _():
                    local(A.at[:, fcols(j)], bv.at[w % 2], bsem.at[w % 2]).start()

        def far(w, q, m):
            j = at(w)[1]
            return remote(pb.at[q, j, 2 + m], (m1, m2)[q].at[:, wcols(j, fq)], pe_s.at[q, m, j], pe_r.at[q, k, j], (s, nb - k + m))

        def near(w, q):
            j = at(w)[1]
            return remote(pb.at[q, j, 1 - k], (m1, m2)[q].at[:, wcols(j, fq)], ms_s.at[q, j], ms_r.at[q, j], (s, pr))

        def ship(w):
            ps, j, q = at(w)
            for qq in range(2):
                @pl.when(q == qq)
                def _():
                    for m in range(2):
                        local(o.at[qq, m], pb.at[qq, j, m], osem.at[qq, m]).wait()

                    @pl.when(ps == 0)
                    def _():
                        for m in range(2):
                            far(w, qq, m).start()

                    @pl.when(ps == 1)
                    def _():
                        near(w, qq).start()

        def one(ps):
            cols = pl.ds(pl.multiple_of((nb // 2) * dq * (1 - ps) + (r // 2) * dq * ps, 128), dq)
            for qq, A in ((0, ha), (1, ea)):
                def c_t(v):
                    return local(A.at[v // nm, v % nm, :, cols], tb.at[v % 8], tsem.at[v % 8])
                for v in range(7):
                    c_t(v).start()

                def build(v):
                    c_t(v).wait()

                    @pl.when(v + 7 < nc)
                    def _():
                        c_t(v + 7).start()
                    hv[qq, :, pl.ds(pl.multiple_of(v * T2, T2), T2)] = tb[v % 8].T
                with SC('build0'):
                    loop(nc, build)

            def unit(ww):
                w = ps * 2 * nq + ww
                _, j, q = at(w)
                local(qa.at[:, fcols(j)], bv.at[w % 2], bsem.at[w % 2]).wait()

                @pl.when(w + 1 < nw)
                def _():
                    load(w + 1)

                def grads(m):
                    rows = pl.ds(pl.multiple_of(m * dr, dr), dr)

                    @pl.when((w >= 1) & (m == 1))
                    def _():
                        ship(w - 1)
                    o[q, m] = dot(hv[q, rows, :], bv[w % 2])
                    for qq, M in ((0, m1), (1, m2)):
                        here = (ps == 1) & (m == k)

                        @pl.when((q == qq) & here)
                        def _():
                            local(o.at[qq, m], M.at[:, wcols(j, fq)], osem.at[qq, m]).start()

                        @pl.when((q == qq) & jnp.logical_not(here))
                        def _():
                            local(o.at[qq, m], pb.at[qq, j, 2 * (1 - ps) + m], osem.at[qq, m]).start()
                with SC('grads0'):
                    loop(2, grads)
            loop(2 * nq, unit)
        load(0)
        loop(2, one)
        ship(nw - 1)

        def finish(j):
            w = 2 * j
            for q in range(2):
                near(w, q).wait()
                for m in range(2):
                    far(w, q, m).wait_send()
                    remote(pb.at[q, j, 0], (m1, m2)[q].at[:, wcols(j, fq)], ms_s.at[q, j], pe_r.at[q, m, j], (s, pr)).wait_recv()
        with SC('finish0'):
            loop(nq, finish)

    def sums1(wb1, wb2, ht, et, gv, qv, ab, o, dv, wsem, tsem, asem, gqsem, osem):
        def weights(j):
            return (local(w1.at[:, wcols(j, fb)], wb1.at[j % 2], wsem.at[0, j % 2]),
                    local(w2.at[wcols(j, fb), :], wb2.at[j % 2], wsem.at[1, j % 2]))

        def stream(v):
            i, sl = v % nm, v % 2
            return (local(ha.at[1, i], ab.at[sl], asem.at[0, sl]), local(ea.at[1, i], ab.at[2 + sl], asem.at[1, sl]))

        def saved(j, i):
            rows = pl.ds(pl.multiple_of(i * T2, T2), T2)
            return (local(gb.at[i, :, fcols(j)], gv.at[rows], gqsem.at[0, i]),
                    local(qb.at[i, :, fcols(j)], qv.at[rows], gqsem.at[1, i]))

        for c in weights(0):
            c.start()

        cols = (chip_cols(r), chip_cols(pe))
        for q, A, dst in ((0, ha, ht), (1, ea, et)):
            def c_t(v):
                return [local(A.at[v // nm, v % nm, :, cols[c]], ab.at[v % 4, :, c * dq:(c + 1) * dq], tsem.at[v % 4, c]) for c in range(2)]

            def start(v):
                @pl.when(v >= nm)
                def _():
                    for h in range(2):
                        got_half(n_r.at[q * nm + v - nm, h]).wait_recv()
                for c in c_t(v):
                    c.start()
            for v in range(3):
                start(v)

            def build(v):
                for c in c_t(v):
                    c.wait()

                @pl.when(v + 3 < 2 * nm)
                def _():
                    start(v + 3)
                for c in range(2):
                    dst[c * dq:(c + 1) * dq, pl.ds(pl.multiple_of(v * T2, T2), T2)] = ab[v % 4, :, c * dq:(c + 1) * dq].T
            with SC('build1'):
                loop(2 * nm, build)

        for c in stream(0):
            c.start()

        def kept(q, j, m):
            mine = local(o.at[q, m], (m1, m2)[q].at[:, wcols(j, fb)], osem.at[q, m])
            rest = local(o.at[q, m], pb.at[q, j, m], osem.at[q, m])
            return mine, rest

        def far(j):
            return [remote(pb.at[q, j, 2 + c], (r1, r2)[q].at[:, wcols(j, fb)], pe_s.at[q, c, j], pe_r.at[q, k, j], (s, pe - k + c))
                    for q in range(2) for c in range(2)]

        def near(j):
            return [remote(pb.at[q, j, 1 - k], (m1, m2)[q].at[:, wcols(j, fb)], ms_s.at[q, j], ms_r.at[q, j], (s, pr)) for q in range(2)]

        def ship(j, m0, copies):
            for q in range(2):
                for m in (m0, m0 + 1):
                    kept(q, j, m)[1].wait()
            for c in copies:
                c.start()

        def part(j):
            ws = j % 2
            for c in weights(j):
                c.wait()

            @pl.when(j >= 1)
            def _():
                ship(j - 1, 0, near(j - 1))

            def again(i):
                v = j * nm + i
                sl = v % 2
                for c in stream(v):
                    c.wait()

                @pl.when(v + 1 < nj * nm)
                def _():
                    for c in stream(v + 1):
                        c.start()
                for c in saved(j, i):
                    c.start()
                rows = pl.ds(pl.multiple_of((nm + i) * T2, T2), T2)
                for h in range(4):
                    T4 = T // 2
                    part_rows = pl.ds(pl.multiple_of((nm + i) * T2 + h * T4, T4), T4)
                    g, dv[h * T4:(h + 1) * T4] = gelu_both(dot(ab[sl, h * T4:(h + 1) * T4], wb1[ws]))
                    gv[part_rows, :] = g.astype(BF16)
                p = dot_cols(ab[2 + sl], wb2[ws]).astype(BF16)
                qv[rows, :] = (p.astype(F32) * dv[...]).astype(BF16)
            with SC('again'):
                loop(nm, again)

            @pl.when(j + 1 < nj)
            def _():
                for c in weights(j + 1):
                    c.start()
            loop(nm, lambda i: [c.wait() for c in saved(j, i)])

            def grads(v):
                m = (v + 2) % 4
                rows = pl.ds(pl.multiple_of(m * dr, dr), dr)

                @pl.when(v == 3)
                def _():
                    ship(j, 2, far(j))
                o[0, m] = dot(ht[rows, :], qv[...])
                o[1, m] = dot(et[rows, :], gv[...])
                for q in range(2):
                    mine, rest = kept(q, j, m)

                    @pl.when(m == k)
                    def _():
                        mine.start()

                    @pl.when(m != k)
                    def _():
                        rest.start()
            with SC('grads1'):
                loop(4, grads)
        loop(nj, part)
        ship(nj - 1, 0, near(nj - 1))

        def finish(j):
            for c in far(j) + near(j):
                c.wait_send()
            for q in range(2):
                remote(pb.at[q, j, 0], (m1, m2)[q].at[:, wcols(j, fb)], ms_s.at[q, j], ms_r.at[q, j], (s, pr)).wait_recv()
                for c in range(2):
                    remote(pb.at[q, j, 0], (r1, r2)[q].at[:, wcols(j, fb)], ms_s.at[q, j], pe_r.at[q, c, j], (s, pr)).wait_recv()
        with SC('finish1'):
            loop(nj, finish)

    nr = 2 * nm * T2

    @pl.when(is0)
    def _():
        pl.run_scoped(
            all_tokens,
            VMEM((nq, D, fs), BF16), VMEM((nq, fs, D), BF16), VMEM((2, T2, D), BF16),
            VMEM((2, T2, fs), F32), VMEM((4, T2, fs), F32), VMEM((2, T2, fs), BF16),
            DMA((2, nq)), DMA((2,)), DMA((2,)), DMA((4,)), DMA((2,)),
        )
        pl.run_scoped(
            sums0,
            VMEM((2, dq, 2 * nr), BF16), VMEM((2, 2 * nr, fs), BF16), VMEM((2, 2, dr, fs), F32), VMEM((8, T2, dq), BF16),
            DMA((8,)), DMA((2,)), DMA((2, 2)),
        )

    @pl.when(is1)
    def _():
        pl.run_scoped(
            sums1,
            VMEM((2, D, fs), BF16), VMEM((2, fs, D), BF16),
            VMEM((2 * dq, nr), BF16), VMEM((2 * dq, nr), BF16), VMEM((nr, fs), BF16), VMEM((nr, fs), BF16),
            VMEM((4, T2, D), BF16), VMEM((2, 4, dr, fs), F32), VMEM((T2, fs), F32),
            DMA((2, 2)), DMA((4, 2)), DMA((2, 2)), DMA((2, nm)), DMA((2, 4)),
        )

    for i in (nm - 2, nm - 1):
        n = i + nm * s
        remote(ob.at[0], ea.at[0, i, own], z_s.at[n], z_r.at[n], (1 - s, r)).wait_send()

    def settle(n):
        A = ha

        @pl.when(is0 | (n < nm))
        def _():
            for c in give(A.at[0, 0, own], A, n, 0, False):
                c.wait_send()

        @pl.when(is0)
        def _():
            remote(A.at[3, 0, own], A.at[3, 0, own], x_s.at[n], x_r.at[n], (s, dg)).wait_send()
            remote(A.at[3, 0, own], A.at[3, 0, own], h_s.at[n], h_r.at[n], (s, pr)).wait_send()
            remote(A.at[1, 0], A.at[2, 0], f_s.at[n], f_r.at[n], (s, pr)).wait_send()
    with SC('settle'):
        loop(nt, settle)

    @pl.when(is1)
    def _():
        def sent(d):
            @pl.when(d != 8 + r)
            def _():
                loss_copy(d).wait_send()
        loop(16, sent)
        loss_self().wait()

    def got(n):
        @pl.when(is0 | (n != r))
        def _():
            remote(lacc, lb.at[n], ls_s.at[n], ls_r.at[n], (s, r)).wait_recv()
    loop(8, got)


def solution(mesh):
    n_data = mesh.shape['data']

    def per_device(inputs, targets, w_up, w_down):
        nm, T, D = inputs.shape
        F = w_up.shape[2]
        Fk = F // 2
        fs = min(512, Fk // 4)
        nj = Fk // fs
        dr = D // 8
        inv = 1.0 / (n_data * nm * T)
        dims = (nm, T, D, Fk, fs, inv)
        sd = jax.ShapeDtypeStruct
        rows = 4 * nm * 2 * T
        out_shape = [
            sd((dr, F), F32), sd((dr, F), F32), sd((dr, F), F32), sd((dr, F), F32), sd((8, 8, 128), F32),
            sd((4, nm, 2 * T, D), BF16), sd((4, nm, 2 * T, D), BF16),
            sd((nm, 2 * T, Fk), F32), sd((nm, 2 * T, Fk), BF16), sd((nm, 2 * T, Fk), BF16),
            sd((rows, Fk // 2), F32), sd((rows, Fk // 2), BF16), sd((rows, Fk // 2), BF16),
            sd((2 * nm, T, D), F32), sd((2, nj, 4, dr, fs), F32),
        ]
        any_spec = pl.BlockSpec(memory_space=pl.ANY)
        n2 = 2 * nm
        outs = pl.pallas_call(
            functools.partial(kernel, dims),
            out_shape=out_shape,
            in_specs=[any_spec] * 4,
            out_specs=[any_spec] * len(out_shape),
            scratch_shapes=[
                VMEM((8, 128), F32), VMEM((2, T, D), BF16),
                DMA((n2,)), DMA((n2,)), DMA((n2,)), DMA((n2,)), DMA((n2,)), DMA((n2,)), DMA((n2, 2)), DMA((n2, 2)),
                DMA((n2,)), DMA((n2,)), DMA((n2,)), DMA((n2,)), DMA((n2,)), DMA((n2,)),
                DMA((2, nj)), DMA((2, nj)), DMA((2, 2, nj)), DMA((2, 2, nj)), DMA((16,)), DMA((8,)),
            ],
            compiler_params=pltpu.CompilerParams(has_side_effects=True, vmem_limit_bytes=67_000_000),
            cost_estimate=pl.CostEstimate(flops=16 * nm * T * D * F, bytes_accessed=10**9, transcendentals=0),
            name='train_step',
        )(inputs, targets, w_up.reshape(D, F), w_down.reshape(F, D))
        m1, r1, m2, r2, lb = outs[:5]
        loss = jnp.sum(lb) * (0.5 * inv)
        whole = lax.axis_index('stage') == 0
        up = jnp.where(whole, m1, m1 + r1)
        down = jnp.where(whole, m2, m2 + r2)
        return loss, up[None], down.T[None]

    return jax.shard_map(per_device, mesh=mesh, in_specs=(P('data', None, None), P('data', None, None), P('stage', None, None), P('stage', None, None)), out_specs=(P(), P('stage', 'data', None), P('stage', None, 'data')), check_vma=False)
```

```python
import functools
import math

import jax
import jax.numpy as jnp
from jax import lax
from jax.experimental import pallas as pl
from jax.experimental.pallas import tpu as pltpu
from jax.sharding import PartitionSpec as P

F32 = jnp.float32
BF16 = jnp.bfloat16
MESH = pl.DeviceIdType.MESH
SC = jax.named_scope
COLS = (((1,), (1,)), ((), ()))
GC = math.sqrt(2.0 / math.pi)
DMA = pltpu.SemaphoreType.DMA
PAIR = (0, 1)
AHEAD = (0, 1, 2)
VMEM = pltpu.VMEM


def dot(a, b):
    return jnp.dot(a, b, preferred_element_type=F32)


def dot_cols(a, b):
    return lax.dot_general(a, b, COLS, preferred_element_type=F32)


def gelu_both(u):
    u2 = u * u
    t = jnp.tanh(GC * (u + 0.044715 * (u2 * u)))
    half = 0.5 * (1.0 + t)
    return u * half, half + (0.5 * u) * (1.0 - t * t) * (GC + (3.0 * 0.044715 * GC) * u2)


def loop(n, body):
    lax.fori_loop(0, n, lambda i, c: (body(i), c)[1], 0)


def local(src, dst, sem):
    return pltpu.make_async_copy(src, dst, sem)


def remote(src, dst, ss, rs, dev):
    return pltpu.make_async_remote_copy(src_ref=src, dst_ref=dst, send_sem=ss, recv_sem=rs, device_id=dev, device_id_type=MESH)


def kernel(dims, x, y, w1, w2, m1, r1, m2, r2, lb, ha, ea, ub, gb, qb, ua, ga, qa, vx, pb,
           lacc, ob, z_s, z_r, d_s, d_r, v_s, v_r, n_s, n_r, x_s, x_r, f_s, f_r, h_s, h_r, ms_s, ms_r, pe_s, pe_r, ls_s, ls_r):
    nm, T, D, Fk, fs, inv = dims
    nj = Fk // fs
    nq = nj // 2
    nt = 2 * nm
    T2 = 2 * T
    dq, dr = D // 4, D // 8
    s = lax.axis_index('stage')
    r = lax.axis_index('data')
    k = r % 2
    xb = (r // 2) % 2
    yb_ = r // 4
    pr = r + 1 - 2 * k
    fx = r + 2 - 4 * xb
    fy = r + 4 - 8 * yb_
    dg = fy + 2 - 4 * xb
    ry, rx = fy - k, fx - k + 1
    nb = fy * (1 - k) + fx * k
    pe = fx * (1 - k) + fy * k
    fb = k * Fk
    q0 = (yb_ * (1 - k) + xb * k) * nq
    fq = fb + q0 * fs
    own = pl.ds(pl.multiple_of(k * T, T), T)
    oth = pl.ds(pl.multiple_of((1 - k) * T, T), T)
    is0, is1 = s == 0, s == 1

    def fcols(j):
        return pl.ds(pl.multiple_of(j * fs, fs), fs)

    def wcols(j, base):
        return pl.ds(pl.multiple_of(base + j * fs, fs), fs)

    def chip_cols(dev):
        return pl.ds(pl.multiple_of((dev // 2) * dq, 128), dq)

    def give(src, A, n, i, far):
        out = [
            remote(src, A.at[0, i, own], d_s.at[n], d_r.at[n], (s, pr)),
            remote(src, A.at[1, i, own], n_s.at[n, 0], n_r.at[n, k], (s, ry)),
            remote(src, A.at[1, i, own], n_s.at[n, 1], n_r.at[n, k], (s, rx)),
        ]
        if far:
            out.append(remote(src, A.at[3, i, own], x_s.at[n], x_r.at[n], (s, dg)))
        return out

    def got_half(sem):
        return remote(ha.at[0, 0, own], ha.at[0, 0, oth], x_s.at[0], sem, (s, pr))

    @pl.when(is0)
    def _():
        for i in range(nm):
            for c in give(x.at[i], ha, i, i, True):
                c.start()

    def phase1(wb1, wb2, ab, acc, uo, ui, go, tmp, yb, wsem, alsem, usem, isem, gsem, psem, lsem, hsem):
        lacc[...] = jnp.zeros_like(lacc)

        def sched(t):
            mid = (t > 0) & (t < nt - 1)
            kind1 = jnp.where(mid, (t + 1) % 2, jnp.where(t == 0, 0, 1))
            i1 = jnp.where(mid, jnp.where(t % 2 == 1, (t + 1) // 2, (t - 2) // 2), jnp.where(t == 0, 0, nm - 1))
            return jnp.where(is1, kind1, 0), jnp.where(is1, i1, t)

        def wslot(t, j):
            return (t * nj + j) % 3

        def c_w1(t, j):
            return local(w1.at[:, wcols(j, fb)], wb1.at[wslot(t, j)], wsem.at[0, wslot(t, j)])

        def c_w2(t, j):
            return local(w2.at[wcols(j, fb), :], wb2.at[wslot(t, j)], wsem.at[1, wslot(t, j)])

        def first_weights(t, js):
            for j in js:
                c_w1(t, j).start()
                c_w2(t, j).start()

        def prep_a(t):
            kind, i = sched(t)

            @pl.when(is1 & (kind == 0))
            def _():
                with SC('w_z_h'):
                    got_half(z_r.at[i]).wait_recv()
                for c in give(ha.at[0, i, own], ha, i, i, False):
                    c.start()

        def u_in(t, i, j):
            at = (t * nj + j) % 4
            return local(ub.at[i, :, fcols(j)], ui.at[at], isem.at[at])

        def prep_b(t):
            kind, i = sched(t)
            ap = t % 2
            for kk, A in ((0, ha), (1, ea)):
                @pl.when(kind == kk)
                def _():
                    with SC('w_d'):
                        got_half(d_r.at[kk * nm + i]).wait_recv()
                    if kk == 1:
                        local(ob.at[0], ea.at[0, i, own], lsem.at[i]).wait()
                        for j in AHEAD:
                            u_in(t, i, j).start()
                    if kk == 0:
                        @pl.when(is0)
                        def _():
                            local(x.at[i], ab.at[ap, own], alsem.at[ap, 0]).start()

                    @pl.when(is1)
                    def _():
                        local(A.at[0, i, own], ab.at[ap, own], alsem.at[ap, 0]).start()
                    local(A.at[0, i, oth], ab.at[ap, oth], alsem.at[ap, 1]).start()

        def exchange(t):
            kind, i = sched(t)
            n = kind * nm + i
            return remote(acc.at[t % 2, oth], vx.at[n], v_s.at[n], v_r.at[n], (s, pr))

        def wait_out(t):
            kind, i = sched(t)

            @pl.when(is0 | (kind == 1))
            def _():
                n = kind * nm + i
                remote(ob.at[0], ea.at[0, i, own], z_s.at[n], z_r.at[n], (1 - s, r)).wait_send()

            @pl.when(is1 & (kind == 0))
            def _():
                for c in give(ob.at[0], ea, nm + i, i, False):
                    c.wait_send()

        def post_a(t):
            kind, i = sched(t)
            with SC('w_exch'):
                exchange(t).wait()
            local(vx.at[kind * nm + i], tmp, psem.at[0]).start()
            local(y.at[i], yb, psem.at[1]).start()

        def post_b(t):
            kind, i = sched(t)
            n = kind * nm + i
            ap = t % 2

            @pl.when(t >= 2)
            def _():
                with SC('w_out'):
                    wait_out(t - 2)
            local(vx.at[n], tmp, psem.at[0]).wait()
            local(y.at[i], yb, psem.at[1]).wait()
            last = is1 & (kind == 0)
            rb = min(64, T)

            def rows(b):
                lo = pl.ds(pl.multiple_of(b * rb, rb), rb)
                mine = pl.ds(pl.multiple_of(k * T + b * rb, rb), rb)
                h = (ab[ap, mine, :].astype(F32) + (acc[ap, mine, :] + tmp[lo, :])).astype(BF16)

                @pl.when(last)
                def _():
                    d = h.astype(F32) - yb[lo, :].astype(F32)
                    ob[ap, lo, :] = (d * inv).astype(BF16)
                    sq = jnp.sum((d * d).reshape(rb // 8, 8, D), axis=0)
                    part = lacc[...]
                    for c in range(D // 128):
                        part = part + sq[:, c * 128:(c + 1) * 128]
                    lacc[...] = part

                @pl.when(jnp.logical_not(last))
                def _():
                    ob[ap, lo, :] = h
            with SC('post_rows'):
                loop(T // rb, rows)

            @pl.when(is0)
            def _():
                remote(ob.at[ap], ha.at[0, i, own], z_s.at[n], z_r.at[n], (1 - s, r)).start()

            @pl.when(is1 & (kind == 1))
            def _():
                remote(ob.at[ap], ea.at[0, i, own], z_s.at[n], z_r.at[n], (1 - s, r)).start()

            @pl.when(last)
            def _():
                for c in give(ob.at[ap], ea, nm + i, i, False):
                    c.start()
                local(ob.at[ap], ea.at[0, i, own], lsem.at[i]).start()

        j_a = max(0, nj // 2 - 2)
        j_b = j_a + 1
        j_c = min(j_b + 1, nj - 2)
        j_d = nj - 2

        def slot(t):
            kind, i = sched(t)
            ap = t % 2
            more = t + 1 < nm + nm * s

            @pl.when(is0 | (t == 0))
            def _():
                prep_a(t)
                prep_b(t)

            @pl.when(t == 0)
            def _():
                first_weights(0, PAIR[1:])

            local(ha.at[0, i, own], ab.at[ap, own], alsem.at[ap, 0]).wait()
            local(ha.at[0, i, oth], ab.at[ap, oth], alsem.at[ap, 1]).wait()

            @pl.when(is0)
            def _():
                local(ab.at[ap, own], ha.at[0, i, own], hsem).start()

            def hooks(j):
                late = is1 & (t > 0)

                @pl.when(late & (j == j_a))
                def _():
                    post_a(t - 1)

                @pl.when(late & (j == j_b))
                def _():
                    post_b(t - 1)

                @pl.when(is1 & more & (j == jnp.where(t == 0, j_d, j_c)))
                def _():
                    prep_a(t + 1)

                @pl.when(is1 & more & (j == j_d))
                def _():
                    prep_b(t + 1)

            def run(c1, c2, before, first, second, after):
                c1(t, 0).wait()
                c1(t, 2).start()
                before(0)
                acc[ap] = jnp.zeros((T2, D), F32)
                first(0)
                after(0)

                def step(j):
                    c1(t, j + 1).wait()
                    c2(t, j).wait()

                    @pl.when(j + 3 < nj)
                    def _():
                        c1(t, j + 3).start()

                    @pl.when(j + 2 < nj)
                    def _():
                        c2(t, j + 2).start()
                    hooks(j)
                    before(j + 1)
                    first(j + 1)
                    acc[ap] += second(j)
                    after(j + 1)
                loop(nj - 1, step)
                c2(t, nj - 1).wait()

                @pl.when(more)
                def _():
                    first_weights(t + 1, PAIR)
                acc[ap] += second(nj - 1)

            def g_out(j, dst):
                return local(go.at[j % 2], dst.at[i, :, fcols(j)], gsem.at[j % 2])

            def u_out(j):
                return local(uo.at[j % 2], ub.at[i, :, fcols(j)], usem.at[j % 2])

            def mine(j):
                return (j >= q0) & (j < q0 + nq)

            def keep(j):
                @pl.when(is1)
                def _():
                    u_out(j).start()
                    g_out(j, gb).start()

                @pl.when(is0 & mine(j))
                def _():
                    rows = pl.ds(pl.multiple_of(i * T2, T2), T2)
                    local(uo.at[j % 2], ua.at[rows, fcols(j - q0)], usem.at[j % 2]).start()
                    local(go.at[j % 2], ga.at[rows, fcols(j - q0)], gsem.at[j % 2]).start()

            def kept(j):
                @pl.when(is1 | mine(j))
                def _():
                    u_out(j).wait()
                    g_out(j, gb).wait()

            @pl.when(kind == 0)
            def _():
                def before(j):
                    @pl.when(j >= 2)
                    def _():
                        kept(j - 2)

                def first(j):
                    for hq in range(4):
                        h = slice(hq * T // 2, (hq + 1) * T // 2)
                        g, uo[j % 2, h] = gelu_both(dot(ab[ap, h], wb1[wslot(t, j)]))
                        go[j % 2, h] = g.astype(BF16)

                with SC('slotF'):
                    run(c_w1, c_w2, before, first, lambda j: dot(go[j % 2], wb2[wslot(t, j)]), keep)
                for j in (nj - 2, nj - 1):
                    kept(j)

            @pl.when(kind == 1)
            def _():
                def before(j):
                    @pl.when(j >= 2)
                    def _():
                        g_out(j - 2, qb).wait()
                    u_in(t, i, j).wait()

                    @pl.when(j + 3 < nj)
                    def _():
                        u_in(t, i, j + 3).start()

                def first(j):
                    p = dot_cols(ab[ap], wb2[wslot(t, j)]).astype(BF16)
                    go[j % 2] = (p.astype(F32) * ui[(t * nj + j) % 4]).astype(BF16)
                with SC('slotB'):
                    run(c_w2, c_w1, before, first, lambda j: dot_cols(go[j % 2], wb1[wslot(t, j)]), lambda j: g_out(j, qb).start())
                for j in (nj - 2, nj - 1):
                    g_out(j, qb).wait()

            @pl.when(is0)
            def _():
                local(ab.at[ap, own], ha.at[0, i, own], hsem).wait()
            exchange(t).start()

            @pl.when(is0 | (t == nt - 1))
            def _():
                post_a(t)
                post_b(t)

        first_weights(0, PAIR[:1])
        n_slots = nm + nm * s
        lax.fori_loop(0, n_slots, lambda t, c: (slot(t), c)[1], 0)

    pl.run_scoped(
        phase1,
        VMEM((3, D, fs), BF16), VMEM((3, fs, D), BF16), VMEM((2, T2, D), BF16), VMEM((2, T2, D), F32),
        VMEM((2, T2, fs), F32), VMEM((4, T2, fs), F32), VMEM((2, T2, fs), BF16),
        VMEM((T, D), F32), VMEM((T, D), BF16),
        DMA((2, 3)), DMA((2, 2)), DMA((2,)), DMA((4,)), DMA((2,)), DMA((2,)), DMA((nm,)), DMA,
    )

    def loss_copy(d):
        return remote(lacc, lb.at[r], ls_s.at[d], ls_r.at[r], (d // 8, d % 8))

    def loss_self():
        return local(lacc, lb.at[r], ls_s.at[8 + r])

    @pl.when(is1)
    def _():
        def send(d):
            @pl.when(d != 8 + r)
            def _():
                loss_copy(d).start()
        loop(16, send)
        loss_self().start()

    nc = 4 * nm

    def all_tokens(wq1, wq2, ab, uo, ui, go, qsem, alsem, usem, isem, gsem):
        def c_q1(j):
            return local(w1.at[:, wcols(j, fq)], wq1.at[j], qsem.at[0, j])

        def c_q2(j):
            return local(w2.at[wcols(j, fq), :], wq2.at[j], qsem.at[1, j])
        for j in range(nq):
            c_q1(j).start()

        def arrive(A, n, c, i):
            @pl.when(c == 1)
            def _():
                for h in PAIR:
                    with SC('a_c1'):
                        got_half(n_r.at[n, h]).wait_recv()
                remote(A.at[1, i], A.at[2, i], f_s.at[n], f_r.at[n], (s, pr)).start()

            @pl.when(c == 2)
            def _():
                with SC('a_c2'):
                    remote(A.at[1, i], A.at[2, i], f_s.at[n], f_r.at[n], (s, pr)).wait_recv()

            @pl.when(c == 3)
            def _():
                with SC('a_c3'):
                    got_half(x_r.at[n]).wait_recv()
                remote(A.at[3, i, own], A.at[3, i, own], h_s.at[n], h_r.at[n], (s, pr)).start()
                with SC('a_c3b'):
                    got_half(h_r.at[n]).wait_recv()

        def c_ab(A, c, i, v):
            return local(A.at[c, i], ab.at[v % 2], alsem.at[v % 2])

        def block(c, i):
            return pl.ds(pl.multiple_of((c * nm + i) * T2, T2), T2)

        def pass_on(i):
            n = nm + i
            with SC('a_z'):
                got_half(z_r.at[n]).wait_recv()
            for cp in give(ea.at[0, i, own], ea, n, i, True):
                cp.start()

        def run(nc, A, at, ready, before, first, outs):
            def load(v):
                c, i = at(v)
                ready(c, i)
                c_ab(A, c, i, v).start()
            load(0)

            def chunk(v):
                c, i = at(v)
                c_ab(A, c, i, v).wait()

                def step(j):
                    g = v * nq + j

                    @pl.when((j == nq - 2) & (v + 1 < nc))
                    def _():
                        load(v + 1)

                    @pl.when(g >= 2)
                    def _():
                        for o in outs(g - 2):
                            o.wait()
                    before(g)
                    first(v, j, g % 2)
                    for o in outs(g):
                        o.start()
                with SC('uchunk'):
                    loop(nq, step)
            loop(nc, chunk)
            for g in (nc * nq - 2, nc * nq - 1):
                for o in outs(g):
                    o.wait()

        def at_h(v):
            return 1 + v // nm, v % nm

        def outs_h(g):
            c, i = at_h(g // nq)
            return [local(uo.at[g % 2], ua.at[block(c, i), fcols(g % nq)], usem.at[g % 2]),
                    local(go.at[g % 2], ga.at[block(c, i), fcols(g % nq)], gsem.at[g % 2])]

        def before_h(g):
            @pl.when(g < nq)
            def _():
                c_q1(g).wait()
                c_q2(g).start()

        def first_h(v, j, sl):
            for hq in range(4):
                h = slice(hq * T // 2, (hq + 1) * T // 2)
                g, uo[sl, h] = gelu_both(dot(ab[v % 2, h], wq1[j]))
                go[sl, h] = g.astype(BF16)

        def ready_h(c, i):
            @pl.when((c == 2) & (i == nm // 2))
            def _():
                pass_on(0)
            arrive(ha, i, c, i)
        run(3 * nm, ha, at_h, ready_h, before_h, first_h, outs_h)

        def at_e(v):
            return v % 4, v // 4

        def outs_e(g):
            c, i = at_e(g // nq)
            return [local(go.at[g % 2], qa.at[block(c, i), fcols(g % nq)], gsem.at[g % 2])]

        def u_in(g):
            c, i = at_e(g // nq)
            return local(ua.at[block(c, i), fcols(g % nq)], ui.at[g % 4], isem.at[g % 4])

        def before_e(g):
            @pl.when(g < nq)
            def _():
                c_q2(g).wait()
            u_in(g).wait()

            @pl.when(g + 3 < nc * nq)
            def _():
                u_in(g + 3).start()

        def ready_e(c, i):
            n = nm + i

            @pl.when(c == 0)
            def _():
                with SC('a_d'):
                    got_half(d_r.at[n]).wait_recv()
            arrive(ea, n, c, i)

            @pl.when((c == 1) & (i + 1 < nm))
            def _():
                pass_on(i + 1)

        def first_e(v, j, sl):
            p = dot_cols(ab[v % 2], wq2[j]).astype(BF16)
            go[sl] = (p.astype(F32) * ui[(v * nq + j) % 4]).astype(BF16)
        for g in AHEAD:
            u_in(g).start()
        run(nc, ea, at_e, ready_e, before_e, first_e, outs_e)

    def sums0(hv, bv, o, tb, tsem, bsem, osem):
        nw = 4 * nq

        def at(w):
            return w // (2 * nq), w % nq, (w // nq) % 2

        def load(w):
            _, j, q = at(w)
            for qq, A in ((0, qa), (1, ga)):
                @pl.when(q == qq)
                def _():
                    local(A.at[:, fcols(j)], bv.at[w % 2], bsem.at[w % 2]).start()

        def far(w, q, m):
            j = at(w)[1]
            return remote(pb.at[q, j, 2 + m], (m1, m2)[q].at[:, wcols(j, fq)], pe_s.at[q, m, j], pe_r.at[q, k, j], (s, nb - k + m))

        def near(w, q):
            j = at(w)[1]
            return remote(pb.at[q, j, 1 - k], (m1, m2)[q].at[:, wcols(j, fq)], ms_s.at[q, j], ms_r.at[q, j], (s, pr))

        def ship(w):
            ps, j, q = at(w)
            for qq in PAIR:
                @pl.when(q == qq)
                def _():
                    for m in PAIR:
                        local(o.at[w % 2, m], pb.at[qq, j, m], osem.at[w % 2, m]).wait()

                    @pl.when(ps == 0)
                    def _():
                        for m in PAIR:
                            far(w, qq, m).start()

                    @pl.when(ps == 1)
                    def _():
                        near(w, qq).start()

        def one(ps):
            cols = pl.ds(pl.multiple_of((nb // 2) * dq * (1 - ps) + (r // 2) * dq * ps, 128), dq)
            for qq, A in ((0, ha), (1, ea)):
                def c_t(v):
                    return local(A.at[v // nm, v % nm, :, cols], tb.at[v % 8], tsem.at[v % 8])
                for v in range(7):
                    c_t(v).start()

                def build(v):
                    c_t(v).wait()

                    @pl.when(v + 7 < nc)
                    def _():
                        c_t(v + 7).start()
                    hv[qq, :, pl.ds(pl.multiple_of(v * T2, T2), T2)] = tb[v % 8].T
                with SC('build0'):
                    loop(nc, build)

                def unit(j):
                    w = (ps * 2 + qq) * nq + j
                    local(qa.at[:, fcols(j)], bv.at[w % 2], bsem.at[w % 2]).wait()

                    @pl.when(w + 1 < nw)
                    def _():
                        load(w + 1)

                    def grads(m):
                        rows = pl.ds(pl.multiple_of(m * dr, dr), dr)

                        @pl.when((w >= 1) & (m == 1))
                        def _():
                            ship(w - 1)
                        o[w % 2, m] = dot(hv[qq, rows, :], bv[w % 2])
                        here = (ps == 1) & (m == k)

                        @pl.when(here)
                        def _():
                            local(o.at[w % 2, m], (m1, m2)[qq].at[:, wcols(j, fq)], osem.at[w % 2, m]).start()

                        @pl.when(jnp.logical_not(here))
                        def _():
                            local(o.at[w % 2, m], pb.at[qq, j, 2 * (1 - ps) + m], osem.at[w % 2, m]).start()
                    with SC('grads0'):
                        loop(2, grads)
                loop(nq, unit)

        load(0)
        loop(2, one)
        ship(nw - 1)

        def finish(j):
            w = j
            for q in PAIR:
                near(w, q).wait()
                for m in PAIR:
                    far(w, q, m).wait_send()
                    remote(pb.at[q, j, 0], (m1, m2)[q].at[:, wcols(j, fq)], ms_s.at[q, j], pe_r.at[q, m, j], (s, pr)).wait_recv()
        with SC('finish0'):
            loop(nq, finish)

    def sums1(wb1, wb2, ht, et, gv, qv, ab, o, dv, wsem, tsem, asem, gqsem, osem):
        def weights(j):
            return (local(w1.at[:, wcols(j, fb)], wb1.at[j % 2], wsem.at[0, j % 2]),
                    local(w2.at[wcols(j, fb), :], wb2.at[j % 2], wsem.at[1, j % 2]))

        def stream(v):
            i, sl = v % nm, v % 2
            return (local(ha.at[1, i], ab.at[sl], asem.at[0, sl]), local(ea.at[1, i], ab.at[2 + sl], asem.at[1, sl]))

        def saved(j, i):
            rows = pl.ds(pl.multiple_of(i * T2, T2), T2)
            return (local(gb.at[i, :, fcols(j)], gv.at[rows], gqsem.at[0, i]),
                    local(qb.at[i, :, fcols(j)], qv.at[rows], gqsem.at[1, i]))

        for c in weights(0):
            c.start()

        cols = (chip_cols(r), chip_cols(pe))
        for q, A, dst in ((0, ha, ht), (1, ea, et)):
            def c_t(v):
                return [local(A.at[v // nm, v % nm, :, cols[c]], ab.at[v % 4, :, c * dq:(c + 1) * dq], tsem.at[v % 4, c]) for c in PAIR]

            def start(v):
                @pl.when(v >= nm)
                def _():
                    for h in PAIR:
                        got_half(n_r.at[q * nm + v - nm, h]).wait_recv()
                for c in c_t(v):
                    c.start()
            for v in AHEAD:
                start(v)

            def build(v):
                for c in c_t(v):
                    c.wait()

                @pl.when(v + 3 < 2 * nm)
                def _():
                    start(v + 3)
                for c in PAIR:
                    dst[c * dq:(c + 1) * dq, pl.ds(pl.multiple_of(v * T2, T2), T2)] = ab[v % 4, :, c * dq:(c + 1) * dq].T
            with SC('build1'):
                loop(2 * nm, build)

        for c in stream(0):
            c.start()

        def kept(q, j, m):
            mine = local(o.at[q, m], (m1, m2)[q].at[:, wcols(j, fb)], osem.at[q, m])
            rest = local(o.at[q, m], pb.at[q, j, m], osem.at[q, m])
            return mine, rest

        def far(j):
            return [remote(pb.at[q, j, 2 + c], (r1, r2)[q].at[:, wcols(j, fb)], pe_s.at[q, c, j], pe_r.at[q, k, j], (s, pe - k + c))
                    for q in PAIR for c in PAIR]

        def near(j):
            return [remote(pb.at[q, j, 1 - k], (m1, m2)[q].at[:, wcols(j, fb)], ms_s.at[q, j], ms_r.at[q, j], (s, pr)) for q in PAIR]

        def ship(j, m0, copies):
            for q in PAIR:
                for m in (m0, m0 + 1):
                    kept(q, j, m)[1].wait()
            for c in copies:
                c.start()

        def part(j):
            ws = j % 2
            for c in weights(j):
                c.wait()

            @pl.when(j >= 1)
            def _():
                ship(j - 1, 0, near(j - 1))

            def again(i):
                v = j * nm + i
                sl = v % 2
                for c in stream(v):
                    c.wait()

                @pl.when(v + 1 < nj * nm)
                def _():
                    for c in stream(v + 1):
                        c.start()
                for c in saved(j, i):
                    c.start()
                rows = pl.ds(pl.multiple_of((nm + i) * T2, T2), T2)
                for h in range(4):
                    T4 = T // 2
                    part_rows = pl.ds(pl.multiple_of((nm + i) * T2 + h * T4, T4), T4)
                    g, dv[h * T4:(h + 1) * T4] = gelu_both(dot(ab[sl, h * T4:(h + 1) * T4], wb1[ws]))
                    gv[part_rows, :] = g.astype(BF16)
                p = dot_cols(ab[2 + sl], wb2[ws]).astype(BF16)
                qv[rows, :] = (p.astype(F32) * dv[...]).astype(BF16)
            with SC('again'):
                loop(nm, again)

            @pl.when(j + 1 < nj)
            def _():
                for c in weights(j + 1):
                    c.start()
            loop(nm, lambda i: [c.wait() for c in saved(j, i)])

            def grads(v):
                m = (v + 2) % 4
                rows = pl.ds(pl.multiple_of(m * dr, dr), dr)

                @pl.when(v == 3)
                def _():
                    ship(j, 2, far(j))
                o[0, m] = dot(ht[rows, :], qv[...])
                o[1, m] = dot(et[rows, :], gv[...])
                for q in PAIR:
                    mine, rest = kept(q, j, m)

                    @pl.when(m == k)
                    def _():
                        mine.start()

                    @pl.when(m != k)
                    def _():
                        rest.start()
            with SC('grads1'):
                loop(4, grads)
        loop(nj, part)
        ship(nj - 1, 0, near(nj - 1))

        def finish(j):
            for c in far(j) + near(j):
                c.wait_send()
            for q in PAIR:
                remote(pb.at[q, j, 0], (m1, m2)[q].at[:, wcols(j, fb)], ms_s.at[q, j], ms_r.at[q, j], (s, pr)).wait_recv()
                for c in PAIR:
                    remote(pb.at[q, j, 0], (r1, r2)[q].at[:, wcols(j, fb)], ms_s.at[q, j], pe_r.at[q, c, j], (s, pr)).wait_recv()
        with SC('finish1'):
            loop(nj, finish)

    nr = 2 * nm * T2

    @pl.when(is0)
    def _():
        pl.run_scoped(
            all_tokens,
            VMEM((nq, D, fs), BF16), VMEM((nq, fs, D), BF16), VMEM((2, T2, D), BF16),
            VMEM((2, T2, fs), F32), VMEM((4, T2, fs), F32), VMEM((2, T2, fs), BF16),
            DMA((2, nq)), DMA((2,)), DMA((2,)), DMA((4,)), DMA((2,)),
        )
        pl.run_scoped(
            sums0,
            VMEM((2, dq, 2 * nr), BF16), VMEM((2, 2 * nr, fs), BF16), VMEM((2, 2, dr, fs), F32), VMEM((8, T2, dq), BF16),
            DMA((8,)), DMA((2,)), DMA((2, 2)),
        )

    @pl.when(is1)
    def _():
        pl.run_scoped(
            sums1,
            VMEM((2, D, fs), BF16), VMEM((2, fs, D), BF16),
            VMEM((2 * dq, nr), BF16), VMEM((2 * dq, nr), BF16), VMEM((nr, fs), BF16), VMEM((nr, fs), BF16),
            VMEM((4, T2, D), BF16), VMEM((2, 4, dr, fs), F32), VMEM((T2, fs), F32),
            DMA((2, 2)), DMA((4, 2)), DMA((2, 2)), DMA((2, nm)), DMA((2, 4)),
        )

    for i in (nm - 2, nm - 1):
        n = i + nm * s
        remote(ob.at[0], ea.at[0, i, own], z_s.at[n], z_r.at[n], (1 - s, r)).wait_send()

    def settle(n):
        A = ha

        @pl.when(is0 | (n < nm))
        def _():
            for c in give(A.at[0, 0, own], A, n, 0, False):
                c.wait_send()

        @pl.when(is0)
        def _():
            remote(A.at[3, 0, own], A.at[3, 0, own], x_s.at[n], x_r.at[n], (s, dg)).wait_send()
            remote(A.at[3, 0, own], A.at[3, 0, own], h_s.at[n], h_r.at[n], (s, pr)).wait_send()
            remote(A.at[1, 0], A.at[2, 0], f_s.at[n], f_r.at[n], (s, pr)).wait_send()
    with SC('settle'):
        loop(nt, settle)

    @pl.when(is1)
    def _():
        def sent(d):
            @pl.when(d != 8 + r)
            def _():
                loss_copy(d).wait_send()
        loop(16, sent)
        loss_self().wait()

    def got(n):
        @pl.when(is0 | (n != r))
        def _():
            remote(lacc, lb.at[n], ls_s.at[n], ls_r.at[n], (s, r)).wait_recv()
    loop(8, got)


def solution(mesh):
    n_data = mesh.shape['data']

    def per_device(inputs, targets, w_up, w_down):
        nm, T, D = inputs.shape
        F = w_up.shape[2]
        Fk = F // 2
        fs = min(512, Fk // 4)
        nj = Fk // fs
        dr = D // 8
        inv = 1.0 / (n_data * nm * T)
        dims = (nm, T, D, Fk, fs, inv)
        sd = jax.ShapeDtypeStruct
        rows = 4 * nm * 2 * T
        out_shape = [
            sd((dr, F), F32), sd((dr, F), F32), sd((dr, F), F32), sd((dr, F), F32), sd((8, 8, 128), F32),
            sd((4, nm, 2 * T, D), BF16), sd((4, nm, 2 * T, D), BF16),
            sd((nm, 2 * T, Fk), F32), sd((nm, 2 * T, Fk), BF16), sd((nm, 2 * T, Fk), BF16),
            sd((rows, Fk // 2), F32), sd((rows, Fk // 2), BF16), sd((rows, Fk // 2), BF16),
            sd((2 * nm, T, D), F32), sd((2, nj, 4, dr, fs), F32),
        ]
        any_spec = pl.BlockSpec(memory_space=pl.ANY)
        n2 = 2 * nm
        outs = pl.pallas_call(
            functools.partial(kernel, dims),
            out_shape=out_shape,
            in_specs=[any_spec] * 4,
            out_specs=[any_spec] * len(out_shape),
            scratch_shapes=[
                VMEM((8, 128), F32), VMEM((2, T, D), BF16),
                DMA((n2,)), DMA((n2,)), DMA((n2,)), DMA((n2,)), DMA((n2,)), DMA((n2,)), DMA((n2, 2)), DMA((n2, 2)),
                DMA((n2,)), DMA((n2,)), DMA((n2,)), DMA((n2,)), DMA((n2,)), DMA((n2,)),
                DMA((2, nj)), DMA((2, nj)), DMA((2, 2, nj)), DMA((2, 2, nj)), DMA((16,)), DMA((8,)),
            ],
            compiler_params=pltpu.CompilerParams(has_side_effects=True, vmem_limit_bytes=67_000_000),
            cost_estimate=pl.CostEstimate(flops=16 * nm * T * D * F, bytes_accessed=10**9, transcendentals=0),
            name='train_step',
        )(inputs, targets, w_up.reshape(D, F), w_down.reshape(F, D))
        m1, r1, m2, r2, lb = outs[:5]
        loss = jnp.sum(lb) * (0.5 * inv)
        whole = lax.axis_index('stage') == 0
        up = jnp.where(whole, m1, m1 + r1)
        down = jnp.where(whole, m2, m2 + r2)
        return loss, up[None], down.T[None]

    return jax.shard_map(per_device, mesh=mesh, in_specs=(P('data', None, None), P('data', None, None), P('stage', None, None), P('stage', None, None)), out_specs=(P(), P('stage', 'data', None), P('stage', None, 'data')), check_vma=False)
```

```python
import functools
import math

import jax
import jax.numpy as jnp
from jax import lax
from jax.experimental import pallas as pl
from jax.experimental.pallas import tpu as pltpu
from jax.sharding import PartitionSpec as P

F32 = jnp.float32
BF16 = jnp.bfloat16
MESH = pl.DeviceIdType.MESH
COLS = (((1,), (1,)), ((), ()))
GC = math.sqrt(2.0 / math.pi)
DMA = pltpu.SemaphoreType.DMA
PAIR = (0, 1)
AHEAD = (0, 1, 2)
VMEM = pltpu.VMEM


def dot(a, b):
    return jnp.dot(a, b, preferred_element_type=F32)


def dot_cols(a, b):
    return lax.dot_general(a, b, COLS, preferred_element_type=F32)


def gelu_both(u):
    u2 = u * u
    t = jnp.tanh(GC * (u + 0.044715 * (u2 * u)))
    half = 0.5 * (1.0 + t)
    return u * half, half + (0.5 * u) * (1.0 - t * t) * (GC + (3.0 * 0.044715 * GC) * u2)


def loop(n, body):
    lax.fori_loop(0, n, lambda i, c: (body(i), c)[1], 0)


def local(src, dst, sem):
    return pltpu.make_async_copy(src, dst, sem)


def remote(src, dst, ss, rs, dev):
    return pltpu.make_async_remote_copy(src_ref=src, dst_ref=dst, send_sem=ss, recv_sem=rs, device_id=dev, device_id_type=MESH)


def kernel(dims, x, y, w1, w2, m1, r1, m2, r2, lb, ha, ea, ub, gb, qb, ua, ga, qa, vx, pb,
           lacc, ob, z_s, z_r, d_s, d_r, v_s, v_r, n_s, n_r, x_s, x_r, f_s, f_r, h_s, h_r, ms_s, ms_r, pe_s, pe_r, ls_s, ls_r):
    nm, T, D, Fk, fs, inv = dims
    nj = Fk // fs
    nq = nj // 2
    nt = 2 * nm
    T2 = 2 * T
    dq, dr = D // 4, D // 8
    s = lax.axis_index('stage')
    r = lax.axis_index('data')
    k = r % 2
    xb = (r // 2) % 2
    yb_ = r // 4
    pr = r + 1 - 2 * k
    fx = r + 2 - 4 * xb
    fy = r + 4 - 8 * yb_
    dg = fy + 2 - 4 * xb
    ry, rx = fy - k, fx - k + 1
    nb = fy * (1 - k) + fx * k
    pe = fx * (1 - k) + fy * k
    fb = k * Fk
    q0 = (yb_ * (1 - k) + xb * k) * nq
    fq = fb + q0 * fs
    own = pl.ds(pl.multiple_of(k * T, T), T)
    oth = pl.ds(pl.multiple_of((1 - k) * T, T), T)
    is0, is1 = s == 0, s == 1

    def fcols(j):
        return pl.ds(pl.multiple_of(j * fs, fs), fs)

    def wcols(j, base):
        return pl.ds(pl.multiple_of(base + j * fs, fs), fs)

    def chip_cols(dev):
        return pl.ds(pl.multiple_of((dev // 2) * dq, 128), dq)

    def give(src, A, n, i, far):
        out = [
            remote(src, A.at[0, i, own], d_s.at[n], d_r.at[n], (s, pr)),
            remote(src, A.at[1, i, own], n_s.at[n, 0], n_r.at[n, k], (s, ry)),
            remote(src, A.at[1, i, own], n_s.at[n, 1], n_r.at[n, k], (s, rx)),
        ]
        if far:
            out.append(remote(src, A.at[3, i, own], x_s.at[n], x_r.at[n], (s, dg)))
        return out

    def got_half(sem):
        return remote(ha.at[0, 0, own], ha.at[0, 0, oth], x_s.at[0], sem, (s, pr))

    @pl.when(is0)
    def _():
        for i in range(nm):
            for c in give(x.at[i], ha, i, i, True):
                c.start()

    def phase1(wb1, wb2, ab, acc, uo, ui, go, tmp, yb, wsem, alsem, usem, isem, gsem, psem, lsem, hsem):
        lacc[...] = jnp.zeros_like(lacc)

        def sched(t):
            mid = (t > 0) & (t < nt - 1)
            kind1 = jnp.where(mid, (t + 1) % 2, jnp.where(t == 0, 0, 1))
            i1 = jnp.where(mid, jnp.where(t % 2 == 1, (t + 1) // 2, (t - 2) // 2), jnp.where(t == 0, 0, nm - 1))
            return jnp.where(is1, kind1, 0), jnp.where(is1, i1, t)

        def wslot(t, j):
            return (t * nj + j) % 3

        def c_w1(t, j):
            return local(w1.at[:, wcols(j, fb)], wb1.at[wslot(t, j)], wsem.at[0, wslot(t, j)])

        def c_w2(t, j):
            return local(w2.at[wcols(j, fb), :], wb2.at[wslot(t, j)], wsem.at[1, wslot(t, j)])

        def first_weights(t, js):
            for j in js:
                c_w1(t, j).start()
                c_w2(t, j).start()

        def prep_a(t):
            kind, i = sched(t)

            @pl.when(is1 & (kind == 0))
            def _():
                got_half(z_r.at[i]).wait_recv()
                for c in give(ha.at[0, i, own], ha, i, i, False):
                    c.start()

        def u_in(t, i, j):
            at = (t * nj + j) % 4
            return local(ub.at[i, :, fcols(j)], ui.at[at], isem.at[at])

        def prep_b(t):
            kind, i = sched(t)
            ap = t % 2
            for kk, A in ((0, ha), (1, ea)):
                @pl.when(kind == kk)
                def _():
                    got_half(d_r.at[kk * nm + i]).wait_recv()
                    if kk == 1:
                        local(ob.at[0], ea.at[0, i, own], lsem.at[i]).wait()
                        for j in AHEAD:
                            u_in(t, i, j).start()
                    if kk == 0:
                        @pl.when(is0)
                        def _():
                            local(x.at[i], ab.at[ap, own], alsem.at[ap, 0]).start()

                    @pl.when(is1)
                    def _():
                        local(A.at[0, i, own], ab.at[ap, own], alsem.at[ap, 0]).start()
                    local(A.at[0, i, oth], ab.at[ap, oth], alsem.at[ap, 1]).start()

        def exchange(t):
            kind, i = sched(t)
            n = kind * nm + i
            return remote(acc.at[t % 2, oth], vx.at[n], v_s.at[n], v_r.at[n], (s, pr))

        def wait_out(t):
            kind, i = sched(t)

            @pl.when(is0 | (kind == 1))
            def _():
                n = kind * nm + i
                remote(ob.at[0], ea.at[0, i, own], z_s.at[n], z_r.at[n], (1 - s, r)).wait_send()

            @pl.when(is1 & (kind == 0))
            def _():
                for c in give(ob.at[0], ea, nm + i, i, False):
                    c.wait_send()

        def post_a(t):
            kind, i = sched(t)
            exchange(t).wait()
            local(vx.at[kind * nm + i], tmp, psem.at[0]).start()
            local(y.at[i], yb, psem.at[1]).start()

        def post_b(t):
            kind, i = sched(t)
            n = kind * nm + i
            ap = t % 2

            @pl.when(t >= 2)
            def _():
                wait_out(t - 2)
            local(vx.at[n], tmp, psem.at[0]).wait()
            local(y.at[i], yb, psem.at[1]).wait()
            last = is1 & (kind == 0)
            rb = min(64, T)

            def rows(b):
                lo = pl.ds(pl.multiple_of(b * rb, rb), rb)
                mine = pl.ds(pl.multiple_of(k * T + b * rb, rb), rb)
                h = (ab[ap, mine, :].astype(F32) + (acc[ap, mine, :] + tmp[lo, :])).astype(BF16)

                @pl.when(last)
                def _():
                    d = h.astype(F32) - yb[lo, :].astype(F32)
                    ob[ap, lo, :] = (d * inv).astype(BF16)
                    sq = jnp.sum((d * d).reshape(rb // 8, 8, D), axis=0)
                    part = lacc[...]
                    for c in range(D // 128):
                        part = part + sq[:, c * 128:(c + 1) * 128]
                    lacc[...] = part

                @pl.when(jnp.logical_not(last))
                def _():
                    ob[ap, lo, :] = h
            loop(T // rb, rows)

            @pl.when(is0)
            def _():
                remote(ob.at[ap], ha.at[0, i, own], z_s.at[n], z_r.at[n], (1 - s, r)).start()

            @pl.when(is1 & (kind == 1))
            def _():
                remote(ob.at[ap], ea.at[0, i, own], z_s.at[n], z_r.at[n], (1 - s, r)).start()

            @pl.when(last)
            def _():
                for c in give(ob.at[ap], ea, nm + i, i, False):
                    c.start()
                local(ob.at[ap], ea.at[0, i, own], lsem.at[i]).start()

        j_a = max(0, nj // 2 - 2)
        j_b = j_a + 1
        j_c = min(j_b + 1, nj - 2)
        j_d = nj - 2

        def slot(t):
            kind, i = sched(t)
            ap = t % 2
            more = t + 1 < nm + nm * s

            @pl.when(is0 | (t == 0))
            def _():
                prep_a(t)
                prep_b(t)

            @pl.when(t == 0)
            def _():
                first_weights(0, PAIR[1:])

            local(ha.at[0, i, own], ab.at[ap, own], alsem.at[ap, 0]).wait()
            local(ha.at[0, i, oth], ab.at[ap, oth], alsem.at[ap, 1]).wait()

            @pl.when(is0)
            def _():
                local(ab.at[ap, own], ha.at[0, i, own], hsem).start()

            def hooks(j):
                late = is1 & (t > 0)

                @pl.when(late & (j == j_a))
                def _():
                    post_a(t - 1)

                @pl.when(late & (j == j_b))
                def _():
                    post_b(t - 1)

                @pl.when(late & more & (j == j_c))
                def _():
                    prep_a(t + 1)

                @pl.when(late & more & (j == j_d))
                def _():
                    prep_b(t + 1)

            def run(c1, c2, before, first, second, after):
                c1(t, 0).wait()
                c1(t, 2).start()
                before(0)
                acc[ap] = jnp.zeros((T2, D), F32)
                first(0)
                after(0)

                def step(j):
                    c1(t, j + 1).wait()
                    c2(t, j).wait()

                    @pl.when(j + 3 < nj)
                    def _():
                        c1(t, j + 3).start()

                    @pl.when(j + 2 < nj)
                    def _():
                        c2(t, j + 2).start()
                    hooks(j)
                    before(j + 1)
                    first(j + 1)
                    acc[ap] += second(j)
                    after(j + 1)
                loop(nj - 1, step)
                c2(t, nj - 1).wait()

                @pl.when(more)
                def _():
                    first_weights(t + 1, PAIR)
                acc[ap] += second(nj - 1)

            def g_out(j, dst):
                return local(go.at[j % 2], dst.at[i, :, fcols(j)], gsem.at[j % 2])

            def u_out(j):
                return local(uo.at[j % 2], ub.at[i, :, fcols(j)], usem.at[j % 2])

            def mine(j):
                return (j >= q0) & (j < q0 + nq)

            def keep(j):
                @pl.when(is1)
                def _():
                    u_out(j).start()
                    g_out(j, gb).start()

                @pl.when(is0 & mine(j))
                def _():
                    rows = pl.ds(pl.multiple_of(i * T2, T2), T2)
                    local(uo.at[j % 2], ua.at[rows, fcols(j - q0)], usem.at[j % 2]).start()
                    local(go.at[j % 2], ga.at[rows, fcols(j - q0)], gsem.at[j % 2]).start()

            def kept(j):
                @pl.when(is1 | mine(j))
                def _():
                    u_out(j).wait()
                    g_out(j, gb).wait()

            @pl.when(kind == 0)
            def _():
                def before(j):
                    @pl.when(j >= 2)
                    def _():
                        kept(j - 2)

                def first(j):
                    for hq in range(4):
                        h = slice(hq * T // 2, (hq + 1) * T // 2)
                        g, uo[j % 2, h] = gelu_both(dot(ab[ap, h], wb1[wslot(t, j)]))
                        go[j % 2, h] = g.astype(BF16)

                run(c_w1, c_w2, before, first, lambda j: dot(go[j % 2], wb2[wslot(t, j)]), keep)
                for j in (nj - 2, nj - 1):
                    kept(j)

            @pl.when(kind == 1)
            def _():
                def before(j):
                    @pl.when(j >= 2)
                    def _():
                        g_out(j - 2, qb).wait()
                    u_in(t, i, j).wait()

                    @pl.when(j + 3 < nj)
                    def _():
                        u_in(t, i, j + 3).start()

                def first(j):
                    p = dot_cols(ab[ap], wb2[wslot(t, j)]).astype(BF16)
                    go[j % 2] = (p.astype(F32) * ui[(t * nj + j) % 4]).astype(BF16)
                run(c_w2, c_w1, before, first, lambda j: dot_cols(go[j % 2], wb1[wslot(t, j)]), lambda j: g_out(j, qb).start())
                for j in (nj - 2, nj - 1):
                    g_out(j, qb).wait()

            @pl.when(is0)
            def _():
                local(ab.at[ap, own], ha.at[0, i, own], hsem).wait()
            exchange(t).start()

            @pl.when(is1 & (t == 0))
            def _():
                prep_a(t + 1)
                prep_b(t + 1)

            @pl.when(is0 | (t == nt - 1))
            def _():
                post_a(t)
                post_b(t)

        first_weights(0, PAIR[:1])
        n_slots = nm + nm * s
        lax.fori_loop(0, n_slots, lambda t, c: (slot(t), c)[1], 0)

    pl.run_scoped(
        phase1,
        VMEM((3, D, fs), BF16), VMEM((3, fs, D), BF16), VMEM((2, T2, D), BF16), VMEM((2, T2, D), F32),
        VMEM((2, T2, fs), F32), VMEM((4, T2, fs), F32), VMEM((2, T2, fs), BF16),
        VMEM((T, D), F32), VMEM((T, D), BF16),
        DMA((2, 3)), DMA((2, 2)), DMA((2,)), DMA((4,)), DMA((2,)), DMA((2,)), DMA((nm,)), DMA,
    )

    def loss_copy(d):
        return remote(lacc, lb.at[r], ls_s.at[d], ls_r.at[r], (d // 8, d % 8))

    def loss_self():
        return local(lacc, lb.at[r], ls_s.at[8 + r])

    @pl.when(is1)
    def _():
        def send(d):
            @pl.when(d != 8 + r)
            def _():
                loss_copy(d).start()
        loop(16, send)
        loss_self().start()

    nc = 4 * nm

    def all_tokens(wq1, wq2, ab, uo, ui, go, qsem, alsem, usem, isem, gsem):
        def c_q1(j):
            return local(w1.at[:, wcols(j, fq)], wq1.at[j], qsem.at[0, j])

        def c_q2(j):
            return local(w2.at[wcols(j, fq), :], wq2.at[j], qsem.at[1, j])
        for j in range(nq):
            c_q1(j).start()

        def arrive(A, n, c, i):
            @pl.when(c == 1)
            def _():
                for h in PAIR:
                    got_half(n_r.at[n, h]).wait_recv()
                remote(A.at[1, i], A.at[2, i], f_s.at[n], f_r.at[n], (s, pr)).start()

            @pl.when(c == 2)
            def _():
                remote(A.at[1, i], A.at[2, i], f_s.at[n], f_r.at[n], (s, pr)).wait_recv()

            @pl.when(c == 3)
            def _():
                got_half(x_r.at[n]).wait_recv()
                remote(A.at[3, i, own], A.at[3, i, own], h_s.at[n], h_r.at[n], (s, pr)).start()
                got_half(h_r.at[n]).wait_recv()

        def c_ab(A, c, i, v):
            return local(A.at[c, i], ab.at[v % 2], alsem.at[v % 2])

        def block(c, i):
            return pl.ds(pl.multiple_of((c * nm + i) * T2, T2), T2)

        def pass_on(i):
            n = nm + i
            got_half(z_r.at[n]).wait_recv()
            for cp in give(ea.at[0, i, own], ea, n, i, True):
                cp.start()

        def run(nc, A, at, ready, before, first, outs):
            def load(v):
                c, i = at(v)
                ready(c, i)
                c_ab(A, c, i, v).start()
            load(0)

            def chunk(v):
                c, i = at(v)
                c_ab(A, c, i, v).wait()

                def step(j):
                    g = v * nq + j

                    @pl.when((j == nq - 2) & (v + 1 < nc))
                    def _():
                        load(v + 1)

                    @pl.when(g >= 2)
                    def _():
                        for o in outs(g - 2):
                            o.wait()
                    before(g)
                    first(v, j, g % 2)
                    for o in outs(g):
                        o.start()
                loop(nq, step)
            loop(nc, chunk)
            for g in (nc * nq - 2, nc * nq - 1):
                for o in outs(g):
                    o.wait()

        def at_h(v):
            return 1 + v // nm, v % nm

        def outs_h(g):
            c, i = at_h(g // nq)
            return [local(uo.at[g % 2], ua.at[block(c, i), fcols(g % nq)], usem.at[g % 2]),
                    local(go.at[g % 2], ga.at[block(c, i), fcols(g % nq)], gsem.at[g % 2])]

        def before_h(g):
            @pl.when(g < nq)
            def _():
                c_q1(g).wait()
                c_q2(g).start()

        def first_h(v, j, sl):
            for hq in range(4):
                h = slice(hq * T // 2, (hq + 1) * T // 2)
                g, uo[sl, h] = gelu_both(dot(ab[v % 2, h], wq1[j]))
                go[sl, h] = g.astype(BF16)

        def ready_h(c, i):
            @pl.when((c == 2) & (i == nm // 2))
            def _():
                pass_on(0)
            arrive(ha, i, c, i)
        run(3 * nm, ha, at_h, ready_h, before_h, first_h, outs_h)

        def at_e(v):
            return v % 4, v // 4

        def outs_e(g):
            c, i = at_e(g // nq)
            return [local(go.at[g % 2], qa.at[block(c, i), fcols(g % nq)], gsem.at[g % 2])]

        def u_in(g):
            c, i = at_e(g // nq)
            return local(ua.at[block(c, i), fcols(g % nq)], ui.at[g % 4], isem.at[g % 4])

        def before_e(g):
            @pl.when(g < nq)
            def _():
                c_q2(g).wait()
            u_in(g).wait()

            @pl.when(g + 3 < nc * nq)
            def _():
                u_in(g + 3).start()

        def ready_e(c, i):
            n = nm + i

            @pl.when(c == 0)
            def _():
                got_half(d_r.at[n]).wait_recv()
            arrive(ea, n, c, i)

            @pl.when((c == 1) & (i + 1 < nm))
            def _():
                pass_on(i + 1)

        def first_e(v, j, sl):
            p = dot_cols(ab[v % 2], wq2[j]).astype(BF16)
            go[sl] = (p.astype(F32) * ui[(v * nq + j) % 4]).astype(BF16)
        for g in AHEAD:
            u_in(g).start()
        run(nc, ea, at_e, ready_e, before_e, first_e, outs_e)

    def sums0(hv, bv, o, tb, tsem, bsem, osem):
        nw = 4 * nq

        def at(w):
            return w // (2 * nq), w % nq, (w // nq) % 2

        def load(w):
            _, j, q = at(w)
            for qq, A in ((0, qa), (1, ga)):
                @pl.when(q == qq)
                def _():
                    local(A.at[:, fcols(j)], bv.at[w % 2], bsem.at[w % 2]).start()

        def far(w, q, m):
            j = at(w)[1]
            return remote(pb.at[q, j, 2 + m], (m1, m2)[q].at[:, wcols(j, fq)], pe_s.at[q, m, j], pe_r.at[q, k, j], (s, nb - k + m))

        def near(w, q):
            j = at(w)[1]
            return remote(pb.at[q, j, 1 - k], (m1, m2)[q].at[:, wcols(j, fq)], ms_s.at[q, j], ms_r.at[q, j], (s, pr))

        def ship(w):
            ps, j, q = at(w)
            for qq in PAIR:
                @pl.when(q == qq)
                def _():
                    for m in PAIR:
                        local(o.at[w % 2, m], pb.at[qq, j, m], osem.at[w % 2, m]).wait()

                    @pl.when(ps == 0)
                    def _():
                        for m in PAIR:
                            far(w, qq, m).start()

                    @pl.when(ps == 1)
                    def _():
                        near(w, qq).start()

        def one(ps):
            cols = pl.ds(pl.multiple_of((nb // 2) * dq * (1 - ps) + (r // 2) * dq * ps, 128), dq)
            for qq, A in ((0, ha), (1, ea)):
                def c_t(v):
                    return local(A.at[v // nm, v % nm, :, cols], tb.at[v % 8], tsem.at[v % 8])
                for v in range(7):
                    c_t(v).start()

                def build(v):
                    c_t(v).wait()

                    @pl.when(v + 7 < nc)
                    def _():
                        c_t(v + 7).start()
                    hv[qq, :, pl.ds(pl.multiple_of(v * T2, T2), T2)] = tb[v % 8].T
                loop(nc, build)

                def unit(j):
                    w = (ps * 2 + qq) * nq + j
                    local(qa.at[:, fcols(j)], bv.at[w % 2], bsem.at[w % 2]).wait()

                    @pl.when(w + 1 < nw)
                    def _():
                        load(w + 1)

                    def grads(m):
                        rows = pl.ds(pl.multiple_of(m * dr, dr), dr)

                        @pl.when((w >= 1) & (m == 1))
                        def _():
                            ship(w - 1)
                        o[w % 2, m] = dot(hv[qq, rows, :], bv[w % 2])
                        here = (ps == 1) & (m == k)

                        @pl.when(here)
                        def _():
                            local(o.at[w % 2, m], (m1, m2)[qq].at[:, wcols(j, fq)], osem.at[w % 2, m]).start()

                        @pl.when(jnp.logical_not(here))
                        def _():
                            local(o.at[w % 2, m], pb.at[qq, j, 2 * (1 - ps) + m], osem.at[w % 2, m]).start()
                    loop(2, grads)
                loop(nq, unit)

        load(0)
        loop(2, one)
        ship(nw - 1)

        def finish(j):
            w = j
            for q in PAIR:
                near(w, q).wait()
                for m in PAIR:
                    far(w, q, m).wait_send()
                    remote(pb.at[q, j, 0], (m1, m2)[q].at[:, wcols(j, fq)], ms_s.at[q, j], pe_r.at[q, m, j], (s, pr)).wait_recv()
        loop(nq, finish)

    def sums1(wb1, wb2, ht, et, gv, qv, ab, o, dv, wsem, tsem, asem, gqsem, osem):
        def weights(j):
            return (local(w1.at[:, wcols(j, fb)], wb1.at[j % 2], wsem.at[0, j % 2]),
                    local(w2.at[wcols(j, fb), :], wb2.at[j % 2], wsem.at[1, j % 2]))

        def stream(v):
            i, sl = v % nm, v % 4
            return local(ha.at[1, i], ab.at[sl], asem.at[sl]), local(ea.at[1, i], ab.at[sl], asem.at[sl])

        def fetch(v):
            of_h, of_e = stream(v)
            is_h = v % nt < nm

            @pl.when(is_h)
            def _():
                of_h.start()

            @pl.when(jnp.logical_not(is_h))
            def _():
                of_e.start()

        def saved(j, i):
            rows = pl.ds(pl.multiple_of(i * T2, T2), T2)
            return (local(gb.at[i, :, fcols(j)], gv.at[rows], gqsem.at[0, i]),
                    local(qb.at[i, :, fcols(j)], qv.at[rows], gqsem.at[1, i]))

        for c in weights(0):
            c.start()

        cols = (chip_cols(r), chip_cols(pe))
        for q, A, dst in ((0, ha, ht), (1, ea, et)):
            def c_t(v):
                return [local(A.at[v // nm, v % nm, :, cols[c]], ab.at[v % 4, :, c * dq:(c + 1) * dq], tsem.at[v % 4, c]) for c in PAIR]

            def start(v):
                @pl.when(v >= nm)
                def _():
                    for h in PAIR:
                        got_half(n_r.at[q * nm + v - nm, h]).wait_recv()
                for c in c_t(v):
                    c.start()
            for v in AHEAD:
                start(v)

            def build(v):
                for c in c_t(v):
                    c.wait()

                @pl.when(v + 3 < 2 * nm)
                def _():
                    start(v + 3)
                for c in PAIR:
                    dst[c * dq:(c + 1) * dq, pl.ds(pl.multiple_of(v * T2, T2), T2)] = ab[v % 4, :, c * dq:(c + 1) * dq].T
            loop(2 * nm, build)

        for v in PAIR:
            fetch(v)

        def far(j, q):
            return [remote(pb.at[q, j, 2 + c], (r1, r2)[q].at[:, wcols(j, fb)], pe_s.at[q, c, j], pe_r.at[q, k, j], (s, pe - k + c)) for c in PAIR]

        def near(j, q):
            return [remote(pb.at[q, j, 1 - k], (m1, m2)[q].at[:, wcols(j, fb)], ms_s.at[q, j], ms_r.at[q, j], (s, pr))]

        def ship(q, copies):
            for m in PAIR:
                local(o.at[q, m], pb.at[q, 0, m], osem.at[q, m]).wait()
            for c in copies:
                c.start()

        def sums(j, q, first, hook):
            lhs, rhs, M = ((ht, qv, m1), (et, gv, m2))[q]

            def grads(v):
                m = first + v

                @pl.when(v == 1)
                def _():
                    hook()
                o[q, v] = dot(lhs[pl.ds(pl.multiple_of(m * dr, dr), dr), :], rhs[...])

                @pl.when(m == k)
                def _():
                    local(o.at[q, v], M.at[:, wcols(j, fb)], osem.at[q, v]).start()

                @pl.when(m != k)
                def _():
                    local(o.at[q, v], pb.at[q, j, m], osem.at[q, v]).start()
            loop(2, grads)

        def nothing():
            return None

        def part(j):
            ws = j % 2
            for c in weights(j):
                c.wait()

            @pl.when(j >= 1)
            def _():
                for q in PAIR:
                    ship(q, near(j - 1, q))

            def next_chunk(v):
                stream(v)[0].wait()

                @pl.when(v + 2 < nj * nt)
                def _():
                    fetch(v + 2)
                return v % 4

            def u_again(i):
                sl = next_chunk(j * nt + i)
                for c in saved(j, i):
                    c.start()
                T4 = T2 // 4
                for h in range(4):
                    lo = pl.ds(pl.multiple_of(i * T2 + h * T4, T4), T4)
                    hi = pl.ds(pl.multiple_of((nm + i) * T2 + h * T4, T4), T4)
                    g, dv[lo, :] = gelu_both(dot(ab[sl, h * T4:(h + 1) * T4], wb1[ws]))
                    gv[hi, :] = g.astype(BF16)
            loop(nm, u_again)
            loop(nm, lambda i: saved(j, i)[0].wait())
            sums(j, 1, 2, nothing)

            def p_again(i):
                sl = next_chunk(j * nt + nm + i)

                @pl.when(i == 1)
                def _():
                    ship(1, far(j, 1))
                lo = pl.ds(pl.multiple_of(i * T2, T2), T2)
                hi = pl.ds(pl.multiple_of((nm + i) * T2, T2), T2)
                p = dot_cols(ab[sl], wb2[ws]).astype(BF16)
                qv[hi, :] = (p.astype(F32) * dv[lo, :]).astype(BF16)
            loop(nm, p_again)

            @pl.when(j + 1 < nj)
            def _():
                for c in weights(j + 1):
                    c.start()
            loop(nm, lambda i: saved(j, i)[1].wait())
            sums(j, 0, 2, nothing)
            sums(j, 1, 0, lambda: ship(0, far(j, 0)))
            sums(j, 0, 0, nothing)
        loop(nj, part)
        for q in PAIR:
            ship(q, near(nj - 1, q))

        def finish(j):
            for q in PAIR:
                for c in far(j, q) + near(j, q):
                    c.wait_send()
                remote(pb.at[q, j, 0], (m1, m2)[q].at[:, wcols(j, fb)], ms_s.at[q, j], ms_r.at[q, j], (s, pr)).wait_recv()
                for c in PAIR:
                    remote(pb.at[q, j, 0], (r1, r2)[q].at[:, wcols(j, fb)], ms_s.at[q, j], pe_r.at[q, c, j], (s, pr)).wait_recv()
        loop(nj, finish)

    nr = 2 * nm * T2

    @pl.when(is0)
    def _():
        pl.run_scoped(
            all_tokens,
            VMEM((nq, D, fs), BF16), VMEM((nq, fs, D), BF16), VMEM((2, T2, D), BF16),
            VMEM((2, T2, fs), F32), VMEM((4, T2, fs), F32), VMEM((2, T2, fs), BF16),
            DMA((2, nq)), DMA((2,)), DMA((2,)), DMA((4,)), DMA((2,)),
        )
        pl.run_scoped(
            sums0,
            VMEM((2, dq, 2 * nr), BF16), VMEM((2, 2 * nr, fs), BF16), VMEM((2, 2, dr, fs), F32), VMEM((8, T2, dq), BF16),
            DMA((8,)), DMA((2,)), DMA((2, 2)),
        )

    @pl.when(is1)
    def _():
        pl.run_scoped(
            sums1,
            VMEM((2, D, fs), BF16), VMEM((2, fs, D), BF16),
            VMEM((2 * dq, nr), BF16), VMEM((2 * dq, nr), BF16), VMEM((nr, fs), BF16), VMEM((nr, fs), BF16),
            VMEM((4, T2, D), BF16), VMEM((2, 2, dr, fs), F32), VMEM((nm * T2, fs), F32),
            DMA((2, 2)), DMA((4, 2)), DMA((4,)), DMA((2, nm)), DMA((2, 2)),
        )

    for i in (nm - 2, nm - 1):
        n = i + nm * s
        remote(ob.at[0], ea.at[0, i, own], z_s.at[n], z_r.at[n], (1 - s, r)).wait_send()

    def settle(n):
        A = ha

        @pl.when(is0 | (n < nm))
        def _():
            for c in give(A.at[0, 0, own], A, n, 0, False):
                c.wait_send()

        @pl.when(is0)
        def _():
            remote(A.at[3, 0, own], A.at[3, 0, own], x_s.at[n], x_r.at[n], (s, dg)).wait_send()
            remote(A.at[3, 0, own], A.at[3, 0, own], h_s.at[n], h_r.at[n], (s, pr)).wait_send()
            remote(A.at[1, 0], A.at[2, 0], f_s.at[n], f_r.at[n], (s, pr)).wait_send()
    loop(nt, settle)

    @pl.when(is1)
    def _():
        def sent(d):
            @pl.when(d != 8 + r)
            def _():
                loss_copy(d).wait_send()
        loop(16, sent)
        loss_self().wait()

    def got(n):
        @pl.when(is0 | (n != r))
        def _():
            remote(lacc, lb.at[n], ls_s.at[n], ls_r.at[n], (s, r)).wait_recv()
    loop(8, got)


def solution(mesh):
    n_data = mesh.shape['data']

    def per_device(inputs, targets, w_up, w_down):
        nm, T, D = inputs.shape
        F = w_up.shape[2]
        Fk = F // 2
        fs = min(512, Fk // 4)
        nj = Fk // fs
        dr = D // 8
        inv = 1.0 / (n_data * nm * T)
        dims = (nm, T, D, Fk, fs, inv)
        sd = jax.ShapeDtypeStruct
        rows = 4 * nm * 2 * T
        out_shape = [
            sd((dr, F), F32), sd((dr, F), F32), sd((dr, F), F32), sd((dr, F), F32), sd((8, 8, 128), F32),
            sd((4, nm, 2 * T, D), BF16), sd((4, nm, 2 * T, D), BF16),
            sd((nm, 2 * T, Fk), F32), sd((nm, 2 * T, Fk), BF16), sd((nm, 2 * T, Fk), BF16),
            sd((rows, Fk // 2), F32), sd((rows, Fk // 2), BF16), sd((rows, Fk // 2), BF16),
            sd((2 * nm, T, D), F32), sd((2, nj, 4, dr, fs), F32),
        ]
        any_spec = pl.BlockSpec(memory_space=pl.ANY)
        n2 = 2 * nm
        outs = pl.pallas_call(
            functools.partial(kernel, dims),
            out_shape=out_shape,
            in_specs=[any_spec] * 4,
            out_specs=[any_spec] * len(out_shape),
            scratch_shapes=[
                VMEM((8, 128), F32), VMEM((2, T, D), BF16),
                DMA((n2,)), DMA((n2,)), DMA((n2,)), DMA((n2,)), DMA((n2,)), DMA((n2,)), DMA((n2, 2)), DMA((n2, 2)),
                DMA((n2,)), DMA((n2,)), DMA((n2,)), DMA((n2,)), DMA((n2,)), DMA((n2,)),
                DMA((2, nj)), DMA((2, nj)), DMA((2, 2, nj)), DMA((2, 2, nj)), DMA((16,)), DMA((8,)),
            ],
            compiler_params=pltpu.CompilerParams(has_side_effects=True, vmem_limit_bytes=67_000_000),
            cost_estimate=pl.CostEstimate(flops=16 * nm * T * D * F, bytes_accessed=10**9, transcendentals=0),
            name='train_step',
        )(inputs, targets, w_up.reshape(D, F), w_down.reshape(F, D))
        m1, r1, m2, r2, lb = outs[:5]
        loss = jnp.sum(lb) * (0.5 * inv)
        whole = lax.axis_index('stage') == 0
        up = jnp.where(whole, m1, m1 + r1)
        down = jnp.where(whole, m2, m2 + r2)
        return loss, up[None], down.T[None]

    return jax.shard_map(per_device, mesh=mesh, in_specs=(P('data', None, None), P('data', None, None), P('stage', None, None), P('stage', None, None)), out_specs=(P(), P('stage', 'data', None), P('stage', None, 'data')), check_vma=False)
```
